32 devices in a mesh: rep: 8 (over y, x, core), shard: 4 (over z).
Axes of the slice: x: 2, y: 2, z: 4, core: 2. Of those that a mesh axis runs over, the one named last changes fastest.
Arguments:
- layer_input: bfloat16 [8192, 1024], P(('rep', 'shard')), may hold values from -6 to 6
- query_weight: bfloat16 [1024, 1024], P('shard'), may hold values from -0.1875 to 0.1875
- query_bias: bfloat16 [1024], P('shard'), may hold values from -3 to 3
- key_weight: bfloat16 [1024, 1024], P('shard'), may hold values from -0.1875 to 0.1875
- key_bias: bfloat16 [1024], P('shard'), may hold values from -3 to 3
- value_weight: bfloat16 [1024, 1024], P('shard'), may hold values from -0.1875 to 0.1875
- value_bias: bfloat16 [1024], P('shard'), may hold values from -3 to 3
- output_weight: bfloat16 [1024, 1024], P('shard'), may hold values from -0.75 to 0.75
- output_bias: bfloat16 [1024], P('shard'), may hold values from -2.5 to 2.5
- up_weight: bfloat16 [1024, 4096], P('shard'), may hold values from -0.1875 to 0.1875
- up_bias: bfloat16 [4096], P('shard'), may hold values from -3 to 3
- down_weight: bfloat16 [4096, 1024], P('shard'), may hold values from -0.09375 to 0.09375
- down_bias: bfloat16 [1024], P('shard'), may hold values from -1.1953125 to 1.1953125
- attention_gain_in: bfloat16 [1024], P('shard'), may hold values from 0.25 to 1.75
- attention_gain_out: bfloat16 [1024], P('shard'), may hold values from 0.25 to 1.75
- feedforward_gain_in: bfloat16 [1024], P('shard'), may hold values from 0.25 to 1.75
- feedforward_gain_out: bfloat16 [1024], P('shard'), may hold values from 0.25 to 1.75
- layer_cotangent: bfloat16 [8192, 1024], P(('rep', 'shard')), may hold values from -6 to 6
Outputs:
- layer_output: bfloat16 [8192, 1024], P(('rep', 'shard'))
- input_gradient: float32 [8192, 1024], P(('rep', 'shard'))
- query_weight_gradient: float32 [1024, 1024], P('shard')
- query_bias_gradient: float32 [1024], P('shard')
- key_weight_gradient: float32 [1024, 1024], P('shard')
- key_bias_gradient: float32 [1024], P('shard')
- value_weight_gradient: float32 [1024, 1024], P('shard')
- value_bias_gradient: float32 [1024], P('shard')
- output_weight_gradient: float32 [1024, 1024], P('shard')
- output_bias_gradient: float32 [1024], P('shard')
- up_weight_gradient: float32 [1024, 4096], P('shard')
- up_bias_gradient: float32 [4096], P('shard')
- down_weight_gradient: float32 [4096, 1024], P('shard')
- down_bias_gradient: float32 [1024], P('shard')
- attention_gain_in_gradient: float32 [1024], P('shard')
- attention_gain_out_gradient: float32 [1024], P('shard')
- feedforward_gain_in_gradient: float32 [1024], P('shard')
- feedforward_gain_out_gradient: float32 [1024], P('shard')
The draws below stay inside these ranges and needn't reach their ends.
All inputs are finite; a program needn't handle non-finite values.
Results may differ from the reference program's by a relative error of at most 0.03.
Values may be sent and summed in bfloat16 or wider, within the bound.
No kernel may reach another device: no remote copies, remote signals or barrier semaphores. Data moves between devices by JAX's collectives and lax.ppermute only.
A program may use at most 256 MiB of HBM per device.

```python
import jax
import jax.numpy as jnp
from jax import lax

D = 1024
HEADS = 16
HEAD_DIM = 64
FF = 4096
SEQ = 1024
SEQS = 8
TOKENS = 8192


def block_levels(rng, dims, shards, low, largest):
    gain, own = 1.0, jax.random.fold_in(rng, 6)
    for axis_at, blocks in shards:
        steps = jnp.exp(jax.random.uniform(jax.random.fold_in(own, axis_at), (blocks,), jnp.float32, low / len(shards), largest / len(shards)))
        gain = gain * jnp.repeat(steps, dims[axis_at] // blocks).reshape([-1 if axis == axis_at else 1 for axis in range(len(dims))])
    return gain


def normal_values(key, shape, width, most, cuts=(), kind=jnp.bfloat16):
    gain = block_levels(key, shape, cuts, -0.22, 0.18) if cuts else 1.0
    drawn = jax.random.normal(key, shape, jnp.float32) * width * gain
    return jnp.minimum(jnp.maximum(drawn, -most), most).astype(kind)


def setup_inputs(seed: int = 0) -> dict:
    key_of = jax.random.split(jax.random.key(seed), 19)
    return {
        "layer_input": normal_values(key_of[0], (TOKENS, D), 1.0, 6.0, ((0, 32),)),
        "query_weight": normal_values(key_of[1], (D, D), D ** -0.5, 0.1875, ((0, 4),)),
        "query_bias": normal_values(key_of[2], (D,), 0.5, 3.0, ((0, 4),)),
        "key_weight": normal_values(key_of[3], (D, D), D ** -0.5, 0.1875, ((0, 4),)),
        "key_bias": normal_values(key_of[4], (D,), 0.5, 3.0, ((0, 4),)),
        "value_weight": normal_values(key_of[5], (D, D), D ** -0.5, 0.1875, ((0, 4),)),
        "value_bias": normal_values(key_of[6], (D,), 0.5, 3.0, ((0, 4),)),
        "output_weight": normal_values(key_of[7], (D, D), (D // 16) ** -0.5, 0.75, ((0, 4),)),
        "output_bias": normal_values(key_of[8], (D,), 0.4, 2.5, ((0, 4),)),
        "up_weight": normal_values(key_of[9], (D, FF), D ** -0.5, 0.1875, ((0, 4),)),
        "up_bias": normal_values(key_of[10], (FF,), 0.5, 3.0, ((0, 4),)),
        "down_weight": normal_values(key_of[11], (FF, D), FF ** -0.5, 0.09375, ((0, 4),)),
        "down_bias": normal_values(key_of[12], (D,), 0.2, 1.1953125, ((0, 4),)),
        "attention_gain_in": jnp.clip(1.0 + 0.15 * jax.random.normal(key_of[13], (D,), jnp.float32), 0.25, 1.75).astype(jnp.bfloat16),
        "attention_gain_out": jnp.clip(1.0 + 0.15 * jax.random.normal(key_of[14], (D,), jnp.float32), 0.25, 1.75).astype(jnp.bfloat16),
        "feedforward_gain_in": jnp.clip(1.0 + 0.15 * jax.random.normal(key_of[15], (D,), jnp.float32), 0.25, 1.75).astype(jnp.bfloat16),
        "feedforward_gain_out": jnp.clip(1.0 + 0.15 * jax.random.normal(key_of[16], (D,), jnp.float32), 0.25, 1.75).astype(jnp.bfloat16),
        "layer_cotangent": normal_values(key_of[17], (TOKENS, D), 1.0, 6.0, ((0, 32),)),
    }


@jax.custom_vjp
def low(v):
    return lax.optimization_barrier(v.astype(jnp.bfloat16)).astype(jnp.float32)

@jax.custom_vjp
def low_back(v):
    return v

def low_keep(v):
    return (low(v), None)

def low_pass(kept, grad):
    return (grad,)

def back_keep(v):
    return (v, None)

def back_low(kept, grad):
    return (low(grad),)
low.defvjp(low_keep, low_pass)
low_back.defvjp(back_keep, back_low)
highest_precision = lax.Precision.HIGHEST
norm_epsilon = 1e-05

def normalize(values):
    centered = values - lax.optimization_barrier(jnp.mean(values, axis=-1, keepdims=True))
    return centered * lax.rsqrt(lax.optimization_barrier(jnp.mean(centered * centered, axis=-1, keepdims=True)) + norm_epsilon)

def rotation(positions, head_dim):
    half_dim = head_dim // 2
    freqs = 10000.0 ** (-jnp.arange(half_dim, dtype=jnp.float32) / half_dim)
    angles = positions.astype(jnp.float32)[:, None] * freqs[None, :]
    return (jnp.cos(angles)[:, None, :], jnp.sin(angles)[:, None, :])

def rotate(tensor, cosines, sines, sign):
    half_dim = tensor.shape[-1] // 2
    first = tensor[..., :half_dim]
    second = tensor[..., half_dim:]
    return jnp.concatenate([first * cosines - sign * second * sines, second * cosines + sign * first * sines], axis=-1)

def sequence_forward(rows_in, params):
    query_weight, query_bias, key_weight, key_bias, value_weight, value_bias, output_weight, output_bias, up_weight, up_bias, down_weight, down_bias, gain_attend_in, gain_attend_out, gain_feed_in, gain_feed_out = params
    positions = jnp.arange(SEQ, dtype=jnp.int32)
    cosines, sines = rotation(positions, HEAD_DIM)
    hidden_a = low(normalize(rows_in) * gain_attend_in)

    def project(matrix, shift):
        return jnp.dot(hidden_a, matrix, precision=highest_precision) + shift
    queries = low(rotate(low_back(project(query_weight, query_bias)).reshape(SEQ, HEADS, HEAD_DIM), cosines, sines, 1.0))
    key_rows = low(rotate(low_back(project(key_weight, key_bias)).reshape(SEQ, HEADS, HEAD_DIM), cosines, sines, 1.0))
    value_rows = low(low_back(project(value_weight, value_bias))).reshape(SEQ, HEADS, HEAD_DIM)
    block = min(512, SEQ)
    factor = HEAD_DIM ** (-0.5)

    def attend(query_block, first):
        scores = low_back(jnp.einsum('qhd,khd->hqk', query_block, key_rows, precision=highest_precision) * factor)
        query_pos = first + jnp.arange(block, dtype=jnp.int32)
        allowed = positions[None, None, :] <= query_pos[None, :, None]
        masked = jnp.where(allowed, scores, -1e+30)
        shifted = masked - lax.optimization_barrier(jnp.max(masked, axis=-1, keepdims=True))
        exps = jnp.exp(shifted)
        probs = low(exps / lax.optimization_barrier(jnp.sum(exps, axis=-1, keepdims=True)))
        return jnp.einsum('hqk,khd->qhd', probs, value_rows, precision=highest_precision)
    checked = jax.checkpoint(attend)

    def attend_pair(pair_args):
        return checked(pair_args[0], pair_args[1])
    starts = (jnp.arange(SEQ // block, dtype=jnp.int32) * block).astype(jnp.int32)
    mixed = lax.map(attend_pair, (queries.reshape(SEQ // block, block, HEADS, HEAD_DIM), starts))
    attended = low(low_back(mixed.reshape(SEQ, D)))
    branch_a = low_back(jnp.dot(attended, output_weight, precision=highest_precision) + output_bias)
    middle = rows_in + normalize(branch_a) * gain_attend_out
    hidden_f = low(normalize(middle) * gain_feed_in)
    pre_act = low_back(jnp.dot(hidden_f, up_weight, precision=highest_precision) + up_bias)
    activated = low(jax.nn.gelu(pre_act))
    branch_f = low_back(jnp.dot(activated, down_weight, precision=highest_precision) + down_bias)
    return middle + normalize(branch_f) * gain_feed_out

def reference(layer_input, query_weight, query_bias, key_weight, key_bias, value_weight, value_bias, output_weight, output_bias, up_weight, up_bias, down_weight, down_bias, attention_gain_in, attention_gain_out, feedforward_gain_in, feedforward_gain_out, layer_cotangent):
    params = tuple((item.astype(jnp.float32) for item in (query_weight, query_bias, key_weight, key_bias, value_weight, value_bias, output_weight, output_bias, up_weight, up_bias, down_weight, down_bias, attention_gain_in, attention_gain_out, feedforward_gain_in, feedforward_gain_out)))

    def whole(inputs, weights):

        def single(rows_in):
            return sequence_forward(rows_in, weights)
        outputs = lax.map(single, inputs.reshape(SEQS, SEQ, D))
        return outputs.reshape(TOKENS, D)
    result, pull = jax.vjp(whole, layer_input.astype(jnp.float32), params)
    input_gradient, grads = pull(layer_cotangent.astype(jnp.float32))
    return (result.astype(jnp.bfloat16), input_gradient, grads[0], grads[1], grads[2], grads[3], grads[4], grads[5], grads[6], grads[7], grads[8], grads[9], grads[10], grads[11], grads[12], grads[13], grads[14], grads[15])
```

```python
import functools
import math

import jax
import jax.numpy as jnp
import numpy as np
from jax import lax
from jax.experimental import pallas as pl
from jax.experimental.pallas import tpu as pltpu
from jax.sharding import PartitionSpec as P

HEADS = 16


norm_epsilon = 1e-05


def normalize(values):
    centered = values - jnp.mean(values, axis=-1, keepdims=True)
    inverse = lax.rsqrt(jnp.mean(centered * centered, axis=-1, keepdims=True) + norm_epsilon)
    return (centered * inverse, inverse)


def norm_back(normed, inverse, upstream):
    return inverse * (
        upstream
        - jnp.mean(upstream, axis=-1, keepdims=True)
        - normed * jnp.mean(upstream * normed, axis=-1, keepdims=True)
    )


def rotation(positions, head_dim):
    half_dim = head_dim // 2
    freqs = 10000.0 ** (-jnp.arange(half_dim, dtype=jnp.float32) / half_dim)
    angles = positions.astype(jnp.float32)[:, None] * freqs[None, :]
    return (jnp.cos(angles)[:, None, :], jnp.sin(angles)[:, None, :])


def rotate(tensor, cosines, sines, sign):
    half_dim = tensor.shape[-1] // 2
    first = tensor[..., :half_dim]
    second = tensor[..., half_dim:]
    return jnp.concatenate(
        [first * cosines - sign * second * sines, second * cosines + sign * first * sines], axis=-1
    )


def col_sum(values):
    return jnp.sum(values.astype(jnp.float32), axis=0)


def general_device(
    layer_input,
    query_weight,
    query_bias,
    key_weight,
    key_bias,
    value_weight,
    value_bias,
    output_weight,
    output_bias,
    up_weight,
    up_bias,
    down_weight,
    down_bias,
    attention_gain_in,
    attention_gain_out,
    feedforward_gain_in,
    feedforward_gain_out,
    layer_cotangent,
):
    rows = layer_input.shape[0]
    width = layer_input.shape[1]
    heads = HEADS
    head_dim = width // heads
    seq_rows = rows * lax.axis_size("shard")
    factor = head_dim ** (-0.5)
    positions = lax.axis_index("shard") * rows + jnp.arange(rows, dtype=jnp.int32)
    cosines, sines = rotation(positions, head_dim)
    attention_local = (
        query_weight,
        key_weight,
        value_weight,
        output_weight,
        query_bias,
        key_bias,
        value_bias,
        output_bias,
        attention_gain_in,
        attention_gain_out,
    )
    feed_local = (
        up_weight,
        up_bias,
        down_weight,
        down_bias,
        feedforward_gain_in,
        feedforward_gain_out,
    )
    attention_full = (
        lax.all_gather(attention_local[0], "shard", axis=0, tiled=True),
        lax.all_gather(attention_local[1], "shard", axis=0, tiled=True),
        lax.all_gather(attention_local[2], "shard", axis=0, tiled=True),
        lax.all_gather(attention_local[3], "shard", axis=0, tiled=True),
        lax.all_gather(attention_local[4], "shard", axis=0, tiled=True),
        lax.all_gather(attention_local[5], "shard", axis=0, tiled=True),
        lax.all_gather(attention_local[6], "shard", axis=0, tiled=True),
        lax.all_gather(attention_local[7], "shard", axis=0, tiled=True),
        lax.all_gather(attention_local[8], "shard", axis=0, tiled=True),
        lax.all_gather(attention_local[9], "shard", axis=0, tiled=True),
    )
    (
        query_mat,
        key_mat,
        value_mat,
        out_mat,
        query_shift,
        key_shift,
        value_shift,
        out_shift,
        gain_in_a,
        gain_out_a,
    ) = attention_full
    residual_in = layer_input.astype(jnp.float32)
    normed_a, inverse_a = normalize(residual_in)
    hidden_a = (normed_a * gain_in_a.astype(jnp.float32)).astype(jnp.bfloat16)

    def project(matrix, shift):
        return jnp.dot(hidden_a, matrix, preferred_element_type=jnp.float32) + shift.astype(
            jnp.float32
        )

    query_heads = rotate(
        project(query_mat, query_shift).reshape(rows, heads, head_dim), cosines, sines, 1.0
    ).astype(jnp.bfloat16)
    key_rows = (
        rotate(project(key_mat, key_shift).reshape(rows, heads, head_dim), cosines, sines, 1.0)
        .astype(jnp.bfloat16)
        .reshape(rows, width)
    )
    value_rows = project(value_mat, value_shift).astype(jnp.bfloat16)
    start_state = (
        jnp.full((heads, rows), -1e30, jnp.float32),
        jnp.zeros((heads, rows), jnp.float32),
        jnp.zeros((heads, rows, head_dim), jnp.float32),
    )
    key_piece = lax.all_gather(key_rows, "shard", axis=0, tiled=True)
    value_piece = lax.all_gather(value_rows, "shard", axis=0, tiled=True)
    count = key_piece.shape[0]
    block = math.gcd(count, 512)

    def forward_inner(index, state):
        best, total, accum = state
        offset = index * block
        key_block = lax.dynamic_slice_in_dim(key_piece, offset, block, 0).reshape(
            block, heads, head_dim
        )
        value_block = lax.dynamic_slice_in_dim(value_piece, offset, block, 0).reshape(
            block, heads, head_dim
        )
        key_pos = offset + jnp.arange(block, dtype=jnp.int32)
        allowed = key_pos[None, None, :] <= positions[None, :, None]
        scores = (
            jnp.einsum("qhd,khd->hqk", query_heads, key_block, preferred_element_type=jnp.float32)
            * factor
        )
        scores = jnp.where(allowed, scores, -1e30)
        newest = jnp.maximum(best, jnp.max(scores, axis=-1))
        weights = jnp.where(allowed, jnp.exp(scores - newest[..., None]), 0.0)
        decay = jnp.exp(best - newest)
        total = total * decay + jnp.sum(weights, axis=-1)
        accum = accum * decay[..., None] + jnp.einsum(
            "hqk,khd->hqd",
            weights.astype(jnp.bfloat16),
            value_block,
            preferred_element_type=jnp.float32,
        )
        return (newest, total, accum)

    best, total, accum = lax.fori_loop(0, count // block, forward_inner, start_state)
    logsum = best + jnp.log(total)
    attended = (
        jnp.transpose(accum / total[..., None], (1, 0, 2)).reshape(rows, width).astype(jnp.bfloat16)
    )
    branch_a = jnp.dot(attended, out_mat, preferred_element_type=jnp.float32) + out_shift.astype(
        jnp.float32
    )
    normed_o, inverse_o = normalize(branch_a)
    middle = residual_in + normed_o * gain_out_a.astype(jnp.float32)
    feed_full = (
        lax.all_gather(feed_local[0], "shard", axis=0, tiled=True),
        lax.all_gather(feed_local[1], "shard", axis=0, tiled=True),
        lax.all_gather(feed_local[2], "shard", axis=0, tiled=True),
        lax.all_gather(feed_local[3], "shard", axis=0, tiled=True),
        lax.all_gather(feed_local[4], "shard", axis=0, tiled=True),
        lax.all_gather(feed_local[5], "shard", axis=0, tiled=True),
    )
    up_mat, up_shift, down_mat, down_shift, gain_in_f, gain_out_f = feed_full
    normed_f, inverse_f = normalize(middle)
    hidden_f = (normed_f * gain_in_f.astype(jnp.float32)).astype(jnp.bfloat16)
    pre_act = jnp.dot(hidden_f, up_mat, preferred_element_type=jnp.float32) + up_shift.astype(
        jnp.float32
    )
    activated = jax.nn.gelu(pre_act).astype(jnp.bfloat16)
    branch_f = jnp.dot(activated, down_mat, preferred_element_type=jnp.float32) + down_shift.astype(
        jnp.float32
    )
    normed_d, inverse_d = normalize(branch_f)
    layer_output = (middle + normed_d * gain_out_f.astype(jnp.float32)).astype(jnp.bfloat16)
    feed_back = (
        lax.all_gather(feed_local[0], "shard", axis=0, tiled=True),
        lax.all_gather(feed_local[1], "shard", axis=0, tiled=True),
        lax.all_gather(feed_local[2], "shard", axis=0, tiled=True),
        lax.all_gather(feed_local[3], "shard", axis=0, tiled=True),
        lax.all_gather(feed_local[4], "shard", axis=0, tiled=True),
        lax.all_gather(feed_local[5], "shard", axis=0, tiled=True),
    )
    up_back, up_unused, down_back, down_unused, gain_in_fb, gain_out_fb = feed_back
    upstream = layer_cotangent.astype(jnp.float32)
    grad_gain_out_f = jnp.sum(upstream * normed_d, axis=0)
    d_branch_f = norm_back(normed_d, inverse_d, upstream * gain_out_fb.astype(jnp.float32)).astype(
        jnp.bfloat16
    )
    grad_down = jnp.einsum("tf,td->fd", activated, d_branch_f, preferred_element_type=jnp.float32)
    grad_down_shift = col_sum(d_branch_f)
    d_activated = jnp.einsum("td,fd->tf", d_branch_f, down_back, preferred_element_type=jnp.float32)
    gelu_out, gelu_pull = jax.vjp(jax.nn.gelu, pre_act)
    d_pre = gelu_pull(d_activated)[0].astype(jnp.bfloat16)
    grad_up = jnp.einsum("td,tf->df", hidden_f, d_pre, preferred_element_type=jnp.float32)
    grad_up_shift = col_sum(d_pre)
    d_hidden_f = jnp.einsum("tf,df->td", d_pre, up_back, preferred_element_type=jnp.float32)
    grad_gain_in_f = jnp.sum(d_hidden_f * normed_f, axis=0)
    d_middle = upstream + norm_back(
        normed_f, inverse_f, d_hidden_f * gain_in_fb.astype(jnp.float32)
    )
    feed_grads = (
        lax.psum_scatter(
            grad_up.astype(jnp.bfloat16), "shard", scatter_dimension=0, tiled=True
        ).astype(jnp.float32),
        lax.psum_scatter(
            grad_up_shift.astype(jnp.bfloat16), "shard", scatter_dimension=0, tiled=True
        ).astype(jnp.float32),
        lax.psum_scatter(
            grad_down.astype(jnp.bfloat16), "shard", scatter_dimension=0, tiled=True
        ).astype(jnp.float32),
        lax.psum_scatter(
            grad_down_shift.astype(jnp.bfloat16), "shard", scatter_dimension=0, tiled=True
        ).astype(jnp.float32),
        lax.psum_scatter(
            grad_gain_in_f.astype(jnp.bfloat16), "shard", scatter_dimension=0, tiled=True
        ).astype(jnp.float32),
        lax.psum_scatter(
            grad_gain_out_f.astype(jnp.bfloat16), "shard", scatter_dimension=0, tiled=True
        ).astype(jnp.float32),
    )
    attention_back = (
        lax.all_gather(attention_local[0], "shard", axis=0, tiled=True),
        lax.all_gather(attention_local[1], "shard", axis=0, tiled=True),
        lax.all_gather(attention_local[2], "shard", axis=0, tiled=True),
        lax.all_gather(attention_local[3], "shard", axis=0, tiled=True),
        lax.all_gather(attention_local[4], "shard", axis=0, tiled=True),
        lax.all_gather(attention_local[5], "shard", axis=0, tiled=True),
        lax.all_gather(attention_local[6], "shard", axis=0, tiled=True),
        lax.all_gather(attention_local[7], "shard", axis=0, tiled=True),
        lax.all_gather(attention_local[8], "shard", axis=0, tiled=True),
        lax.all_gather(attention_local[9], "shard", axis=0, tiled=True),
    )
    (
        query_back,
        key_back,
        value_back,
        out_back,
        qshift_unused,
        kshift_unused,
        vshift_unused,
        oshift_unused,
        gain_in_ab,
        gain_out_ab,
    ) = attention_back
    grad_gain_out_a = jnp.sum(d_middle * normed_o, axis=0)
    d_branch_a = norm_back(normed_o, inverse_o, d_middle * gain_out_ab.astype(jnp.float32)).astype(
        jnp.bfloat16
    )
    grad_out_mat = jnp.einsum("td,te->de", attended, d_branch_a, preferred_element_type=jnp.float32)
    grad_out_shift = col_sum(d_branch_a)
    d_attended = jnp.einsum(
        "te,de->td", d_branch_a, out_back, preferred_element_type=jnp.float32
    ).astype(jnp.bfloat16)
    d_heads = d_attended.reshape(rows, heads, head_dim)
    row_delta = jnp.einsum(
        "qhd,qhd->hq",
        d_heads.astype(jnp.float32),
        attended.reshape(rows, heads, head_dim).astype(jnp.float32),
    )

    def query_terms(key_block, value_block, key_pos):
        allowed = key_pos[None, None, :] <= positions[None, :, None]
        scores = (
            jnp.einsum("qhd,khd->hqk", query_heads, key_block, preferred_element_type=jnp.float32)
            * factor
        )
        probs = jnp.where(allowed, jnp.exp(scores - logsum[..., None]), 0.0)
        d_probs = jnp.einsum(
            "qhd,khd->hqk", d_heads, value_block, preferred_element_type=jnp.float32
        )
        d_scores = (probs * (d_probs - row_delta[..., None])).astype(jnp.bfloat16)
        return (probs, d_scores)

    back_state = (
        jnp.zeros((rows, heads, head_dim), jnp.float32),
        jnp.zeros((seq_rows, width), jnp.float32),
        jnp.zeros((seq_rows, width), jnp.float32),
    )
    backward_key_piece = lax.all_gather(key_rows, "shard", axis=0, tiled=True)
    backward_value_piece = lax.all_gather(value_rows, "shard", axis=0, tiled=True)
    count = backward_key_piece.shape[0]
    backward_block = math.gcd(count, 512)

    def backward_inner(index, state):
        grad_query, grad_keys, grad_values = state
        offset = index * backward_block
        key_block = lax.dynamic_slice_in_dim(backward_key_piece, offset, backward_block, 0).reshape(
            backward_block, heads, head_dim
        )
        value_block = lax.dynamic_slice_in_dim(
            backward_value_piece, offset, backward_block, 0
        ).reshape(backward_block, heads, head_dim)
        key_pos = offset + jnp.arange(backward_block, dtype=jnp.int32)
        probs, d_scores = query_terms(key_block, value_block, key_pos)
        grad_query = (
            grad_query
            + jnp.einsum("hqk,khd->qhd", d_scores, key_block, preferred_element_type=jnp.float32)
            * factor
        )
        key_grad = (
            jnp.einsum("hqk,qhd->khd", d_scores, query_heads, preferred_element_type=jnp.float32)
            * factor
        )
        value_grad = jnp.einsum(
            "hqk,qhd->khd", probs.astype(jnp.bfloat16), d_heads, preferred_element_type=jnp.float32
        )
        grad_keys = lax.dynamic_update_slice_in_dim(
            grad_keys, key_grad.reshape(backward_block, width), offset, 0
        )
        grad_values = lax.dynamic_update_slice_in_dim(
            grad_values, value_grad.reshape(backward_block, width), offset, 0
        )
        return (grad_query, grad_keys, grad_values)

    back_result = lax.fori_loop(0, count // backward_block, backward_inner, back_state)
    grad_query = back_result[0]
    key_total, value_total = (
        lax.psum_scatter(
            back_result[1].astype(jnp.bfloat16), "shard", scatter_dimension=0, tiled=True
        ).astype(jnp.float32),
        lax.psum_scatter(
            back_result[2].astype(jnp.bfloat16), "shard", scatter_dimension=0, tiled=True
        ).astype(jnp.float32),
    )
    d_query = rotate(grad_query, cosines, sines, -1.0).reshape(rows, width).astype(jnp.bfloat16)
    d_key = (
        rotate(key_total.reshape(rows, heads, head_dim), cosines, sines, -1.0)
        .reshape(rows, width)
        .astype(jnp.bfloat16)
    )
    d_value = value_total.astype(jnp.bfloat16)
    grad_query_mat = jnp.einsum("td,te->de", hidden_a, d_query, preferred_element_type=jnp.float32)
    grad_key_mat = jnp.einsum("td,te->de", hidden_a, d_key, preferred_element_type=jnp.float32)
    grad_value_mat = jnp.einsum("td,te->de", hidden_a, d_value, preferred_element_type=jnp.float32)
    d_hidden_a = jnp.einsum("te,de->td", d_query, query_back, preferred_element_type=jnp.float32)
    d_hidden_a = d_hidden_a + jnp.einsum(
        "te,de->td", d_key, key_back, preferred_element_type=jnp.float32
    )
    d_hidden_a = d_hidden_a + jnp.einsum(
        "te,de->td", d_value, value_back, preferred_element_type=jnp.float32
    )
    grad_gain_in_a = jnp.sum(d_hidden_a * normed_a, axis=0)
    input_gradient = d_middle + norm_back(
        normed_a, inverse_a, d_hidden_a * gain_in_ab.astype(jnp.float32)
    )
    attention_grads = (
        lax.psum_scatter(
            grad_query_mat.astype(jnp.bfloat16), "shard", scatter_dimension=0, tiled=True
        ).astype(jnp.float32),
        lax.psum_scatter(
            grad_key_mat.astype(jnp.bfloat16), "shard", scatter_dimension=0, tiled=True
        ).astype(jnp.float32),
        lax.psum_scatter(
            grad_value_mat.astype(jnp.bfloat16), "shard", scatter_dimension=0, tiled=True
        ).astype(jnp.float32),
        lax.psum_scatter(
            grad_out_mat.astype(jnp.bfloat16), "shard", scatter_dimension=0, tiled=True
        ).astype(jnp.float32),
        lax.psum_scatter(
            col_sum(d_query).astype(jnp.bfloat16), "shard", scatter_dimension=0, tiled=True
        ).astype(jnp.float32),
        lax.psum_scatter(
            col_sum(d_key).astype(jnp.bfloat16), "shard", scatter_dimension=0, tiled=True
        ).astype(jnp.float32),
        lax.psum_scatter(
            col_sum(d_value).astype(jnp.bfloat16), "shard", scatter_dimension=0, tiled=True
        ).astype(jnp.float32),
        lax.psum_scatter(
            grad_out_shift.astype(jnp.bfloat16), "shard", scatter_dimension=0, tiled=True
        ).astype(jnp.float32),
        lax.psum_scatter(
            grad_gain_in_a.astype(jnp.bfloat16), "shard", scatter_dimension=0, tiled=True
        ).astype(jnp.float32),
        lax.psum_scatter(
            grad_gain_out_a.astype(jnp.bfloat16), "shard", scatter_dimension=0, tiled=True
        ).astype(jnp.float32),
    )
    (
        g_query,
        g_key,
        g_value,
        g_out,
        g_qshift,
        g_kshift,
        g_vshift,
        g_oshift,
        g_gain_in_a,
        g_gain_out_a,
    ) = attention_grads
    g_up, g_up_shift, g_down, g_down_shift, g_gain_in_f, g_gain_out_f = feed_grads
    summed = (
        lax.psum(g_query.astype(jnp.bfloat16), "rep").astype(jnp.float32),
        lax.psum(g_qshift.astype(jnp.bfloat16), "rep").astype(jnp.float32),
        lax.psum(g_key.astype(jnp.bfloat16), "rep").astype(jnp.float32),
        lax.psum(g_kshift.astype(jnp.bfloat16), "rep").astype(jnp.float32),
        lax.psum(g_value.astype(jnp.bfloat16), "rep").astype(jnp.float32),
        lax.psum(g_vshift.astype(jnp.bfloat16), "rep").astype(jnp.float32),
        lax.psum(g_out.astype(jnp.bfloat16), "rep").astype(jnp.float32),
        lax.psum(g_oshift.astype(jnp.bfloat16), "rep").astype(jnp.float32),
        lax.psum(g_up.astype(jnp.bfloat16), "rep").astype(jnp.float32),
        lax.psum(g_up_shift.astype(jnp.bfloat16), "rep").astype(jnp.float32),
        lax.psum(g_down.astype(jnp.bfloat16), "rep").astype(jnp.float32),
        lax.psum(g_down_shift.astype(jnp.bfloat16), "rep").astype(jnp.float32),
        lax.psum(g_gain_in_a.astype(jnp.bfloat16), "rep").astype(jnp.float32),
        lax.psum(g_gain_out_a.astype(jnp.bfloat16), "rep").astype(jnp.float32),
        lax.psum(g_gain_in_f.astype(jnp.bfloat16), "rep").astype(jnp.float32),
        lax.psum(g_gain_out_f.astype(jnp.bfloat16), "rep").astype(jnp.float32),
    )
    return (
        layer_output,
        input_gradient,
        summed[0],
        summed[1],
        summed[2],
        summed[3],
        summed[4],
        summed[5],
        summed[6],
        summed[7],
        summed[8],
        summed[9],
        summed[10],
        summed[11],
        summed[12],
        summed[13],
        summed[14],
        summed[15],
    )


def swap(values, bit):
    count = lax.axis_size("rep")
    return lax.ppermute(values, "rep", [(i, i ^ bit) for i in range(count)])


def shift(values, step):
    count = lax.axis_size("shard")
    return lax.ppermute(values, "shard", [(i, (i + step) % count) for i in range(count)])


def token_pairs(count):
    pairs = []
    for rep in range(count):
        for z in range(4):
            there = (rep & ~3) | ((z & 1) << 1) | (z >> 1)
            pairs.append((rep * 4 + z, there * 4 + (rep & 3)))
    return pairs


def by_bit(bit, own, other):
    return jnp.where(bit == 0, jnp.stack([own, other]), jnp.stack([other, own]))


def pick(values, index, size, axis=0):
    return lax.dynamic_slice_in_dim(values, index * size, size, axis)


def gather_shards(piece, place):
    out = jnp.zeros((4,) + piece.shape, piece.dtype)
    out = lax.dynamic_update_index_in_dim(out, piece, place, 0)
    for step in (1, 2, 3):
        out = lax.dynamic_update_index_in_dim(out, shift(piece, step), (place + 4 - step) % 4, 0)
    return out


def rope_tables(tokens, head_dim):
    half = head_dim // 2
    freqs = 10000.0 ** (-np.arange(half, dtype=np.float64) / half)
    angles = np.arange(tokens, dtype=np.float64)[:, None] * freqs[None, :]
    cosines = np.tile(np.cos(angles), (1, 4)).astype(np.float32)
    sines = np.tile(np.concatenate([-np.sin(angles), np.sin(angles)], 1), (1, 2)).astype(np.float32)
    return jnp.asarray(cosines), jnp.asarray(sines)


def turn(values, cosines, sines):
    lane = lax.broadcasted_iota(jnp.int32, values.shape, 1)
    swapped = jnp.where(
        lane % 64 < 32, pltpu.roll(values, 96, 1), pltpu.roll(values, 32, 1)
    )
    return values * cosines + swapped * sines


def nt(left, right):
    return lax.dot_general(left, right, (((1,), (1,)), ((), ())), preferred_element_type=jnp.float32)


def tn(left, right):
    return lax.dot_general(left, right, (((0,), (0,)), ((), ())), preferred_element_type=jnp.float32)


BLOCK = 256


def head_lanes(shape, parity):
    lane = lax.broadcasted_iota(jnp.int32, shape, 1)
    return (lane // 64) == parity


def attend_kernel(hidden, weights, shifts, cosines, sines, query, key, value, mixed, logs):
    tokens = hidden.shape[0]
    blocks = tokens // BLOCK
    width = 256

    def project(index, carry):
        rows = pl.ds(pl.multiple_of(index * BLOCK, BLOCK), BLOCK)
        raw = jnp.dot(hidden[rows, :], weights[...], preferred_element_type=jnp.float32) + shifts[...]
        cos, sin = cosines[rows, :], sines[rows, :]
        for tile in range(width // 128):
            lanes = slice(tile * 128, tile * 128 + 128)
            query[rows, lanes] = (
                turn(raw[:, lanes], cos, sin).astype(jnp.bfloat16) * jnp.bfloat16(0.125)
            )
            key[rows, lanes] = turn(raw[:, width:][:, lanes], cos, sin).astype(jnp.bfloat16)
        value[rows, :] = raw[:, 2 * width :].astype(jnp.bfloat16)
        return carry

    lax.fori_loop(0, blocks, project, 0)
    causal = lax.broadcasted_iota(jnp.int32, (BLOCK, BLOCK), 0) >= lax.broadcasted_iota(
        jnp.int32, (BLOCK, BLOCK), 1
    )
    logs[...] = jnp.zeros_like(logs)

    def pair_step(pair, carry):
        lanes = pl.ds(pl.multiple_of(pair * 128, 128), 128)
        lane = lax.broadcasted_iota(jnp.int32, (BLOCK, 128), 1)
        for block in range(blocks):
            rows = slice(block * BLOCK, block * BLOCK + BLOCK)
            seen = (block + 1) * BLOCK
            queries = query[rows, lanes]
            keys, values = key[:seen, lanes], value[:seen, lanes]
            outs = []
            log_rows = logs[rows, :]
            for parity in range(2):
                masked = jnp.where(head_lanes(queries.shape, parity), queries, jnp.bfloat16(0))
                scores = nt(masked, keys)
                last = jnp.where(causal, scores[:, seen - BLOCK :], -1e30)
                if block:
                    scores = jnp.concatenate([scores[:, : seen - BLOCK], last], 1)
                else:
                    scores = last
                best = jnp.max(scores, axis=1, keepdims=True)
                exps = jnp.exp(scores - best)
                total = jnp.sum(exps, axis=1, keepdims=True)
                out = jnp.dot(exps.astype(jnp.bfloat16), values, preferred_element_type=jnp.float32)
                outs.append(out / total)
                log_rows = jnp.where(lane == pair * 2 + parity, best + jnp.log(total), log_rows)
            mixed[rows, lanes] = jnp.where(lane < 64, outs[0], outs[1]).astype(jnp.bfloat16)
            logs[rows, :] = log_rows
        return carry

    lax.fori_loop(0, 2, pair_step, 0)


def attend(hidden, weights, shifts, cosines, sines):
    tokens = hidden.shape[0]
    shaped = lambda width, kind: jax.ShapeDtypeStruct((tokens, width), kind)
    return pl.pallas_call(
        attend_kernel,
        out_shape=(
            shaped(256, jnp.bfloat16),
            shaped(256, jnp.bfloat16),
            shaped(256, jnp.bfloat16),
            shaped(256, jnp.bfloat16),
            shaped(128, jnp.float32),
        ),
        in_specs=[pl.BlockSpec(memory_space=pltpu.VMEM)] * 5,
        out_specs=[pl.BlockSpec(memory_space=pltpu.VMEM)] * 5,
        compiler_params=pltpu.CompilerParams(vmem_limit_bytes=48 << 20),
        cost_estimate=pl.CostEstimate(
            flops=2 * tokens * 1024 * 768 + 16 * tokens * tokens * 64,
            bytes_accessed=8 << 20,
            transcendentals=4 * tokens * tokens,
        ),
        name="attend",
    )(hidden, weights, shifts, cosines, sines)


def attend_back_kernel(
    upstream, out_rows, query, key, value, mixed, logs, cosines, sines, grads, d_out, d_key, d_value, d_query
):
    tokens = upstream.shape[0]
    blocks = tokens // BLOCK
    width = 256

    def project(index, carry):
        rows = pl.ds(pl.multiple_of(index * BLOCK, BLOCK), BLOCK)
        d_out[rows, :] = nt(upstream[rows, :], out_rows[...]).astype(jnp.bfloat16)
        return carry

    lax.fori_loop(0, blocks, project, 0)
    d_key[...] = jnp.zeros_like(d_key)
    d_value[...] = jnp.zeros_like(d_value)
    d_query[...] = jnp.zeros_like(d_query)
    causal = lax.broadcasted_iota(jnp.int32, (BLOCK, BLOCK), 0) >= lax.broadcasted_iota(
        jnp.int32, (BLOCK, BLOCK), 1
    )

    def pair_step(pair, carry):
        lanes = pl.ds(pl.multiple_of(pair * 128, 128), 128)
        for block in range(blocks):
            rows = slice(block * BLOCK, block * BLOCK + BLOCK)
            seen = (block + 1) * BLOCK
            queries, d_outs = query[rows, lanes], d_out[rows, lanes]
            keys, values = key[:seen, lanes], value[:seen, lanes]
            products = d_outs.astype(jnp.float32) * mixed[rows, lanes].astype(jnp.float32)
            log_rows = logs[rows, :]
            lane = lax.broadcasted_iota(jnp.int32, (BLOCK, 128), 1)
            for parity in range(2):
                mine = head_lanes((BLOCK, 128), parity)
                masked_q = jnp.where(mine, queries, jnp.bfloat16(0))
                masked_d = jnp.where(mine, d_outs, jnp.bfloat16(0))
                log = jnp.sum(jnp.where(lane == pair * 2 + parity, log_rows, 0.0), 1, keepdims=True)
                delta = jnp.sum(jnp.where(mine, products, 0.0), 1, keepdims=True)
                scores = nt(masked_q, keys)
                probs = jnp.exp(scores - log)
                last = jnp.where(causal, probs[:, seen - BLOCK :], 0.0)
                if block:
                    probs = jnp.concatenate([probs[:, : seen - BLOCK], last], 1)
                else:
                    probs = last
                d_probs = nt(masked_d, values)
                d_scores = (probs * (d_probs - delta)).astype(jnp.bfloat16)
                probs = probs.astype(jnp.bfloat16)
                d_query[rows, lanes] += jnp.where(
                    mine, jnp.dot(d_scores, keys, preferred_element_type=jnp.float32), 0.0
                )
                d_value[:seen, lanes] += tn(probs, masked_d)
                d_key[:seen, lanes] += tn(d_scores, masked_q)
        return carry

    lax.fori_loop(0, 2, pair_step, 0)

    def finish(index, carry):
        rows = pl.ds(pl.multiple_of(index * BLOCK, BLOCK), BLOCK)
        cos, sin = cosines[rows, :], -sines[rows, :]
        for tile in range(width // 128):
            lanes = slice(tile * 128, tile * 128 + 128)
            at = tile * 128
            grads[rows, at : at + 128] = turn(d_query[rows, lanes] * 0.125, cos, sin).astype(jnp.bfloat16)
            at += width
            grads[rows, at : at + 128] = turn(d_key[rows, lanes], cos, sin).astype(jnp.bfloat16)
        grads[rows, 2 * width :] = d_value[rows, :].astype(jnp.bfloat16)
        return carry

    lax.fori_loop(0, blocks, finish, 0)


def attend_back(upstream, out_rows, query, key, value, mixed, logs, cosines, sines):
    tokens = upstream.shape[0]
    return pl.pallas_call(
        attend_back_kernel,
        out_shape=jax.ShapeDtypeStruct((tokens, 768), jnp.bfloat16),
        in_specs=[pl.BlockSpec(memory_space=pltpu.VMEM)] * 9,
        out_specs=pl.BlockSpec(memory_space=pltpu.VMEM),
        scratch_shapes=[
            pltpu.VMEM((tokens, 256), jnp.bfloat16),
            pltpu.VMEM((tokens, 256), jnp.float32),
            pltpu.VMEM((tokens, 256), jnp.float32),
            pltpu.VMEM((tokens, 256), jnp.float32),
        ],
        compiler_params=pltpu.CompilerParams(vmem_limit_bytes=48 << 20),
        cost_estimate=pl.CostEstimate(
            flops=2 * tokens * 1024 * 256 + 40 * tokens * tokens * 64,
            bytes_accessed=8 << 20,
            transcendentals=4 * tokens * tokens,
        ),
        name="attend_back",
    )(upstream, out_rows, query, key, value, mixed, logs, cosines, sines)


def fast_device(
    layer_input,
    query_weight,
    query_bias,
    key_weight,
    key_bias,
    value_weight,
    value_bias,
    output_weight,
    output_bias,
    up_weight,
    up_bias,
    down_weight,
    down_bias,
    attention_gain_in,
    attention_gain_out,
    feedforward_gain_in,
    feedforward_gain_out,
    layer_cotangent,
):
    f32, bf16 = jnp.float32, jnp.bfloat16
    replicas = lax.axis_size("rep")
    rows, width = layer_input.shape
    tokens = rows * 4
    rep, place = lax.axis_index("rep"), lax.axis_index("shard")
    core, x_bit, y_bit = rep & 1, (rep >> 1) & 1, rep >> 2
    quarter = rep & 3
    wide = up_weight.shape[1]
    local = wide // 4
    block = local // 4
    pairs = token_pairs(replicas)
    back_pairs = [(there, here) for here, there in pairs]
    both = ("rep", "shard")

    own_rows = lax.ppermute(layer_input, both, pairs)

    def head_columns(weight):
        return weight.reshape(rows, 4, 4, 64)[:, :, quarter, :].reshape(rows, 256)

    qkv_piece = jnp.concatenate(
        [head_columns(query_weight), head_columns(key_weight), head_columns(value_weight)], 1
    )
    small_piece = jnp.concatenate(
        [
            query_bias,
            key_bias,
            value_bias,
            output_bias,
            down_bias,
            attention_gain_in,
            attention_gain_out,
            feedforward_gain_in,
            feedforward_gain_out,
            up_bias,
        ]
    )
    small_piece = small_piece.reshape(-1, 128)
    small = gather_shards(small_piece, place).reshape(4, -1).astype(f32)
    per = width // 4

    def whole(index):
        return small[:, index * per : (index + 1) * per].reshape(width)

    def local_heads(index):
        return small[:, index * per : (index + 1) * per].reshape(4, 4, 64)[:, quarter, :].reshape(256)

    out_shift, down_shift = whole(3), whole(4)
    gain_in_a, gain_out_a, gain_in_f, gain_out_f = whole(5), whole(6), whole(7), whole(8)
    up_shift = small[:, 9 * per :].reshape(4, 4, block)[:, quarter, :].reshape(local)
    qkv_shift = jnp.concatenate([local_heads(0), local_heads(1), local_heads(2)]).reshape(1, 768)

    qkv = gather_shards(qkv_piece, place).reshape(width, 768)
    out_rows = gather_shards(pick(output_weight, quarter, 64), place).reshape(256, width)
    up_piece = jnp.concatenate([pick(up_weight, 4 * i + quarter, block, 1) for i in range(4)], 1)
    up_mat = gather_shards(up_piece, place).reshape(width, local)
    down_mat = gather_shards(pick(down_weight, quarter, block), place).reshape(local, width)

    def gather_group(values):
        mine = by_bit(x_bit, values, swap(values, 2)).reshape(2 * rows, width)
        return by_bit(core, mine, swap(mine, 1)).reshape(tokens, width)

    def scatter_group(partial):
        there = pick(partial, 1 - core, 2 * rows).astype(bf16)
        partial = pick(partial, core, 2 * rows) + swap(there, 1).astype(f32)
        there = pick(partial, 1 - x_bit, rows).astype(bf16)
        return pick(partial, x_bit, rows) + swap(there, 2).astype(f32)

    residual_in = own_rows.astype(f32)
    normed_a, inverse_a = normalize(residual_in)
    hidden_a = gather_group((normed_a * gain_in_a).astype(bf16))
    cosines, sines = rope_tables(tokens, 64)
    query, key, value, mixed, logs = attend(hidden_a, qkv, qkv_shift, cosines, sines)
    branch_a = scatter_group(jnp.dot(mixed, out_rows, preferred_element_type=f32)) + out_shift
    normed_o, inverse_o = normalize(branch_a)
    middle = residual_in + normed_o * gain_out_a
    normed_f, inverse_f = normalize(middle)
    hidden_f = gather_group((normed_f * gain_in_f).astype(bf16))
    pre_act = jnp.dot(hidden_f, up_mat, preferred_element_type=f32) + up_shift
    activated = jax.nn.gelu(pre_act).astype(bf16)
    branch_f = scatter_group(jnp.dot(activated, down_mat, preferred_element_type=f32)) + down_shift
    normed_d, inverse_d = normalize(branch_f)
    layer_output = (middle + normed_d * gain_out_f).astype(bf16)
    layer_output = lax.ppermute(layer_output, both, back_pairs)

    upstream = lax.ppermute(layer_cotangent, both, pairs).astype(f32)
    grad_gain_out_f = jnp.sum(upstream * normed_d, axis=0)
    d_branch_f = norm_back(normed_d, inverse_d, upstream * gain_out_f).astype(bf16)
    grad_down_shift = col_sum(d_branch_f)
    d_branch_f = gather_group(d_branch_f)
    grad_down = tn(activated, d_branch_f).astype(bf16)
    d_activated = nt(d_branch_f, down_mat)
    gelu_out, gelu_pull = jax.vjp(jax.nn.gelu, pre_act)
    d_pre = gelu_pull(d_activated)[0].astype(bf16)
    grad_up = tn(hidden_f, d_pre).astype(bf16)
    grad_up_shift = col_sum(d_pre)
    d_hidden_f = scatter_group(nt(d_pre, up_mat))
    grad_gain_in_f = jnp.sum(d_hidden_f * normed_f, axis=0)
    d_middle = upstream + norm_back(normed_f, inverse_f, d_hidden_f * gain_in_f)
    grad_gain_out_a = jnp.sum(d_middle * normed_o, axis=0)
    d_branch_a = norm_back(normed_o, inverse_o, d_middle * gain_out_a).astype(bf16)
    grad_out_shift = col_sum(d_branch_a)
    d_branch_a = gather_group(d_branch_a)
    grad_out = tn(mixed, d_branch_a).astype(bf16)
    d_qkv = attend_back(
        d_branch_a, out_rows, query, key, value, mixed, logs, cosines, sines
    )
    grad_qkv = tn(hidden_a, d_qkv).astype(bf16)
    grad_qkv_shift = col_sum(d_qkv)
    d_hidden_a = scatter_group(nt(d_qkv, qkv))
    grad_gain_in_a = jnp.sum(d_hidden_a * normed_a, axis=0)
    input_gradient = d_middle + norm_back(normed_a, inverse_a, d_hidden_a * gain_in_a)
    input_gradient = lax.ppermute(input_gradient.astype(bf16), both, back_pairs).astype(f32)

    def reduce_grad(grad):
        size = grad.shape[1]
        if replicas == 8:
            half = size // 2
            there = swap(pick(grad, 1 - y_bit, half, 1), 4)
            grad = (pick(grad, y_bit, half, 1).astype(f32) + there.astype(f32)).astype(bf16)
        total = lax.dynamic_index_in_dim(grad, place, 0, False).astype(f32)
        for step in (1, 2, 3):
            sent = lax.dynamic_index_in_dim(grad, (place + step) % 4, 0, False)
            total = total + shift(sent, step).astype(f32)
        total = total.astype(bf16)
        total = by_bit(x_bit, total, swap(total, 2))
        if replicas == 8:
            total = by_bit(y_bit, total, swap(total, 4))
        else:
            total = total[None]
        return by_bit(core, total, swap(total, 1))

    def by_rows(total):
        return total.transpose(2, 0, 1, 3, 4).reshape(-1, total.shape[-1]).astype(f32)

    g_down = by_rows(reduce_grad(grad_down.reshape(4, block, width)))
    g_up = reduce_grad(grad_up.reshape(4, rows, local))
    g_up = (
        g_up.reshape(2, -1, 2, g_up.shape[3], 4, block)
        .transpose(1, 3, 4, 2, 0, 5)
        .reshape(rows, wide)
        .astype(f32)
    )
    g_out = by_rows(reduce_grad(grad_out.reshape(4, 64, width)))
    g_qkv = reduce_grad(grad_qkv.reshape(4, rows, 768))
    g_qkv = (
        g_qkv.reshape(2, -1, 2, g_qkv.shape[3], 3, 4, 64)
        .transpose(4, 1, 3, 5, 2, 0, 6)
        .reshape(3, rows, width)
        .astype(f32)
    )

    def spread(values, size):
        out = jnp.zeros((4, 4, size), f32)
        return lax.dynamic_update_slice(out, values.reshape(4, 1, size), (0, quarter, 0)).reshape(4, -1)

    vectors = [spread(grad_qkv_shift[i * 256 : (i + 1) * 256], 64) for i in range(3)]
    for item in (
        grad_out_shift,
        grad_down_shift,
        grad_gain_in_a,
        grad_gain_out_a,
        grad_gain_in_f,
        grad_gain_out_f,
    ):
        vectors.append(item.reshape(4, per))
    vectors.append(spread(grad_up_shift, block))
    vector = jnp.concatenate(vectors, 1)
    vector = lax.psum(vector, both)
    vector = lax.dynamic_index_in_dim(vector, place, 0, False)

    def own(index):
        return vector[index * per : (index + 1) * per]

    return (
        layer_output,
        input_gradient,
        g_qkv[0],
        own(0),
        g_qkv[1],
        own(1),
        g_qkv[2],
        own(2),
        g_out,
        own(3),
        g_up,
        vector[9 * per :],
        g_down,
        own(4),
        own(5),
        own(6),
        own(7),
        own(8),
    )


def solution(mesh):
    replicas, shards = mesh.shape["rep"], mesh.shape["shard"]
    fits = shards == 4 and replicas in (4, 8) and HEADS % 16 == 0
    return jax.shard_map(
        fast_device if fits else general_device,
        mesh=mesh,
        in_specs=(
            P(("rep", "shard"), None),
            P("shard", None),
            P("shard"),
            P("shard", None),
            P("shard"),
            P("shard", None),
            P("shard"),
            P("shard", None),
            P("shard"),
            P("shard", None),
            P("shard"),
            P("shard", None),
            P("shard"),
            P("shard"),
            P("shard"),
            P("shard"),
            P("shard"),
            P(("rep", "shard"), None),
        ),
        out_specs=(
            P(("rep", "shard"), None),
            P(("rep", "shard"), None),
            P("shard", None),
            P("shard"),
            P("shard", None),
            P("shard"),
            P("shard", None),
            P("shard"),
            P("shard", None),
            P("shard"),
            P("shard", None),
            P("shard"),
            P("shard", None),
            P("shard"),
            P("shard"),
            P("shard"),
            P("shard"),
            P("shard"),
        ),
        check_vma=False,
    )
```

```python
import functools
import math

import jax
import jax.numpy as jnp
import numpy as np
from jax import lax
from jax.experimental import pallas as pl
from jax.experimental.pallas import tpu as pltpu
from jax.sharding import PartitionSpec as P

HEADS = 16


norm_epsilon = 1e-05


def normalize(values):
    centered = values - jnp.mean(values, axis=-1, keepdims=True)
    inverse = lax.rsqrt(jnp.mean(centered * centered, axis=-1, keepdims=True) + norm_epsilon)
    return (centered * inverse, inverse)


def norm_back(normed, inverse, upstream):
    return inverse * (
        upstream
        - jnp.mean(upstream, axis=-1, keepdims=True)
        - normed * jnp.mean(upstream * normed, axis=-1, keepdims=True)
    )


def rotation(positions, head_dim):
    half_dim = head_dim // 2
    freqs = 10000.0 ** (-jnp.arange(half_dim, dtype=jnp.float32) / half_dim)
    angles = positions.astype(jnp.float32)[:, None] * freqs[None, :]
    return (jnp.cos(angles)[:, None, :], jnp.sin(angles)[:, None, :])


def rotate(tensor, cosines, sines, sign):
    half_dim = tensor.shape[-1] // 2
    first = tensor[..., :half_dim]
    second = tensor[..., half_dim:]
    return jnp.concatenate(
        [first * cosines - sign * second * sines, second * cosines + sign * first * sines], axis=-1
    )


def col_sum(values):
    return jnp.sum(values.astype(jnp.float32), axis=0)


def general_device(
    layer_input,
    query_weight,
    query_bias,
    key_weight,
    key_bias,
    value_weight,
    value_bias,
    output_weight,
    output_bias,
    up_weight,
    up_bias,
    down_weight,
    down_bias,
    attention_gain_in,
    attention_gain_out,
    feedforward_gain_in,
    feedforward_gain_out,
    layer_cotangent,
):
    rows = layer_input.shape[0]
    width = layer_input.shape[1]
    heads = HEADS
    head_dim = width // heads
    seq_rows = rows * lax.axis_size("shard")
    factor = head_dim ** (-0.5)
    positions = lax.axis_index("shard") * rows + jnp.arange(rows, dtype=jnp.int32)
    cosines, sines = rotation(positions, head_dim)
    attention_local = (
        query_weight,
        key_weight,
        value_weight,
        output_weight,
        query_bias,
        key_bias,
        value_bias,
        output_bias,
        attention_gain_in,
        attention_gain_out,
    )
    feed_local = (
        up_weight,
        up_bias,
        down_weight,
        down_bias,
        feedforward_gain_in,
        feedforward_gain_out,
    )
    attention_full = (
        lax.all_gather(attention_local[0], "shard", axis=0, tiled=True),
        lax.all_gather(attention_local[1], "shard", axis=0, tiled=True),
        lax.all_gather(attention_local[2], "shard", axis=0, tiled=True),
        lax.all_gather(attention_local[3], "shard", axis=0, tiled=True),
        lax.all_gather(attention_local[4], "shard", axis=0, tiled=True),
        lax.all_gather(attention_local[5], "shard", axis=0, tiled=True),
        lax.all_gather(attention_local[6], "shard", axis=0, tiled=True),
        lax.all_gather(attention_local[7], "shard", axis=0, tiled=True),
        lax.all_gather(attention_local[8], "shard", axis=0, tiled=True),
        lax.all_gather(attention_local[9], "shard", axis=0, tiled=True),
    )
    (
        query_mat,
        key_mat,
        value_mat,
        out_mat,
        query_shift,
        key_shift,
        value_shift,
        out_shift,
        gain_in_a,
        gain_out_a,
    ) = attention_full
    residual_in = layer_input.astype(jnp.float32)
    normed_a, inverse_a = normalize(residual_in)
    hidden_a = (normed_a * gain_in_a.astype(jnp.float32)).astype(jnp.bfloat16)

    def project(matrix, shift):
        return jnp.dot(hidden_a, matrix, preferred_element_type=jnp.float32) + shift.astype(
            jnp.float32
        )

    query_heads = rotate(
        project(query_mat, query_shift).reshape(rows, heads, head_dim), cosines, sines, 1.0
    ).astype(jnp.bfloat16)
    key_rows = (
        rotate(project(key_mat, key_shift).reshape(rows, heads, head_dim), cosines, sines, 1.0)
        .astype(jnp.bfloat16)
        .reshape(rows, width)
    )
    value_rows = project(value_mat, value_shift).astype(jnp.bfloat16)
    start_state = (
        jnp.full((heads, rows), -1e30, jnp.float32),
        jnp.zeros((heads, rows), jnp.float32),
        jnp.zeros((heads, rows, head_dim), jnp.float32),
    )
    key_piece = lax.all_gather(key_rows, "shard", axis=0, tiled=True)
    value_piece = lax.all_gather(value_rows, "shard", axis=0, tiled=True)
    count = key_piece.shape[0]
    block = math.gcd(count, 512)

    def forward_inner(index, state):
        best, total, accum = state
        offset = index * block
        key_block = lax.dynamic_slice_in_dim(key_piece, offset, block, 0).reshape(
            block, heads, head_dim
        )
        value_block = lax.dynamic_slice_in_dim(value_piece, offset, block, 0).reshape(
            block, heads, head_dim
        )
        key_pos = offset + jnp.arange(block, dtype=jnp.int32)
        allowed = key_pos[None, None, :] <= positions[None, :, None]
        scores = (
            jnp.einsum("qhd,khd->hqk", query_heads, key_block, preferred_element_type=jnp.float32)
            * factor
        )
        scores = jnp.where(allowed, scores, -1e30)
        newest = jnp.maximum(best, jnp.max(scores, axis=-1))
        weights = jnp.where(allowed, jnp.exp(scores - newest[..., None]), 0.0)
        decay = jnp.exp(best - newest)
        total = total * decay + jnp.sum(weights, axis=-1)
        accum = accum * decay[..., None] + jnp.einsum(
            "hqk,khd->hqd",
            weights.astype(jnp.bfloat16),
            value_block,
            preferred_element_type=jnp.float32,
        )
        return (newest, total, accum)

    best, total, accum = lax.fori_loop(0, count // block, forward_inner, start_state)
    logsum = best + jnp.log(total)
    attended = (
        jnp.transpose(accum / total[..., None], (1, 0, 2)).reshape(rows, width).astype(jnp.bfloat16)
    )
    branch_a = jnp.dot(attended, out_mat, preferred_element_type=jnp.float32) + out_shift.astype(
        jnp.float32
    )
    normed_o, inverse_o = normalize(branch_a)
    middle = residual_in + normed_o * gain_out_a.astype(jnp.float32)
    feed_full = (
        lax.all_gather(feed_local[0], "shard", axis=0, tiled=True),
        lax.all_gather(feed_local[1], "shard", axis=0, tiled=True),
        lax.all_gather(feed_local[2], "shard", axis=0, tiled=True),
        lax.all_gather(feed_local[3], "shard", axis=0, tiled=True),
        lax.all_gather(feed_local[4], "shard", axis=0, tiled=True),
        lax.all_gather(feed_local[5], "shard", axis=0, tiled=True),
    )
    up_mat, up_shift, down_mat, down_shift, gain_in_f, gain_out_f = feed_full
    normed_f, inverse_f = normalize(middle)
    hidden_f = (normed_f * gain_in_f.astype(jnp.float32)).astype(jnp.bfloat16)
    pre_act = jnp.dot(hidden_f, up_mat, preferred_element_type=jnp.float32) + up_shift.astype(
        jnp.float32
    )
    activated = jax.nn.gelu(pre_act).astype(jnp.bfloat16)
    branch_f = jnp.dot(activated, down_mat, preferred_element_type=jnp.float32) + down_shift.astype(
        jnp.float32
    )
    normed_d, inverse_d = normalize(branch_f)
    layer_output = (middle + normed_d * gain_out_f.astype(jnp.float32)).astype(jnp.bfloat16)
    feed_back = (
        lax.all_gather(feed_local[0], "shard", axis=0, tiled=True),
        lax.all_gather(feed_local[1], "shard", axis=0, tiled=True),
        lax.all_gather(feed_local[2], "shard", axis=0, tiled=True),
        lax.all_gather(feed_local[3], "shard", axis=0, tiled=True),
        lax.all_gather(feed_local[4], "shard", axis=0, tiled=True),
        lax.all_gather(feed_local[5], "shard", axis=0, tiled=True),
    )
    up_back, up_unused, down_back, down_unused, gain_in_fb, gain_out_fb = feed_back
    upstream = layer_cotangent.astype(jnp.float32)
    grad_gain_out_f = jnp.sum(upstream * normed_d, axis=0)
    d_branch_f = norm_back(normed_d, inverse_d, upstream * gain_out_fb.astype(jnp.float32)).astype(
        jnp.bfloat16
    )
    grad_down = jnp.einsum("tf,td->fd", activated, d_branch_f, preferred_element_type=jnp.float32)
    grad_down_shift = col_sum(d_branch_f)
    d_activated = jnp.einsum("td,fd->tf", d_branch_f, down_back, preferred_element_type=jnp.float32)
    gelu_out, gelu_pull = jax.vjp(jax.nn.gelu, pre_act)
    d_pre = gelu_pull(d_activated)[0].astype(jnp.bfloat16)
    grad_up = jnp.einsum("td,tf->df", hidden_f, d_pre, preferred_element_type=jnp.float32)
    grad_up_shift = col_sum(d_pre)
    d_hidden_f = jnp.einsum("tf,df->td", d_pre, up_back, preferred_element_type=jnp.float32)
    grad_gain_in_f = jnp.sum(d_hidden_f * normed_f, axis=0)
    d_middle = upstream + norm_back(
        normed_f, inverse_f, d_hidden_f * gain_in_fb.astype(jnp.float32)
    )
    feed_grads = (
        lax.psum_scatter(
            grad_up.astype(jnp.bfloat16), "shard", scatter_dimension=0, tiled=True
        ).astype(jnp.float32),
        lax.psum_scatter(
            grad_up_shift.astype(jnp.bfloat16), "shard", scatter_dimension=0, tiled=True
        ).astype(jnp.float32),
        lax.psum_scatter(
            grad_down.astype(jnp.bfloat16), "shard", scatter_dimension=0, tiled=True
        ).astype(jnp.float32),
        lax.psum_scatter(
            grad_down_shift.astype(jnp.bfloat16), "shard", scatter_dimension=0, tiled=True
        ).astype(jnp.float32),
        lax.psum_scatter(
            grad_gain_in_f.astype(jnp.bfloat16), "shard", scatter_dimension=0, tiled=True
        ).astype(jnp.float32),
        lax.psum_scatter(
            grad_gain_out_f.astype(jnp.bfloat16), "shard", scatter_dimension=0, tiled=True
        ).astype(jnp.float32),
    )
    attention_back = (
        lax.all_gather(attention_local[0], "shard", axis=0, tiled=True),
        lax.all_gather(attention_local[1], "shard", axis=0, tiled=True),
        lax.all_gather(attention_local[2], "shard", axis=0, tiled=True),
        lax.all_gather(attention_local[3], "shard", axis=0, tiled=True),
        lax.all_gather(attention_local[4], "shard", axis=0, tiled=True),
        lax.all_gather(attention_local[5], "shard", axis=0, tiled=True),
        lax.all_gather(attention_local[6], "shard", axis=0, tiled=True),
        lax.all_gather(attention_local[7], "shard", axis=0, tiled=True),
        lax.all_gather(attention_local[8], "shard", axis=0, tiled=True),
        lax.all_gather(attention_local[9], "shard", axis=0, tiled=True),
    )
    (
        query_back,
        key_back,
        value_back,
        out_back,
        qshift_unused,
        kshift_unused,
        vshift_unused,
        oshift_unused,
        gain_in_ab,
        gain_out_ab,
    ) = attention_back
    grad_gain_out_a = jnp.sum(d_middle * normed_o, axis=0)
    d_branch_a = norm_back(normed_o, inverse_o, d_middle * gain_out_ab.astype(jnp.float32)).astype(
        jnp.bfloat16
    )
    grad_out_mat = jnp.einsum("td,te->de", attended, d_branch_a, preferred_element_type=jnp.float32)
    grad_out_shift = col_sum(d_branch_a)
    d_attended = jnp.einsum(
        "te,de->td", d_branch_a, out_back, preferred_element_type=jnp.float32
    ).astype(jnp.bfloat16)
    d_heads = d_attended.reshape(rows, heads, head_dim)
    row_delta = jnp.einsum(
        "qhd,qhd->hq",
        d_heads.astype(jnp.float32),
        attended.reshape(rows, heads, head_dim).astype(jnp.float32),
    )

    def query_terms(key_block, value_block, key_pos):
        allowed = key_pos[None, None, :] <= positions[None, :, None]
        scores = (
            jnp.einsum("qhd,khd->hqk", query_heads, key_block, preferred_element_type=jnp.float32)
            * factor
        )
        probs = jnp.where(allowed, jnp.exp(scores - logsum[..., None]), 0.0)
        d_probs = jnp.einsum(
            "qhd,khd->hqk", d_heads, value_block, preferred_element_type=jnp.float32
        )
        d_scores = (probs * (d_probs - row_delta[..., None])).astype(jnp.bfloat16)
        return (probs, d_scores)

    back_state = (
        jnp.zeros((rows, heads, head_dim), jnp.float32),
        jnp.zeros((seq_rows, width), jnp.float32),
        jnp.zeros((seq_rows, width), jnp.float32),
    )
    backward_key_piece = lax.all_gather(key_rows, "shard", axis=0, tiled=True)
    backward_value_piece = lax.all_gather(value_rows, "shard", axis=0, tiled=True)
    count = backward_key_piece.shape[0]
    backward_block = math.gcd(count, 512)

    def backward_inner(index, state):
        grad_query, grad_keys, grad_values = state
        offset = index * backward_block
        key_block = lax.dynamic_slice_in_dim(backward_key_piece, offset, backward_block, 0).reshape(
            backward_block, heads, head_dim
        )
        value_block = lax.dynamic_slice_in_dim(
            backward_value_piece, offset, backward_block, 0
        ).reshape(backward_block, heads, head_dim)
        key_pos = offset + jnp.arange(backward_block, dtype=jnp.int32)
        probs, d_scores = query_terms(key_block, value_block, key_pos)
        grad_query = (
            grad_query
            + jnp.einsum("hqk,khd->qhd", d_scores, key_block, preferred_element_type=jnp.float32)
            * factor
        )
        key_grad = (
            jnp.einsum("hqk,qhd->khd", d_scores, query_heads, preferred_element_type=jnp.float32)
            * factor
        )
        value_grad = jnp.einsum(
            "hqk,qhd->khd", probs.astype(jnp.bfloat16), d_heads, preferred_element_type=jnp.float32
        )
        grad_keys = lax.dynamic_update_slice_in_dim(
            grad_keys, key_grad.reshape(backward_block, width), offset, 0
        )
        grad_values = lax.dynamic_update_slice_in_dim(
            grad_values, value_grad.reshape(backward_block, width), offset, 0
        )
        return (grad_query, grad_keys, grad_values)

    back_result = lax.fori_loop(0, count // backward_block, backward_inner, back_state)
    grad_query = back_result[0]
    key_total, value_total = (
        lax.psum_scatter(
            back_result[1].astype(jnp.bfloat16), "shard", scatter_dimension=0, tiled=True
        ).astype(jnp.float32),
        lax.psum_scatter(
            back_result[2].astype(jnp.bfloat16), "shard", scatter_dimension=0, tiled=True
        ).astype(jnp.float32),
    )
    d_query = rotate(grad_query, cosines, sines, -1.0).reshape(rows, width).astype(jnp.bfloat16)
    d_key = (
        rotate(key_total.reshape(rows, heads, head_dim), cosines, sines, -1.0)
        .reshape(rows, width)
        .astype(jnp.bfloat16)
    )
    d_value = value_total.astype(jnp.bfloat16)
    grad_query_mat = jnp.einsum("td,te->de", hidden_a, d_query, preferred_element_type=jnp.float32)
    grad_key_mat = jnp.einsum("td,te->de", hidden_a, d_key, preferred_element_type=jnp.float32)
    grad_value_mat = jnp.einsum("td,te->de", hidden_a, d_value, preferred_element_type=jnp.float32)
    d_hidden_a = jnp.einsum("te,de->td", d_query, query_back, preferred_element_type=jnp.float32)
    d_hidden_a = d_hidden_a + jnp.einsum(
        "te,de->td", d_key, key_back, preferred_element_type=jnp.float32
    )
    d_hidden_a = d_hidden_a + jnp.einsum(
        "te,de->td", d_value, value_back, preferred_element_type=jnp.float32
    )
    grad_gain_in_a = jnp.sum(d_hidden_a * normed_a, axis=0)
    input_gradient = d_middle + norm_back(
        normed_a, inverse_a, d_hidden_a * gain_in_ab.astype(jnp.float32)
    )
    attention_grads = (
        lax.psum_scatter(
            grad_query_mat.astype(jnp.bfloat16), "shard", scatter_dimension=0, tiled=True
        ).astype(jnp.float32),
        lax.psum_scatter(
            grad_key_mat.astype(jnp.bfloat16), "shard", scatter_dimension=0, tiled=True
        ).astype(jnp.float32),
        lax.psum_scatter(
            grad_value_mat.astype(jnp.bfloat16), "shard", scatter_dimension=0, tiled=True
        ).astype(jnp.float32),
        lax.psum_scatter(
            grad_out_mat.astype(jnp.bfloat16), "shard", scatter_dimension=0, tiled=True
        ).astype(jnp.float32),
        lax.psum_scatter(
            col_sum(d_query).astype(jnp.bfloat16), "shard", scatter_dimension=0, tiled=True
        ).astype(jnp.float32),
        lax.psum_scatter(
            col_sum(d_key).astype(jnp.bfloat16), "shard", scatter_dimension=0, tiled=True
        ).astype(jnp.float32),
        lax.psum_scatter(
            col_sum(d_value).astype(jnp.bfloat16), "shard", scatter_dimension=0, tiled=True
        ).astype(jnp.float32),
        lax.psum_scatter(
            grad_out_shift.astype(jnp.bfloat16), "shard", scatter_dimension=0, tiled=True
        ).astype(jnp.float32),
        lax.psum_scatter(
            grad_gain_in_a.astype(jnp.bfloat16), "shard", scatter_dimension=0, tiled=True
        ).astype(jnp.float32),
        lax.psum_scatter(
            grad_gain_out_a.astype(jnp.bfloat16), "shard", scatter_dimension=0, tiled=True
        ).astype(jnp.float32),
    )
    (
        g_query,
        g_key,
        g_value,
        g_out,
        g_qshift,
        g_kshift,
        g_vshift,
        g_oshift,
        g_gain_in_a,
        g_gain_out_a,
    ) = attention_grads
    g_up, g_up_shift, g_down, g_down_shift, g_gain_in_f, g_gain_out_f = feed_grads
    summed = (
        lax.psum(g_query.astype(jnp.bfloat16), "rep").astype(jnp.float32),
        lax.psum(g_qshift.astype(jnp.bfloat16), "rep").astype(jnp.float32),
        lax.psum(g_key.astype(jnp.bfloat16), "rep").astype(jnp.float32),
        lax.psum(g_kshift.astype(jnp.bfloat16), "rep").astype(jnp.float32),
        lax.psum(g_value.astype(jnp.bfloat16), "rep").astype(jnp.float32),
        lax.psum(g_vshift.astype(jnp.bfloat16), "rep").astype(jnp.float32),
        lax.psum(g_out.astype(jnp.bfloat16), "rep").astype(jnp.float32),
        lax.psum(g_oshift.astype(jnp.bfloat16), "rep").astype(jnp.float32),
        lax.psum(g_up.astype(jnp.bfloat16), "rep").astype(jnp.float32),
        lax.psum(g_up_shift.astype(jnp.bfloat16), "rep").astype(jnp.float32),
        lax.psum(g_down.astype(jnp.bfloat16), "rep").astype(jnp.float32),
        lax.psum(g_down_shift.astype(jnp.bfloat16), "rep").astype(jnp.float32),
        lax.psum(g_gain_in_a.astype(jnp.bfloat16), "rep").astype(jnp.float32),
        lax.psum(g_gain_out_a.astype(jnp.bfloat16), "rep").astype(jnp.float32),
        lax.psum(g_gain_in_f.astype(jnp.bfloat16), "rep").astype(jnp.float32),
        lax.psum(g_gain_out_f.astype(jnp.bfloat16), "rep").astype(jnp.float32),
    )
    return (
        layer_output,
        input_gradient,
        summed[0],
        summed[1],
        summed[2],
        summed[3],
        summed[4],
        summed[5],
        summed[6],
        summed[7],
        summed[8],
        summed[9],
        summed[10],
        summed[11],
        summed[12],
        summed[13],
        summed[14],
        summed[15],
    )


CORE, X, Y = 1, 2, 4
GROUP = 4
BLOCK = 256


def swap(values, bit):
    count = lax.axis_size("rep")
    return lax.ppermute(values, "rep", [(i, i ^ bit) for i in range(count)])


def shift(values, step):
    count = lax.axis_size("shard")
    return lax.ppermute(values, "shard", [(i, (i + step) % count) for i in range(count)])


def token_pairs(count):
    pairs = []
    for rep in range(count):
        for z in range(GROUP):
            there = (rep & ~3) | ((z & 1) << 1) | (z >> 1)
            pairs.append((rep * GROUP + z, there * GROUP + (rep & 3)))
    return pairs


def spot():
    rep, place = lax.axis_index("rep"), lax.axis_index("shard")
    return rep & 3, place, rep >> 2, ((rep >> 1) & 1) + 2 * (rep & 1)


def aligned(index, size):
    return pl.ds(pl.multiple_of(index * size, size), size)


def dot(left, right):
    return jnp.dot(left, right, preferred_element_type=jnp.float32)


def nt(left, right):
    return lax.dot_general(left, right, (((1,), (1,)), ((), ())), preferred_element_type=jnp.float32)


def tn(left, right):
    return lax.dot_general(left, right, (((0,), (0,)), ((), ())), preferred_element_type=jnp.float32)


def rounded(values):
    return values.astype(jnp.bfloat16)


def wide(values):
    return values.astype(jnp.float32)


def shaped(*dims, kind=jnp.bfloat16):
    return jax.ShapeDtypeStruct(dims, kind)


VMEM_SPEC = pl.BlockSpec(memory_space=pltpu.VMEM)


def call(kernel, outs, *operands, scratch=(), flops=0, exps=0, room=6):
    size = lambda items: sum(math.prod(item.shape) * item.dtype.itemsize for item in items)
    moved = size(operands) + size(outs)
    spaces = [jax.ShapeDtypeStruct(item.shape, item.dtype) for item in scratch]
    return pl.pallas_call(
        kernel,
        out_shape=tuple(outs),
        in_specs=[VMEM_SPEC] * len(operands),
        out_specs=tuple([VMEM_SPEC] * len(outs)),
        scratch_shapes=list(scratch),
        compiler_params=pltpu.CompilerParams(vmem_limit_bytes=moved + size(spaces) + (room << 20)),
        cost_estimate=pl.CostEstimate(flops=flops, bytes_accessed=moved, transcendentals=exps),
        name=kernel.__name__,
    )(*operands)


def standardize(values):
    centered = values - jnp.mean(values, axis=-1, keepdims=True)
    inverse = lax.rsqrt(jnp.mean(centered * centered, axis=-1, keepdims=True) + norm_epsilon)
    return centered * inverse, inverse


def turn(values, cosines, sines):
    lane = lax.broadcasted_iota(jnp.int32, values.shape, 1)
    swapped = jnp.where(lane % 64 < 32, pltpu.roll(values, 96, 1), pltpu.roll(values, 32, 1))
    return values * cosines + swapped * sines


def rope_tables(tokens, head_dim):
    half = head_dim // 2
    freqs = 10000.0 ** (-jnp.arange(half, dtype=jnp.float32) / half)
    angles = jnp.arange(tokens, dtype=jnp.int32).astype(jnp.float32)[:, None] * freqs[None, :]
    cosines, sines = jnp.cos(angles), jnp.sin(angles)
    return (
        jnp.concatenate([cosines] * 4, 1),
        jnp.concatenate([-sines, sines, -sines, sines], 1),
    )


def pack_attention(
    query_weight, key_weight, value_weight, out_weight, qb, kb, vb, ub, ob, db, ga, gb, gc, gd, packed
):
    quarter, place, _, _ = spot()
    row = lax.broadcasted_iota(jnp.int32, (1024, 256), 0)
    col = lax.broadcasted_iota(jnp.int32, (1024, 256), 1)
    chosen = rounded(wide(row == (col // 64) * 256 + quarter * 64 + col % 64))
    for index, weight in enumerate((query_weight, key_weight, value_weight)):
        mine = rounded(dot(weight[...], chosen))
        for half in range(2):
            packed[half, :128, index * 256 : index * 256 + 256] = mine[half * 128 : half * 128 + 128]
    out_mine = out_weight[aligned(quarter, 64), :]
    for j in range(4):
        at = (j % 2) * 64
        packed[j // 2, at : at + 64, 768:1024] = out_mine[:, j * 256 : j * 256 + 256]
    row = lax.broadcasted_iota(jnp.int32, (256, 256), 0)
    col = lax.broadcasted_iota(jnp.int32, (256, 256), 1)
    chosen = rounded(wide((row == quarter * 64 + col % 64) & (col // 64 == place)))
    biases = [dot(jnp.broadcast_to(item[...][None, :], (16, 256)), chosen) for item in (qb, kb, vb)]
    full = lambda item: jnp.broadcast_to(wide(item[...])[None, :], (16, 256))
    up_mine = jnp.broadcast_to(wide(ub[aligned(quarter, 256)])[None, :], (16, 256))
    zero = jnp.zeros((16, 256), jnp.float32)
    first = jnp.concatenate(biases + [zero], 1)
    second = jnp.concatenate([up_mine, full(ob), full(db), zero], 1)
    third = jnp.concatenate([full(ga), full(gb), full(gc), full(gd)], 1)
    at = lax.broadcasted_iota(jnp.int32, (16, 1024), 0)
    rows = jnp.where(at == 0, first, jnp.where(at == 1, second, jnp.where(at == 2, third, 0.0)))
    for half in range(2):
        packed[half, 128:144, :] = rounded(rows)


def pack_feed(up_weight, down_weight, up_packed, down_packed, sems):
    quarter, _, _, _ = spot()
    copies = []
    for half in range(2):
        for there in range(4):
            lanes = pl.ds(pl.multiple_of(there * 1024 + quarter * 256, 256), 256)
            copies.append(
                (
                    up_weight.at[half * 128 : half * 128 + 128, lanes],
                    up_packed.at[half, :, there * 256 : there * 256 + 256],
                )
            )
        copies.append((down_weight.at[aligned(quarter * 2 + half, 128), :], down_packed.at[half]))
    copies = [pltpu.make_async_copy(a, b, sems.at[i]) for i, (a, b) in enumerate(copies)]
    for copy in copies:
        copy.start()
    for copy in copies:
        copy.wait()


def call_pack_feed(up_weight, down_weight):
    spec = pl.BlockSpec(memory_space=pl.ANY)
    return pl.pallas_call(
        pack_feed,
        out_shape=(shaped(2, 128, 1024), shaped(2, 128, 1024)),
        in_specs=[spec, spec],
        out_specs=(VMEM_SPEC, VMEM_SPEC),
        scratch_shapes=[pltpu.SemaphoreType.DMA((10,))],
        compiler_params=pltpu.CompilerParams(vmem_limit_bytes=8 << 20),
        cost_estimate=pl.CostEstimate(flops=0, bytes_accessed=2 << 20, transcendentals=0),
        name="pack_feed",
    )(up_weight, down_weight)


def tie(value, *earlier):
    return lax.optimization_barrier((value, *earlier))[0]


def near_pieces(packed, half, *earlier):
    mine = tie(lax.dynamic_index_in_dim(packed, half, 0, False), *earlier)
    return [shift(mine, step) for step in (1, 2, 3)]


def far_pieces(near):
    return [swap(item, Y) for item in near]


def each_piece(own, near, far):
    _, place, y_bit, _ = spot()
    yield place, 0, own.at[0]
    yield place, 1, own.at[1]
    for step in (1, 2, 3):
        yield (place + 4 - step) & 3, y_bit, near[step - 1]
        yield (place + 4 - step) & 3, 1 - y_bit, far[step - 1]


def head_lanes(shape, parity):
    return (lax.broadcasted_iota(jnp.int32, shape, 1) // 64) == parity


def causal_block():
    shape = (BLOCK, BLOCK)
    return lax.broadcasted_iota(jnp.int32, shape, 0) >= lax.broadcasted_iota(jnp.int32, shape, 1)


def attend(
    x0, x1, x2, x3, own, z1, z2, z3, y1, y2, y3, cosines, sines,
    query, key, value, mixed, logs, hidden, qkv, out_rows, vectors, p0, p1, p2, p3,
):
    _, _, _, position = spot()
    for relative, rows_in in enumerate((x0, x1, x2, x3)):
        hidden[aligned(position ^ relative, BLOCK), :] = rows_in[...]
    vectors[...] = jnp.zeros_like(vectors)
    for index, (shard, half, piece) in enumerate(each_piece(own, (z1, z2, z3), (y1, y2, y3))):
        qkv[aligned(shard * 2 + half, 128), :] = piece[:128, :768]
        for j in range(2):
            out_rows[aligned(shard, 64), aligned(half * 2 + j, 256)] = piece[j * 64 : j * 64 + 64, 768:]
        if index == 0 or index >= 2 and index % 2 == 0:
            small = wide(piece[128:144, :])
            lanes = aligned(shard, 256)
            vectors[0:1, lanes] = small[1:2, 256:512]
            vectors[1:2, lanes] = small[1:2, 512:768]
            for gain in range(4):
                vectors[2 + gain : 3 + gain, lanes] = small[2:3, gain * 256 : gain * 256 + 256]
            vectors[6:7, lanes] = small[1:2, :256]
            vectors[7:8, :] += small[0:1, :]

    def project(index, carry):
        rows = aligned(index, BLOCK)
        normed, _ = standardize(wide(hidden[rows, :]))
        block = rounded(normed * vectors[2:3, :])
        hidden[rows, :] = block
        raw = dot(block, qkv[...]) + vectors[7:8, :768]
        cos, sin = cosines[rows, :], sines[rows, :]
        for tile in range(2):
            at = tile * 128
            lanes = slice(at, at + 128)
            query[rows, lanes] = rounded(turn(raw[:, lanes], cos, sin)) * jnp.bfloat16(0.125)
            key[rows, lanes] = rounded(turn(raw[:, 256 + at : 384 + at], cos, sin))
        value[rows, :] = rounded(raw[:, 512:])
        return carry

    lax.fori_loop(0, GROUP, project, 0)
    causal = causal_block()
    logs[...] = jnp.zeros_like(logs)

    def pair_step(pair, carry):
        lanes = aligned(pair, 128)
        lane = lax.broadcasted_iota(jnp.int32, (BLOCK, 128), 1)
        for block in range(GROUP):
            rows = slice(block * BLOCK, block * BLOCK + BLOCK)
            seen = (block + 1) * BLOCK
            queries = query[rows, lanes]
            keys, values = key[:seen, lanes], value[:seen, lanes]
            outs = []
            log_rows = logs[rows, :]
            for parity in range(2):
                masked = jnp.where(head_lanes(queries.shape, parity), queries, jnp.bfloat16(0))
                scores = nt(masked, keys)
                last = jnp.where(causal, scores[:, seen - BLOCK :], -1e30)
                scores = jnp.concatenate([scores[:, : seen - BLOCK], last], 1) if block else last
                best = jnp.max(scores, axis=1, keepdims=True)
                exps = jnp.exp(scores - best)
                total = jnp.sum(exps, axis=1, keepdims=True)
                outs.append(dot(rounded(exps), values) / total)
                log_rows = jnp.where(lane == pair * 2 + parity, best + jnp.log(total), log_rows)
            mixed[rows, lanes] = rounded(jnp.where(lane < 64, outs[0], outs[1]))
            logs[rows, :] = log_rows
        return carry

    lax.fori_loop(0, 2, pair_step, 0)
    for relative, part in enumerate((p0, p1, p2, p3)):
        part[...] = rounded(dot(mixed[aligned(position ^ relative, BLOCK), :], out_rows[...]))


def attend_back(
    a0, a1, a2, a3, out_rows, qkv, query, key, value, mixed, logs, cosines, sines,
    grads, shift_sums, p0, p1, p2, p3, d_out, d_key, d_value, d_query,
):
    _, _, _, position = spot()
    for relative, rows_in in enumerate((a0, a1, a2, a3)):
        d_out[aligned(position ^ relative, BLOCK), :] = rounded(nt(rows_in[...], out_rows[...]))
    d_key[...] = jnp.zeros_like(d_key)
    d_value[...] = jnp.zeros_like(d_value)
    causal = causal_block()

    def pair_step(pair, carry):
        lanes = aligned(pair, 128)
        for block in range(GROUP):
            rows = slice(block * BLOCK, block * BLOCK + BLOCK)
            seen = (block + 1) * BLOCK
            queries, d_outs = query[rows, lanes], d_out[rows, lanes]
            keys, values = key[:seen, lanes], value[:seen, lanes]
            products = wide(d_outs) * wide(mixed[rows, lanes])
            log_rows = logs[rows, :]
            lane = lax.broadcasted_iota(jnp.int32, (BLOCK, 128), 1)
            d_queries = []
            for parity in range(2):
                mine = head_lanes((BLOCK, 128), parity)
                masked_q = jnp.where(mine, queries, jnp.bfloat16(0))
                masked_d = jnp.where(mine, d_outs, jnp.bfloat16(0))
                log = jnp.sum(jnp.where(lane == pair * 2 + parity, log_rows, 0.0), 1, keepdims=True)
                delta = jnp.sum(jnp.where(mine, products, 0.0), 1, keepdims=True)
                probs = jnp.exp(nt(masked_q, keys) - log)
                last = jnp.where(causal, probs[:, seen - BLOCK :], 0.0)
                probs = jnp.concatenate([probs[:, : seen - BLOCK], last], 1) if block else last
                d_scores = rounded(probs * (nt(masked_d, values) - delta))
                d_queries.append(dot(d_scores, keys))
                d_value[:seen, lanes] += tn(rounded(probs), masked_d)
                d_key[:seen, lanes] += tn(d_scores, masked_q)
            d_query[rows, lanes] = jnp.where(lane < 64, d_queries[0], d_queries[1])
        return carry

    lax.fori_loop(0, 2, pair_step, 0)
    shift_sums[...] = jnp.zeros_like(shift_sums)

    def finish(index, carry):
        rows = aligned(index, BLOCK)
        cos, sin = cosines[rows, :], -sines[rows, :]
        for tile in range(2):
            at = tile * 128
            lanes = slice(at, at + 128)
            grads[rows, at : at + 128] = rounded(turn(d_query[rows, lanes] * 0.125, cos, sin))
            grads[rows, at + 256 : at + 384] = rounded(turn(d_key[rows, lanes], cos, sin))
        grads[rows, 512:] = rounded(d_value[rows, :])
        shift_sums[0:1, :] += jnp.sum(wide(grads[rows, :]), axis=0, keepdims=True)
        return carry

    lax.fori_loop(0, GROUP, finish, 0)
    for relative, part in enumerate((p0, p1, p2, p3)):
        part[...] = rounded(nt(grads[aligned(position ^ relative, BLOCK), :], qkv[...]))


def after_attention(p0, core_in, x_in, rows_in, vectors, middle, hidden, normed_o, normed_f, inverses):
    branch = wide(p0[...]) + wide(core_in[...]) + wide(x_in[...]) + vectors[0:1, :]
    normed, inverse_o = standardize(branch)
    normed_o[...] = normed
    total = wide(rows_in[...]) + normed * vectors[3:4, :]
    middle[...] = total
    normed, inverse_f = standardize(total)
    normed_f[...] = normed
    hidden[...] = rounded(normed * vectors[4:5, :])
    lane = lax.broadcasted_iota(jnp.int32, inverses.shape, 1)
    inverses[...] = jnp.where(lane < 64, inverse_o, inverse_f)


def after_feed(p0, core_in, x_in, middle, cotangent, vectors, layer_out, d_branch, sums):
    branch = wide(p0[...]) + wide(core_in[...]) + wide(x_in[...]) + vectors[1:2, :]
    normed, inverse = standardize(branch)
    gain = vectors[5:6, :]
    layer_out[...] = rounded(middle[...] + normed * gain)
    upstream = wide(cotangent[...])
    back = rounded(norm_back(normed, inverse, upstream * gain))
    d_branch[...] = back
    sums[...] = jnp.zeros_like(sums)
    sums[0:1, :] = jnp.sum(upstream * normed, axis=0, keepdims=True)
    sums[1:2, :] = jnp.sum(wide(back), axis=0, keepdims=True)


def after_feed_back(
    p0, core_in, x_in, cotangent, normed_o, normed_f, inverses, vectors, d_middle, d_branch, sums
):
    d_hidden = wide(p0[...]) + wide(core_in[...]) + wide(x_in[...])
    normed = normed_f[...]
    sums[...] = jnp.zeros_like(sums)
    sums[0:1, :] = jnp.sum(d_hidden * normed, axis=0, keepdims=True)
    total = wide(cotangent[...]) + norm_back(normed, inverses[:, 64:65], d_hidden * vectors[4:5, :])
    d_middle[...] = total
    normed = normed_o[...]
    sums[1:2, :] = jnp.sum(total * normed, axis=0, keepdims=True)
    back = rounded(norm_back(normed, inverses[:, 0:1], total * vectors[3:4, :]))
    d_branch[...] = back
    sums[2:3, :] = jnp.sum(wide(back), axis=0, keepdims=True)


def after_attention_back(p0, core_in, x_in, rows_in, d_middle, vectors, d_rows, sums):
    d_hidden = wide(p0[...]) + wide(core_in[...]) + wide(x_in[...])
    normed, inverse = standardize(wide(rows_in[...]))
    sums[...] = jnp.zeros_like(sums)
    sums[0:1, :] = jnp.sum(d_hidden * normed, axis=0, keepdims=True)
    d_rows[...] = rounded(d_middle[...] + norm_back(normed, inverse, d_hidden * vectors[2:3, :]))


GELU_SCALE = math.sqrt(2.0 / math.pi)


def feed_rows(rows_in, up_mat, down_mat, vectors, before, after, part, at):
    rows = slice(at, at + BLOCK)

    def step(index, carry):
        lanes = aligned(index, BLOCK)
        raw = dot(rows_in[...], up_mat[:, lanes]) + vectors[6:7, lanes]
        before[rows, lanes] = raw
        after[rows, lanes] = rounded(jax.nn.gelu(raw))
        return carry

    lax.fori_loop(0, 4, step, 0)

    def out(index, carry):
        lanes = aligned(index, BLOCK)
        part[:, lanes] = rounded(dot(after[rows, :], down_mat[:, lanes]))
        return carry

    lax.fori_loop(0, 4, out, 0)


def feed_first(
    h0, h2, uo, u1, u2, u3, v1, v2, v3, do, d1, d2, d3, e1, e2, e3, vectors,
    up_mat, down_mat, before, after, p0, p2,
):
    for shard, half, piece in each_piece(uo, (u1, u2, u3), (v1, v2, v3)):
        up_mat[aligned(shard * 2 + half, 128), :] = piece[...]
    for shard, half, piece in each_piece(do, (d1, d2, d3), (e1, e2, e3)):
        down_mat[aligned(shard * 2 + half, 128), :] = piece[...]
    feed_rows(h0, up_mat, down_mat, vectors, before, after, p0, 0)
    feed_rows(h2, up_mat, down_mat, vectors, before, after, p2, BLOCK)


def feed_second(h1, h3, up_mat, down_mat, vectors, before, after, p1, p3):
    feed_rows(h3, up_mat, down_mat, vectors, before, after, p3, BLOCK)
    feed_rows(h1, up_mat, down_mat, vectors, before, after, p1, 0)


def feed_back(da, db, up_mat, down_mat, before, d_pre, pa, pb, sums):
    sums[...] = jnp.zeros_like(sums)
    for at, rows_in, part in ((BLOCK, db, pb), (0, da, pa)):
        rows = slice(at, at + BLOCK)

        def step(index, carry):
            lanes = aligned(index, BLOCK)
            upstream = nt(rows_in[...], down_mat[lanes, :])
            raw = before[rows, lanes]
            square = raw * raw
            bent = jnp.tanh(GELU_SCALE * raw * (1.0 + 0.044715 * square))
            slope = 0.5 * (1.0 + bent) + 0.5 * GELU_SCALE * raw * (1.0 - bent * bent) * (
                1.0 + 3.0 * 0.044715 * square
            )
            back = rounded(upstream * slope)
            d_pre[rows, lanes] = back
            sums[0:1, lanes] += jnp.sum(wide(back), axis=0, keepdims=True)
            return carry

        lax.fori_loop(0, 4, step, 0)

        def out(index, carry):
            lanes = aligned(index, BLOCK)
            part[:, lanes] = rounded(nt(d_pre[rows, :], up_mat[lanes, :]))
            return carry

        lax.fori_loop(0, 4, out, 0)


def put_halves(keep, send, step, at, top, bottom):
    _, _, y_bit, _ = spot()

    @pl.when(y_bit == 0)
    def _():
        keep[step, at : at + 128, :] = top
        send[step, at : at + 128, :] = bottom

    @pl.when(y_bit == 1)
    def _():
        keep[step, at : at + 128, :] = bottom
        send[step, at : at + 128, :] = top


def down_grads(first, second, m0, m1, m2, m3, keep, send):
    _, place, _, _ = spot()

    def one(step, carry):
        lanes = aligned((place + step) & 3, BLOCK)
        down = (
            tn(first[:BLOCK, lanes], m0[...])
            + tn(first[BLOCK:, lanes], m2[...])
            + tn(second[:BLOCK, lanes], m1[...])
            + tn(second[BLOCK:, lanes], m3[...])
        )
        down = rounded(down)
        put_halves(keep, send, step, 0, down[:128], down[128:])
        return carry

    lax.fori_loop(0, 4, one, 0)


def up_grads(h0, h1, h2, h3, u_first, u_second, keep, send):
    _, place, _, _ = spot()

    def one(step, carry):
        lanes = aligned((place + step) & 3, BLOCK)
        up = (
            tn(h0[:, lanes], u_first[:BLOCK, :])
            + tn(h2[:, lanes], u_first[BLOCK:, :])
            + tn(h1[:, lanes], u_second[:BLOCK, :])
            + tn(h3[:, lanes], u_second[BLOCK:, :])
        )
        up = rounded(up)
        put_halves(keep, send, step, 0, up[:128], up[128:])
        return carry

    lax.fori_loop(0, 4, one, 0)


def attention_grads(mixed, a0, a1, a2, a3, hidden, d_qkv, keep, send, out_grad, block):
    _, place, _, position = spot()
    total = tn(mixed[aligned(position, BLOCK), :], a0[...])
    for relative, rows_in in ((1, a1), (2, a2), (3, a3)):
        total = total + tn(mixed[aligned(position ^ relative, BLOCK), :], rows_in[...])
    out_grad[...] = rounded(total)

    def one(step, carry):
        shard = (place + step) & 3
        block[:, :768] = rounded(tn(hidden[:, aligned(shard, BLOCK)], d_qkv[...]))
        mine = out_grad[aligned(shard, 64), :]
        for j in range(4):
            block[j * 64 : j * 64 + 64, 768:] = mine[:, j * 256 : j * 256 + 256]
        put_halves(keep, send, step, 0, block[:128, :], block[128:, :])
        return carry

    lax.fori_loop(0, 4, one, 0)


def add_four(keep, come, s0, s1, s2, s3):
    for step, out in enumerate((s0, s1, s2, s3)):
        out[...] = rounded(wide(keep[step]) + wide(come[step]))


def add_shards(s0, r1, r2, r3, total):
    total[...] = rounded(wide(s0[...]) + wide(r1[...]) + wide(r2[...]) + wide(r3[...]))


def each_part(own, x_part, y_part, core_part):
    rep = lax.axis_index("rep")
    refs = [own, x_part, y_part.at[0], y_part.at[1]] + [core_part.at[i] for i in range(4)]
    for relative, ref in enumerate(refs):
        flip = ((relative & 1) << 1) | ((relative & 2) << 1) | (relative >> 2)
        there = rep ^ flip
        yield there >> 2, there & 3, ref


def unpack_down(own, x_part, y_part, core_part, down):
    for y_bit, quarter, ref in each_part(own, x_part, y_part, core_part):
        down[aligned(quarter * 2 + y_bit, 128), :] = wide(ref[...])


def unpack_up(own, x_part, y_part, core_part, up):
    for y_bit, quarter, ref in each_part(own, x_part, y_part, core_part):
        for there in range(4):
            lanes = pl.ds(pl.multiple_of(there * 1024 + quarter * 256, 256), 256)
            up[aligned(y_bit, 128), lanes] = wide(ref[:, there * 256 : there * 256 + 256])


def unpack_attention(own, x_part, y_part, core_part, query, key, value, out_weight):
    rep = lax.axis_index("rep")
    row = lax.broadcasted_iota(jnp.int32, (256, 1024), 0)
    col = lax.broadcasted_iota(jnp.int32, (256, 1024), 1)
    for out in (query, key, value):
        out[...] = jnp.zeros_like(out)
    for y_bit, quarter, ref in each_part(own, x_part, y_part, core_part):
        chosen = rounded(wide(col == (row // 64) * 256 + quarter * 64 + row % 64))
        for index, out in enumerate((query, key, value)):
            out[aligned(y_bit, 128), :] += dot(ref[:, index * 256 : index * 256 + 256], chosen)
        for j in range(2):
            out_weight[aligned(quarter, 64), aligned(y_bit * 2 + j, 256)] = wide(
                ref[j * 64 : j * 64 + 64, 768:]
            )


def reduce_y(keep, send):
    part = shaped(keep.shape[1], 1024)
    return call(add_four, [part] * 4, keep, swap(send, Y))


def reduce_shards(parts):
    s0, s1, s2, s3 = parts
    (total,) = call(add_shards, [s0], s0, shift(s1, 1), shift(s2, 2), shift(s3, 3))
    return total


def gather_packs(total):
    x_part = swap(total, X)
    two = jnp.stack([total, x_part])
    y_part = swap(two, Y)
    return total, x_part, y_part, swap(jnp.concatenate([two, y_part]), CORE)


def split_small(own, r1, r2, r3, *outs):
    total = own[...] + r1[...] + r2[...] + r3[...]
    for index, out in enumerate(outs):
        if index < 9:
            out[...] = total[:, index * 256 : index * 256 + 256]
        else:
            out[...] = total[:, 2304:]


def fast_device(
    layer_input,
    query_weight,
    query_bias,
    key_weight,
    key_bias,
    value_weight,
    value_bias,
    output_weight,
    output_bias,
    up_weight,
    up_bias,
    down_weight,
    down_bias,
    attention_gain_in,
    attention_gain_out,
    feedforward_gain_in,
    feedforward_gain_out,
    layer_cotangent,
):
    f32, bf16 = jnp.float32, jnp.bfloat16
    replicas = lax.axis_size("rep")
    rows, width = layer_input.shape
    tokens = rows * GROUP
    quarter, place, y_bit, _ = spot()
    pairs = token_pairs(replicas)
    back_pairs = [(there, here) for here, there in pairs]
    both = ("rep", "shard")
    part = shaped(rows, width)
    part32 = shaped(rows, width, kind=f32)
    sums = shaped(8, width, kind=f32)

    def spread(piece):
        near, far = swap(piece, X), swap(piece, CORE)
        return piece, near, far, swap(near, CORE)

    def gather_sum(p1, p2, p3):
        across = rounded(wide(p1) + wide(swap(p3, CORE)))
        x_in = swap(across, X)
        return swap(p2, CORE), x_in

    own_rows = lax.ppermute(layer_input, both, pairs)
    (packed,) = call(
        pack_attention,
        [shaped(2, 144, width)],
        query_weight,
        key_weight,
        value_weight,
        output_weight,
        query_bias,
        key_bias,
        value_bias,
        up_bias,
        output_bias,
        down_bias,
        attention_gain_in,
        attention_gain_out,
        feedforward_gain_in,
        feedforward_gain_out,
    )
    near_a = near_pieces(packed, y_bit)
    cosines, sines = rope_tables(tokens, 64)
    up_packed, down_packed = call_pack_feed(up_weight, down_weight)
    own_rows = tie(own_rows, cosines, sines, up_packed)
    blocks = spread(own_rows)
    far_a = far_pieces(near_a)
    near_u = near_pieces(up_packed, y_bit, *near_a)
    near_d = near_pieces(down_packed, y_bit, *near_a)
    head_rows = shaped(tokens, 256)
    query, key, value, mixed, logs, hidden_a, qkv, out_rows, vectors, *parts = call(
        attend,
        [head_rows] * 4
        + [
            shaped(tokens, 128, kind=f32),
            shaped(tokens, width),
            shaped(width, 768),
            shaped(256, width),
            sums,
        ]
        + [part] * 4,
        *blocks,
        packed,
        *near_a,
        *far_a,
        cosines,
        sines,
        flops=2 * tokens * 1024 * 1024 + 8 * tokens * tokens * 64 * 2,
        exps=2 * tokens * tokens,
        room=14,
    )
    core_in, x_in = gather_sum(*parts[1:])
    far_u = far_pieces(near_u)
    x_in = tie(x_in, *near_u)
    middle, hidden_own, normed_o, normed_f, inverses = call(
        after_attention,
        [part32, part, part32, part32, shaped(rows, 128, kind=f32)],
        parts[0],
        core_in,
        x_in,
        own_rows,
        vectors,
    )
    h0, h1, h2, h3 = spread(hidden_own)
    far_d = far_pieces(near_d)
    cotangent = lax.ppermute(tie(layer_cotangent, *near_d), both, pairs)
    two32, two16 = shaped(2 * rows, width, kind=f32), shaped(2 * rows, width)
    square = shaped(width, width)
    flops = 4 * 2 * rows * 1024 * 1024
    up_mat, down_mat, before_a, after_a, p0, p2 = call(
        feed_first,
        [square, square, two32, two16, part, part],
        h0, h2, up_packed, *near_u, *far_u, down_packed, *near_d, *far_d, vectors,
        flops=flops, room=10,
    )
    h1 = tie(h1, up_mat)
    before_b, after_b, p1, p3 = call(
        feed_second,
        [two32, two16, part, part],
        h1, h3, up_mat, down_mat, vectors,
        flops=flops, room=10,
    )
    core_in, x_in = gather_sum(p1, p2, p3)
    layer_output, d_branch, sums_f = call(
        after_feed, [part, part, sums], p0, core_in, x_in, middle, cotangent, vectors
    )
    layer_output = lax.ppermute(layer_output, both, back_pairs)

    m0, m1, m2, m3 = spread(d_branch)
    u_first, p0, p2, sums_ua = call(
        feed_back,
        [two16, part, part, sums],
        m0, m2, up_mat, down_mat, before_a,
        flops=flops, room=10,
    )
    m1 = tie(m1, u_first)
    u_second, p1, p3, sums_ub = call(
        feed_back,
        [two16, part, part, sums],
        m1, m3, up_mat, down_mat, before_b,
        flops=flops, room=10,
    )
    core_in, x_in = gather_sum(p1, p2, p3)
    packs = [shaped(4, 128, width)] * 2
    flops = 2 * tokens * 1024 * 1024
    pack_d = call(down_grads, packs, after_a, after_b, m0, m1, m2, m3, flops=flops, room=10)
    pack_u = call(up_grads, packs, h0, h1, h2, h3, u_first, u_second, flops=flops, room=10)
    x_in = tie(x_in, *pack_d, *pack_u)
    d_middle, d_branch, sums_b = call(
        after_feed_back,
        [part32, part, sums],
        p0,
        core_in,
        x_in,
        cotangent,
        normed_o,
        normed_f,
        inverses,
        vectors,
    )
    a0, a1, a2, a3 = spread(d_branch)
    parts_d = reduce_y(*pack_d)
    a1 = tie(a1, layer_output, *parts_d)
    a_blocks = a0, a1, a2, a3
    grad32 = pltpu.VMEM((tokens, 256), f32)
    d_qkv, sums_q, p0, p1, p2, p3 = call(
        attend_back,
        [shaped(tokens, 768), shaped(8, 768, kind=f32)] + [part] * 4,
        *a_blocks, out_rows, qkv, query, key, value, mixed, logs, cosines, sines,
        scratch=[pltpu.VMEM((tokens, 256), bf16), grad32, grad32, grad32],
        flops=2 * tokens * 1024 * 1024 + 20 * tokens * tokens * 64 * 2,
        exps=2 * tokens * tokens,
        room=14,
    )
    core_in, x_in = gather_sum(p1, p2, p3)
    pack_a = call(
        attention_grads,
        packs,
        mixed, *a_blocks, hidden_a, d_qkv,
        scratch=[pltpu.VMEM((256, width), bf16), pltpu.VMEM((256, width), bf16)],
        flops=flops,
        room=10,
    )
    parts_u = reduce_y(*pack_u)
    total_d = reduce_shards(parts_d)
    x_in = tie(x_in, *pack_a, total_d)
    input_gradient, sums_a = call(
        after_attention_back, [part, sums], p0, core_in, x_in, own_rows, d_middle, vectors
    )
    input_gradient = lax.ppermute(input_gradient, both, back_pairs).astype(f32)
    parts_a = reduce_y(*pack_a)
    total_u = reduce_shards(parts_u)
    total_a = reduce_shards(parts_a)
    (g_down,) = call(unpack_down, [shaped(*down_weight.shape, kind=f32)], *gather_packs(total_d))
    (g_up,) = call(unpack_up, [shaped(*up_weight.shape, kind=f32)], *gather_packs(total_u))
    g_query, g_key, g_value, g_out = call(unpack_attention, [part32] * 4, *gather_packs(total_a))

    def local(values, size):
        out = jnp.zeros((4, 4, size), f32)
        return lax.dynamic_update_slice(out, values.reshape(4, 1, size), (0, quarter, 0)).reshape(4, -1)

    per = width // 4
    vector = [local(sums_q[0, i * 256 : (i + 1) * 256], 64) for i in range(3)]
    for item in (sums_b[2], sums_f[1], sums_a[0], sums_b[1], sums_b[0], sums_f[0]):
        vector.append(item.reshape(4, per))
    vector.append(local(sums_ua[0] + sums_ub[0], 256))
    vector = jnp.concatenate(vector, 1)
    for bit in (CORE, X, Y):
        vector = vector + swap(vector, bit)
    pieces = [lax.dynamic_index_in_dim(vector, (place + step) % 4, 0, True) for step in range(4)]
    pieces = [pieces[0]] + [shift(pieces[step], step) for step in (1, 2, 3)]
    small = call(
        split_small, [shaped(1, 256, kind=f32)] * 9 + [shaped(1, 1024, kind=f32)], *pieces
    )
    small = [item.reshape(-1) for item in small]
    return (
        layer_output,
        input_gradient,
        g_query,
        small[0],
        g_key,
        small[1],
        g_value,
        small[2],
        g_out,
        small[3],
        g_up,
        small[9],
        g_down,
        small[4],
        small[5],
        small[6],
        small[7],
        small[8],
    )


def solution(mesh):
    replicas, shards = mesh.shape["rep"], mesh.shape["shard"]
    fits = shards == 4 and replicas == 8 and HEADS % 16 == 0
    return jax.shard_map(
        fast_device if fits else general_device,
        mesh=mesh,
        in_specs=(
            P(("rep", "shard"), None),
            P("shard", None),
            P("shard"),
            P("shard", None),
            P("shard"),
            P("shard", None),
            P("shard"),
            P("shard", None),
            P("shard"),
            P("shard", None),
            P("shard"),
            P("shard", None),
            P("shard"),
            P("shard"),
            P("shard"),
            P("shard"),
            P("shard"),
            P(("rep", "shard"), None),
        ),
        out_specs=(
            P(("rep", "shard"), None),
            P(("rep", "shard"), None),
            P("shard", None),
            P("shard"),
            P("shard", None),
            P("shard"),
            P("shard", None),
            P("shard"),
            P("shard", None),
            P("shard"),
            P("shard", None),
            P("shard"),
            P("shard", None),
            P("shard"),
            P("shard"),
            P("shard"),
            P("shard"),
            P("shard"),
        ),
        check_vma=False,
    )
```

```python
import functools
import math

import jax
import jax.numpy as jnp
import numpy as np
from jax import lax
from jax.experimental import pallas as pl
from jax.experimental.pallas import tpu as pltpu
from jax.sharding import PartitionSpec as P

HEADS = 16


norm_epsilon = 1e-05


def normalize(values):
    centered = values - jnp.mean(values, axis=-1, keepdims=True)
    inverse = lax.rsqrt(jnp.mean(centered * centered, axis=-1, keepdims=True) + norm_epsilon)
    return (centered * inverse, inverse)


def norm_back(normed, inverse, upstream):
    return inverse * (
        upstream
        - jnp.mean(upstream, axis=-1, keepdims=True)
        - normed * jnp.mean(upstream * normed, axis=-1, keepdims=True)
    )


def rotation(positions, head_dim):
    half_dim = head_dim // 2
    freqs = 10000.0 ** (-jnp.arange(half_dim, dtype=jnp.float32) / half_dim)
    angles = positions.astype(jnp.float32)[:, None] * freqs[None, :]
    return (jnp.cos(angles)[:, None, :], jnp.sin(angles)[:, None, :])


def rotate(tensor, cosines, sines, sign):
    half_dim = tensor.shape[-1] // 2
    first = tensor[..., :half_dim]
    second = tensor[..., half_dim:]
    return jnp.concatenate(
        [first * cosines - sign * second * sines, second * cosines + sign * first * sines], axis=-1
    )


def col_sum(values):
    return jnp.sum(values.astype(jnp.float32), axis=0)


def general_device(
    layer_input,
    query_weight,
    query_bias,
    key_weight,
    key_bias,
    value_weight,
    value_bias,
    output_weight,
    output_bias,
    up_weight,
    up_bias,
    down_weight,
    down_bias,
    attention_gain_in,
    attention_gain_out,
    feedforward_gain_in,
    feedforward_gain_out,
    layer_cotangent,
):
    rows = layer_input.shape[0]
    width = layer_input.shape[1]
    heads = HEADS
    head_dim = width // heads
    seq_rows = rows * lax.axis_size("shard")
    factor = head_dim ** (-0.5)
    positions = lax.axis_index("shard") * rows + jnp.arange(rows, dtype=jnp.int32)
    cosines, sines = rotation(positions, head_dim)
    attention_local = (
        query_weight,
        key_weight,
        value_weight,
        output_weight,
        query_bias,
        key_bias,
        value_bias,
        output_bias,
        attention_gain_in,
        attention_gain_out,
    )
    feed_local = (
        up_weight,
        up_bias,
        down_weight,
        down_bias,
        feedforward_gain_in,
        feedforward_gain_out,
    )
    attention_full = (
        lax.all_gather(attention_local[0], "shard", axis=0, tiled=True),
        lax.all_gather(attention_local[1], "shard", axis=0, tiled=True),
        lax.all_gather(attention_local[2], "shard", axis=0, tiled=True),
        lax.all_gather(attention_local[3], "shard", axis=0, tiled=True),
        lax.all_gather(attention_local[4], "shard", axis=0, tiled=True),
        lax.all_gather(attention_local[5], "shard", axis=0, tiled=True),
        lax.all_gather(attention_local[6], "shard", axis=0, tiled=True),
        lax.all_gather(attention_local[7], "shard", axis=0, tiled=True),
        lax.all_gather(attention_local[8], "shard", axis=0, tiled=True),
        lax.all_gather(attention_local[9], "shard", axis=0, tiled=True),
    )
    (
        query_mat,
        key_mat,
        value_mat,
        out_mat,
        query_shift,
        key_shift,
        value_shift,
        out_shift,
        gain_in_a,
        gain_out_a,
    ) = attention_full
    residual_in = layer_input.astype(jnp.float32)
    normed_a, inverse_a = normalize(residual_in)
    hidden_a = (normed_a * gain_in_a.astype(jnp.float32)).astype(jnp.bfloat16)

    def project(matrix, shift):
        return jnp.dot(hidden_a, matrix, preferred_element_type=jnp.float32) + shift.astype(
            jnp.float32
        )

    query_heads = rotate(
        project(query_mat, query_shift).reshape(rows, heads, head_dim), cosines, sines, 1.0
    ).astype(jnp.bfloat16)
    key_rows = (
        rotate(project(key_mat, key_shift).reshape(rows, heads, head_dim), cosines, sines, 1.0)
        .astype(jnp.bfloat16)
        .reshape(rows, width)
    )
    value_rows = project(value_mat, value_shift).astype(jnp.bfloat16)
    start_state = (
        jnp.full((heads, rows), -1e30, jnp.float32),
        jnp.zeros((heads, rows), jnp.float32),
        jnp.zeros((heads, rows, head_dim), jnp.float32),
    )
    key_piece = lax.all_gather(key_rows, "shard", axis=0, tiled=True)
    value_piece = lax.all_gather(value_rows, "shard", axis=0, tiled=True)
    count = key_piece.shape[0]
    block = math.gcd(count, 512)

    def forward_inner(index, state):
        best, total, accum = state
        offset = index * block
        key_block = lax.dynamic_slice_in_dim(key_piece, offset, block, 0).reshape(
            block, heads, head_dim
        )
        value_block = lax.dynamic_slice_in_dim(value_piece, offset, block, 0).reshape(
            block, heads, head_dim
        )
        key_pos = offset + jnp.arange(block, dtype=jnp.int32)
        allowed = key_pos[None, None, :] <= positions[None, :, None]
        scores = (
            jnp.einsum("qhd,khd->hqk", query_heads, key_block, preferred_element_type=jnp.float32)
            * factor
        )
        scores = jnp.where(allowed, scores, -1e30)
        newest = jnp.maximum(best, jnp.max(scores, axis=-1))
        weights = jnp.where(allowed, jnp.exp(scores - newest[..., None]), 0.0)
        decay = jnp.exp(best - newest)
        total = total * decay + jnp.sum(weights, axis=-1)
        accum = accum * decay[..., None] + jnp.einsum(
            "hqk,khd->hqd",
            weights.astype(jnp.bfloat16),
            value_block,
            preferred_element_type=jnp.float32,
        )
        return (newest, total, accum)

    best, total, accum = lax.fori_loop(0, count // block, forward_inner, start_state)
    logsum = best + jnp.log(total)
    attended = (
        jnp.transpose(accum / total[..., None], (1, 0, 2)).reshape(rows, width).astype(jnp.bfloat16)
    )
    branch_a = jnp.dot(attended, out_mat, preferred_element_type=jnp.float32) + out_shift.astype(
        jnp.float32
    )
    normed_o, inverse_o = normalize(branch_a)
    middle = residual_in + normed_o * gain_out_a.astype(jnp.float32)
    feed_full = (
        lax.all_gather(feed_local[0], "shard", axis=0, tiled=True),
        lax.all_gather(feed_local[1], "shard", axis=0, tiled=True),
        lax.all_gather(feed_local[2], "shard", axis=0, tiled=True),
        lax.all_gather(feed_local[3], "shard", axis=0, tiled=True),
        lax.all_gather(feed_local[4], "shard", axis=0, tiled=True),
        lax.all_gather(feed_local[5], "shard", axis=0, tiled=True),
    )
    up_mat, up_shift, down_mat, down_shift, gain_in_f, gain_out_f = feed_full
    normed_f, inverse_f = normalize(middle)
    hidden_f = (normed_f * gain_in_f.astype(jnp.float32)).astype(jnp.bfloat16)
    pre_act = jnp.dot(hidden_f, up_mat, preferred_element_type=jnp.float32) + up_shift.astype(
        jnp.float32
    )
    activated = jax.nn.gelu(pre_act).astype(jnp.bfloat16)
    branch_f = jnp.dot(activated, down_mat, preferred_element_type=jnp.float32) + down_shift.astype(
        jnp.float32
    )
    normed_d, inverse_d = normalize(branch_f)
    layer_output = (middle + normed_d * gain_out_f.astype(jnp.float32)).astype(jnp.bfloat16)
    feed_back = (
        lax.all_gather(feed_local[0], "shard", axis=0, tiled=True),
        lax.all_gather(feed_local[1], "shard", axis=0, tiled=True),
        lax.all_gather(feed_local[2], "shard", axis=0, tiled=True),
        lax.all_gather(feed_local[3], "shard", axis=0, tiled=True),
        lax.all_gather(feed_local[4], "shard", axis=0, tiled=True),
        lax.all_gather(feed_local[5], "shard", axis=0, tiled=True),
    )
    up_back, up_unused, down_back, down_unused, gain_in_fb, gain_out_fb = feed_back
    upstream = layer_cotangent.astype(jnp.float32)
    grad_gain_out_f = jnp.sum(upstream * normed_d, axis=0)
    d_branch_f = norm_back(normed_d, inverse_d, upstream * gain_out_fb.astype(jnp.float32)).astype(
        jnp.bfloat16
    )
    grad_down = jnp.einsum("tf,td->fd", activated, d_branch_f, preferred_element_type=jnp.float32)
    grad_down_shift = col_sum(d_branch_f)
    d_activated = jnp.einsum("td,fd->tf", d_branch_f, down_back, preferred_element_type=jnp.float32)
    gelu_out, gelu_pull = jax.vjp(jax.nn.gelu, pre_act)
    d_pre = gelu_pull(d_activated)[0].astype(jnp.bfloat16)
    grad_up = jnp.einsum("td,tf->df", hidden_f, d_pre, preferred_element_type=jnp.float32)
    grad_up_shift = col_sum(d_pre)
    d_hidden_f = jnp.einsum("tf,df->td", d_pre, up_back, preferred_element_type=jnp.float32)
    grad_gain_in_f = jnp.sum(d_hidden_f * normed_f, axis=0)
    d_middle = upstream + norm_back(
        normed_f, inverse_f, d_hidden_f * gain_in_fb.astype(jnp.float32)
    )
    feed_grads = (
        lax.psum_scatter(
            grad_up.astype(jnp.bfloat16), "shard", scatter_dimension=0, tiled=True
        ).astype(jnp.float32),
        lax.psum_scatter(
            grad_up_shift.astype(jnp.bfloat16), "shard", scatter_dimension=0, tiled=True
        ).astype(jnp.float32),
        lax.psum_scatter(
            grad_down.astype(jnp.bfloat16), "shard", scatter_dimension=0, tiled=True
        ).astype(jnp.float32),
        lax.psum_scatter(
            grad_down_shift.astype(jnp.bfloat16), "shard", scatter_dimension=0, tiled=True
        ).astype(jnp.float32),
        lax.psum_scatter(
            grad_gain_in_f.astype(jnp.bfloat16), "shard", scatter_dimension=0, tiled=True
        ).astype(jnp.float32),
        lax.psum_scatter(
            grad_gain_out_f.astype(jnp.bfloat16), "shard", scatter_dimension=0, tiled=True
        ).astype(jnp.float32),
    )
    attention_back = (
        lax.all_gather(attention_local[0], "shard", axis=0, tiled=True),
        lax.all_gather(attention_local[1], "shard", axis=0, tiled=True),
        lax.all_gather(attention_local[2], "shard", axis=0, tiled=True),
        lax.all_gather(attention_local[3], "shard", axis=0, tiled=True),
        lax.all_gather(attention_local[4], "shard", axis=0, tiled=True),
        lax.all_gather(attention_local[5], "shard", axis=0, tiled=True),
        lax.all_gather(attention_local[6], "shard", axis=0, tiled=True),
        lax.all_gather(attention_local[7], "shard", axis=0, tiled=True),
        lax.all_gather(attention_local[8], "shard", axis=0, tiled=True),
        lax.all_gather(attention_local[9], "shard", axis=0, tiled=True),
    )
    (
        query_back,
        key_back,
        value_back,
        out_back,
        qshift_unused,
        kshift_unused,
        vshift_unused,
        oshift_unused,
        gain_in_ab,
        gain_out_ab,
    ) = attention_back
    grad_gain_out_a = jnp.sum(d_middle * normed_o, axis=0)
    d_branch_a = norm_back(normed_o, inverse_o, d_middle * gain_out_ab.astype(jnp.float32)).astype(
        jnp.bfloat16
    )
    grad_out_mat = jnp.einsum("td,te->de", attended, d_branch_a, preferred_element_type=jnp.float32)
    grad_out_shift = col_sum(d_branch_a)
    d_attended = jnp.einsum(
        "te,de->td", d_branch_a, out_back, preferred_element_type=jnp.float32
    ).astype(jnp.bfloat16)
    d_heads = d_attended.reshape(rows, heads, head_dim)
    row_delta = jnp.einsum(
        "qhd,qhd->hq",
        d_heads.astype(jnp.float32),
        attended.reshape(rows, heads, head_dim).astype(jnp.float32),
    )

    def query_terms(key_block, value_block, key_pos):
        allowed = key_pos[None, None, :] <= positions[None, :, None]
        scores = (
            jnp.einsum("qhd,khd->hqk", query_heads, key_block, preferred_element_type=jnp.float32)
            * factor
        )
        probs = jnp.where(allowed, jnp.exp(scores - logsum[..., None]), 0.0)
        d_probs = jnp.einsum(
            "qhd,khd->hqk", d_heads, value_block, preferred_element_type=jnp.float32
        )
        d_scores = (probs * (d_probs - row_delta[..., None])).astype(jnp.bfloat16)
        return (probs, d_scores)

    back_state = (
        jnp.zeros((rows, heads, head_dim), jnp.float32),
        jnp.zeros((seq_rows, width), jnp.float32),
        jnp.zeros((seq_rows, width), jnp.float32),
    )
    backward_key_piece = lax.all_gather(key_rows, "shard", axis=0, tiled=True)
    backward_value_piece = lax.all_gather(value_rows, "shard", axis=0, tiled=True)
    count = backward_key_piece.shape[0]
    backward_block = math.gcd(count, 512)

    def backward_inner(index, state):
        grad_query, grad_keys, grad_values = state
        offset = index * backward_block
        key_block = lax.dynamic_slice_in_dim(backward_key_piece, offset, backward_block, 0).reshape(
            backward_block, heads, head_dim
        )
        value_block = lax.dynamic_slice_in_dim(
            backward_value_piece, offset, backward_block, 0
        ).reshape(backward_block, heads, head_dim)
        key_pos = offset + jnp.arange(backward_block, dtype=jnp.int32)
        probs, d_scores = query_terms(key_block, value_block, key_pos)
        grad_query = (
            grad_query
            + jnp.einsum("hqk,khd->qhd", d_scores, key_block, preferred_element_type=jnp.float32)
            * factor
        )
        key_grad = (
            jnp.einsum("hqk,qhd->khd", d_scores, query_heads, preferred_element_type=jnp.float32)
            * factor
        )
        value_grad = jnp.einsum(
            "hqk,qhd->khd", probs.astype(jnp.bfloat16), d_heads, preferred_element_type=jnp.float32
        )
        grad_keys = lax.dynamic_update_slice_in_dim(
            grad_keys, key_grad.reshape(backward_block, width), offset, 0
        )
        grad_values = lax.dynamic_update_slice_in_dim(
            grad_values, value_grad.reshape(backward_block, width), offset, 0
        )
        return (grad_query, grad_keys, grad_values)

    back_result = lax.fori_loop(0, count // backward_block, backward_inner, back_state)
    grad_query = back_result[0]
    key_total, value_total = (
        lax.psum_scatter(
            back_result[1].astype(jnp.bfloat16), "shard", scatter_dimension=0, tiled=True
        ).astype(jnp.float32),
        lax.psum_scatter(
            back_result[2].astype(jnp.bfloat16), "shard", scatter_dimension=0, tiled=True
        ).astype(jnp.float32),
    )
    d_query = rotate(grad_query, cosines, sines, -1.0).reshape(rows, width).astype(jnp.bfloat16)
    d_key = (
        rotate(key_total.reshape(rows, heads, head_dim), cosines, sines, -1.0)
        .reshape(rows, width)
        .astype(jnp.bfloat16)
    )
    d_value = value_total.astype(jnp.bfloat16)
    grad_query_mat = jnp.einsum("td,te->de", hidden_a, d_query, preferred_element_type=jnp.float32)
    grad_key_mat = jnp.einsum("td,te->de", hidden_a, d_key, preferred_element_type=jnp.float32)
    grad_value_mat = jnp.einsum("td,te->de", hidden_a, d_value, preferred_element_type=jnp.float32)
    d_hidden_a = jnp.einsum("te,de->td", d_query, query_back, preferred_element_type=jnp.float32)
    d_hidden_a = d_hidden_a + jnp.einsum(
        "te,de->td", d_key, key_back, preferred_element_type=jnp.float32
    )
    d_hidden_a = d_hidden_a + jnp.einsum(
        "te,de->td", d_value, value_back, preferred_element_type=jnp.float32
    )
    grad_gain_in_a = jnp.sum(d_hidden_a * normed_a, axis=0)
    input_gradient = d_middle + norm_back(
        normed_a, inverse_a, d_hidden_a * gain_in_ab.astype(jnp.float32)
    )
    attention_grads = (
        lax.psum_scatter(
            grad_query_mat.astype(jnp.bfloat16), "shard", scatter_dimension=0, tiled=True
        ).astype(jnp.float32),
        lax.psum_scatter(
            grad_key_mat.astype(jnp.bfloat16), "shard", scatter_dimension=0, tiled=True
        ).astype(jnp.float32),
        lax.psum_scatter(
            grad_value_mat.astype(jnp.bfloat16), "shard", scatter_dimension=0, tiled=True
        ).astype(jnp.float32),
        lax.psum_scatter(
            grad_out_mat.astype(jnp.bfloat16), "shard", scatter_dimension=0, tiled=True
        ).astype(jnp.float32),
        lax.psum_scatter(
            col_sum(d_query).astype(jnp.bfloat16), "shard", scatter_dimension=0, tiled=True
        ).astype(jnp.float32),
        lax.psum_scatter(
            col_sum(d_key).astype(jnp.bfloat16), "shard", scatter_dimension=0, tiled=True
        ).astype(jnp.float32),
        lax.psum_scatter(
            col_sum(d_value).astype(jnp.bfloat16), "shard", scatter_dimension=0, tiled=True
        ).astype(jnp.float32),
        lax.psum_scatter(
            grad_out_shift.astype(jnp.bfloat16), "shard", scatter_dimension=0, tiled=True
        ).astype(jnp.float32),
        lax.psum_scatter(
            grad_gain_in_a.astype(jnp.bfloat16), "shard", scatter_dimension=0, tiled=True
        ).astype(jnp.float32),
        lax.psum_scatter(
            grad_gain_out_a.astype(jnp.bfloat16), "shard", scatter_dimension=0, tiled=True
        ).astype(jnp.float32),
    )
    (
        g_query,
        g_key,
        g_value,
        g_out,
        g_qshift,
        g_kshift,
        g_vshift,
        g_oshift,
        g_gain_in_a,
        g_gain_out_a,
    ) = attention_grads
    g_up, g_up_shift, g_down, g_down_shift, g_gain_in_f, g_gain_out_f = feed_grads
    summed = (
        lax.psum(g_query.astype(jnp.bfloat16), "rep").astype(jnp.float32),
        lax.psum(g_qshift.astype(jnp.bfloat16), "rep").astype(jnp.float32),
        lax.psum(g_key.astype(jnp.bfloat16), "rep").astype(jnp.float32),
        lax.psum(g_kshift.astype(jnp.bfloat16), "rep").astype(jnp.float32),
        lax.psum(g_value.astype(jnp.bfloat16), "rep").astype(jnp.float32),
        lax.psum(g_vshift.astype(jnp.bfloat16), "rep").astype(jnp.float32),
        lax.psum(g_out.astype(jnp.bfloat16), "rep").astype(jnp.float32),
        lax.psum(g_oshift.astype(jnp.bfloat16), "rep").astype(jnp.float32),
        lax.psum(g_up.astype(jnp.bfloat16), "rep").astype(jnp.float32),
        lax.psum(g_up_shift.astype(jnp.bfloat16), "rep").astype(jnp.float32),
        lax.psum(g_down.astype(jnp.bfloat16), "rep").astype(jnp.float32),
        lax.psum(g_down_shift.astype(jnp.bfloat16), "rep").astype(jnp.float32),
        lax.psum(g_gain_in_a.astype(jnp.bfloat16), "rep").astype(jnp.float32),
        lax.psum(g_gain_out_a.astype(jnp.bfloat16), "rep").astype(jnp.float32),
        lax.psum(g_gain_in_f.astype(jnp.bfloat16), "rep").astype(jnp.float32),
        lax.psum(g_gain_out_f.astype(jnp.bfloat16), "rep").astype(jnp.float32),
    )
    return (
        layer_output,
        input_gradient,
        summed[0],
        summed[1],
        summed[2],
        summed[3],
        summed[4],
        summed[5],
        summed[6],
        summed[7],
        summed[8],
        summed[9],
        summed[10],
        summed[11],
        summed[12],
        summed[13],
        summed[14],
        summed[15],
    )


CORE, X, Y = 1, 2, 4
GROUP = 4
BLOCK = 256


def swap(values, bit):
    count = lax.axis_size("rep")
    return lax.ppermute(values, "rep", [(i, i ^ bit) for i in range(count)])


def shift(values, step):
    count = lax.axis_size("shard")
    return lax.ppermute(values, "shard", [(i, (i + step) % count) for i in range(count)])


def flip(values, bit):
    count = lax.axis_size("shard")
    return lax.ppermute(values, "shard", [(i, i ^ bit) for i in range(count)])


def token_pairs(count):
    pairs = []
    for rep in range(count):
        for z in range(GROUP):
            there = (rep & ~3) | ((z & 1) << 1) | (z >> 1)
            pairs.append((rep * GROUP + z, there * GROUP + ((rep >> 1) & 1) + 2 * (rep & 1)))
    return pairs


def spot():
    rep, place = lax.axis_index("rep"), lax.axis_index("shard")
    return rep & 3, place, rep >> 2, ((rep >> 1) & 1) + 2 * (rep & 1)


def aligned(index, size):
    return pl.ds(pl.multiple_of(index * size, size), size)


def dot(left, right):
    return jnp.dot(left, right, preferred_element_type=jnp.float32)


def nt(left, right):
    return lax.dot_general(left, right, (((1,), (1,)), ((), ())), preferred_element_type=jnp.float32)


def tn(left, right):
    return lax.dot_general(left, right, (((0,), (0,)), ((), ())), preferred_element_type=jnp.float32)


def rounded(values):
    return values.astype(jnp.bfloat16)


def wide(values):
    return values.astype(jnp.float32)


def shaped(*dims, kind=jnp.bfloat16):
    return jax.ShapeDtypeStruct(dims, kind)


VMEM_SPEC = pl.BlockSpec(memory_space=pltpu.VMEM)


def call(kernel, outs, *operands, scratch=(), flops=0, exps=0, room=6):
    size = lambda items: sum(math.prod(item.shape) * item.dtype.itemsize for item in items)
    moved = size(operands) + size(outs)
    spaces = [jax.ShapeDtypeStruct(item.shape, item.dtype) for item in scratch]
    return pl.pallas_call(
        kernel,
        out_shape=tuple(outs),
        in_specs=[VMEM_SPEC] * len(operands),
        out_specs=tuple([VMEM_SPEC] * len(outs)),
        scratch_shapes=list(scratch),
        compiler_params=pltpu.CompilerParams(vmem_limit_bytes=moved + size(spaces) + (room << 20)),
        cost_estimate=pl.CostEstimate(flops=flops, bytes_accessed=moved, transcendentals=exps),
        name=kernel.__name__,
    )(*operands)


def standardize(values):
    centered = values - jnp.mean(values, axis=-1, keepdims=True)
    inverse = lax.rsqrt(jnp.mean(centered * centered, axis=-1, keepdims=True) + norm_epsilon)
    return centered * inverse, inverse


def turn(values, cosines, sines):
    lane = lax.broadcasted_iota(jnp.int32, values.shape, 1)
    swapped = jnp.where(lane % 64 < 32, pltpu.roll(values, 96, 1), pltpu.roll(values, 32, 1))
    return values * cosines + swapped * sines


def rope_tables(tokens, head_dim):
    half = head_dim // 2
    freqs = 10000.0 ** (-jnp.arange(half, dtype=jnp.float32) / half)
    angles = jnp.arange(tokens, dtype=jnp.int32).astype(jnp.float32)[:, None] * freqs[None, :]
    cosines, sines = jnp.cos(angles), jnp.sin(angles)
    return (
        jnp.concatenate([cosines] * 4, 1),
        jnp.concatenate([-sines, sines, -sines, sines], 1),
    )


def pack_attention(
    query_weight, key_weight, value_weight, out_weight, qb, kb, vb, ub, ob, db, ga, gb, gc, gd, packed
):
    quarter, place, _, _ = spot()
    row = lax.broadcasted_iota(jnp.int32, (1024, 256), 0)
    col = lax.broadcasted_iota(jnp.int32, (1024, 256), 1)
    chosen = rounded(wide(row == (col // 64) * 256 + quarter * 64 + col % 64))
    for index, weight in enumerate((query_weight, key_weight, value_weight)):
        mine = rounded(dot(weight[...], chosen))
        for half in range(2):
            packed[half, :128, index * 256 : index * 256 + 256] = mine[half * 128 : half * 128 + 128]
    out_mine = out_weight[aligned(quarter, 64), :]
    for j in range(4):
        at = (j % 2) * 64
        packed[j // 2, at : at + 64, 768:1024] = out_mine[:, j * 256 : j * 256 + 256]
    row = lax.broadcasted_iota(jnp.int32, (256, 256), 0)
    col = lax.broadcasted_iota(jnp.int32, (256, 256), 1)
    chosen = rounded(wide((row == quarter * 64 + col % 64) & (col // 64 == place)))
    biases = [dot(jnp.broadcast_to(item[...][None, :], (16, 256)), chosen) for item in (qb, kb, vb)]
    full = lambda item: jnp.broadcast_to(wide(item[...])[None, :], (16, 256))
    up_mine = jnp.broadcast_to(wide(ub[aligned(quarter, 256)])[None, :], (16, 256))
    zero = jnp.zeros((16, 256), jnp.float32)
    first = jnp.concatenate(biases + [zero], 1)
    second = jnp.concatenate([up_mine, full(ob), full(db), zero], 1)
    third = jnp.concatenate([full(ga), full(gb), full(gc), full(gd)], 1)
    at = lax.broadcasted_iota(jnp.int32, (16, 1024), 0)
    rows = jnp.where(at == 0, first, jnp.where(at == 1, second, jnp.where(at == 2, third, 0.0)))
    for half in range(2):
        packed[half, 128:144, :] = rounded(rows)


def pack_feed(up_weight, down_weight, up_packed, down_packed, sems):
    quarter, _, _, _ = spot()
    copies = []
    for half in range(2):
        for there in range(4):
            lanes = pl.ds(pl.multiple_of(there * 1024 + quarter * 256, 256), 256)
            copies.append(
                (
                    up_weight.at[half * 128 : half * 128 + 128, lanes],
                    up_packed.at[half, :, there * 256 : there * 256 + 256],
                )
            )
        copies.append((down_weight.at[aligned(quarter * 2 + half, 128), :], down_packed.at[half]))
    copies = [pltpu.make_async_copy(a, b, sems.at[i]) for i, (a, b) in enumerate(copies)]
    for copy in copies:
        copy.start()
    for copy in copies:
        copy.wait()


def call_pack_feed(up_weight, down_weight):
    spec = pl.BlockSpec(memory_space=pl.ANY)
    return pl.pallas_call(
        pack_feed,
        out_shape=(shaped(2, 128, 1024), shaped(2, 128, 1024)),
        in_specs=[spec, spec],
        out_specs=(VMEM_SPEC, VMEM_SPEC),
        scratch_shapes=[pltpu.SemaphoreType.DMA((10,))],
        compiler_params=pltpu.CompilerParams(vmem_limit_bytes=8 << 20),
        cost_estimate=pl.CostEstimate(flops=0, bytes_accessed=2 << 20, transcendentals=0),
        name="pack_feed",
    )(up_weight, down_weight)


def tie(value, *earlier):
    return lax.optimization_barrier((value, *earlier))[0]


def near_pieces(packed, half, *earlier, direct=False):
    mine = tie(lax.dynamic_index_in_dim(packed, half, 0, False), *earlier)
    if direct:
        return [flip(mine, step) for step in (1, 2, 3)]
    second = flip(mine, 2)
    return [flip(mine, 1), second, flip(second, 1)]


def far_pieces(near):
    return [swap(item, Y) for item in near]


def far_together(near):
    return swap(jnp.stack(near), Y)


def each_piece(own, near, far):
    _, place, y_bit, _ = spot()
    yield place, 0, own.at[0]
    yield place, 1, own.at[1]
    for step in (1, 2, 3):
        yield place ^ step, y_bit, near[step - 1]
        yield place ^ step, 1 - y_bit, far[step - 1]


def head_lanes(shape, parity):
    return (lax.broadcasted_iota(jnp.int32, shape, 1) // 64) == parity


def causal_block():
    shape = (BLOCK, BLOCK)
    return lax.broadcasted_iota(jnp.int32, shape, 0) >= lax.broadcasted_iota(jnp.int32, shape, 1)


def attend(
    x0, x1, x2, x3, own, z1, z2, z3, y1, y2, y3, cosines, sines,
    query, key, value, mixed, logs, hidden, qkv, out_rows, vectors, p0, p1, p32,
):
    _, _, _, position = spot()
    for relative, rows_in in enumerate((x0, x1, x2, x3)):
        hidden[aligned(position ^ relative, BLOCK), :] = rows_in[...]
    vectors[...] = jnp.zeros_like(vectors)
    for index, (shard, half, piece) in enumerate(each_piece(own, (z1, z2, z3), (y1, y2, y3))):
        qkv[aligned(shard * 2 + half, 128), :] = piece[:128, :768]
        for j in range(2):
            out_rows[aligned(shard, 64), aligned(half * 2 + j, 256)] = piece[j * 64 : j * 64 + 64, 768:]
        if index == 0 or index >= 2 and index % 2 == 0:
            small = wide(piece[128:144, :])
            lanes = aligned(shard, 256)
            vectors[0:1, lanes] = small[1:2, 256:512]
            vectors[1:2, lanes] = small[1:2, 512:768]
            for gain in range(4):
                vectors[2 + gain : 3 + gain, lanes] = small[2:3, gain * 256 : gain * 256 + 256]
            vectors[6:7, lanes] = small[1:2, :256]
            vectors[7:8, :] += small[0:1, :]

    def project(index, carry):
        rows = aligned(index, BLOCK)
        normed, _ = standardize(wide(hidden[rows, :]))
        block = rounded(normed * vectors[2:3, :])
        hidden[rows, :] = block
        raw = dot(block, qkv[...]) + vectors[7:8, :768]
        cos, sin = cosines[rows, :], sines[rows, :]
        for tile in range(2):
            at = tile * 128
            lanes = slice(at, at + 128)
            query[rows, lanes] = rounded(turn(raw[:, lanes], cos, sin)) * jnp.bfloat16(0.125)
            key[rows, lanes] = rounded(turn(raw[:, 256 + at : 384 + at], cos, sin))
        value[rows, :] = rounded(raw[:, 512:])
        return carry

    lax.fori_loop(0, GROUP, project, 0)
    causal = causal_block()
    logs[...] = jnp.zeros_like(logs)

    def pair_step(pair, carry):
        lanes = aligned(pair, 128)
        lane = lax.broadcasted_iota(jnp.int32, (BLOCK, 128), 1)
        for block in range(GROUP):
            rows = slice(block * BLOCK, block * BLOCK + BLOCK)
            seen = (block + 1) * BLOCK
            queries = query[rows, lanes]
            keys, values = key[:seen, lanes], value[:seen, lanes]
            outs = []
            log_rows = logs[rows, :]
            for parity in range(2):
                masked = jnp.where(head_lanes(queries.shape, parity), queries, jnp.bfloat16(0))
                scores = nt(masked, keys)
                last = jnp.where(causal, scores[:, seen - BLOCK :], -1e30)
                scores = jnp.concatenate([scores[:, : seen - BLOCK], last], 1) if block else last
                best = jnp.max(scores, axis=1, keepdims=True)
                exps = jnp.exp(scores - best)
                total = jnp.sum(exps, axis=1, keepdims=True)
                outs.append(dot(rounded(exps), values) / total)
                log_rows = jnp.where(lane == pair * 2 + parity, best + jnp.log(total), log_rows)
            mixed[rows, lanes] = rounded(jnp.where(lane < 64, outs[0], outs[1]))
            logs[rows, :] = log_rows
        return carry

    lax.fori_loop(0, 2, pair_step, 0)
    for relative, part in enumerate((p0, p1, p32.at[BLOCK:], p32.at[:BLOCK])):
        part[...] = rounded(dot(mixed[aligned(position ^ relative, BLOCK), :], out_rows[...]))


def pair_back(pair, query, key, value, mixed, logs, d_out, d_query, d_key, d_value):
    lanes = slice(pair * 128, pair * 128 + 128)
    causal = causal_block()
    d_key[...] = jnp.zeros_like(d_key)
    d_value[...] = jnp.zeros_like(d_value)
    for block in range(GROUP):
        rows = slice(block * BLOCK, block * BLOCK + BLOCK)
        seen = (block + 1) * BLOCK
        queries, d_outs = query[rows, lanes], d_out[rows, lanes]
        keys, values = key[:seen, lanes], value[:seen, lanes]
        products = wide(d_outs) * wide(mixed[rows, lanes])
        log_rows = logs[rows, :]
        lane = lax.broadcasted_iota(jnp.int32, (BLOCK, 128), 1)
        d_queries = []
        for parity in range(2):
            mine = head_lanes((BLOCK, 128), parity)
            masked_q = jnp.where(mine, queries, jnp.bfloat16(0))
            masked_d = jnp.where(mine, d_outs, jnp.bfloat16(0))
            log = jnp.sum(jnp.where(lane == pair * 2 + parity, log_rows, 0.0), 1, keepdims=True)
            delta = jnp.sum(jnp.where(mine, products, 0.0), 1, keepdims=True)
            probs = jnp.exp(nt(masked_q, keys) - log)
            last = jnp.where(causal, probs[:, seen - BLOCK :], 0.0)
            probs = jnp.concatenate([probs[:, : seen - BLOCK], last], 1) if block else last
            d_scores = rounded(probs * (nt(masked_d, values) - delta))
            d_queries.append(dot(d_scores, keys))
            d_value[:seen, :] += tn(rounded(probs), masked_d)
            d_key[:seen, :] += tn(d_scores, masked_q)
        d_query[rows, :] = jnp.where(lane < 64, d_queries[0], d_queries[1])


def finish_back(cosines, sines, d_query, d_key, d_value, grads, shift_sums):
    shift_sums[...] = jnp.zeros_like(shift_sums)

    def finish(index, carry):
        rows = aligned(index, BLOCK)
        cos, sin = cosines[rows, :], -sines[rows, :]
        grads[rows, :128] = rounded(turn(d_query[rows, :] * 0.125, cos, sin))
        grads[rows, 128:256] = rounded(turn(d_key[rows, :], cos, sin))
        grads[rows, 256:] = rounded(d_value[rows, :])
        shift_sums[0:1, :] += jnp.sum(wide(grads[rows, :]), axis=0, keepdims=True)
        return carry

    lax.fori_loop(0, GROUP, finish, 0)


def attend_back_first(
    a0, a1, a2, a3, out_rows, query, key, value, mixed, logs, cosines, sines,
    d_out, grads, shift_sums, d_query, d_key, d_value,
):
    _, _, _, position = spot()
    for relative, rows_in in enumerate((a0, a1, a2, a3)):
        d_out[aligned(position ^ relative, BLOCK), :] = rounded(nt(rows_in[...], out_rows[...]))
    pair_back(0, query, key, value, mixed, logs, d_out, d_query, d_key, d_value)
    finish_back(cosines, sines, d_query, d_key, d_value, grads, shift_sums)


def attend_back_second(
    d_out, before, qkv, query, key, value, mixed, logs, cosines, sines,
    grads, shift_sums, p0, p1, p32, d_query, d_key, d_value, joined,
):
    _, _, _, position = spot()
    pair_back(1, query, key, value, mixed, logs, d_out, d_query, d_key, d_value)
    finish_back(cosines, sines, d_query, d_key, d_value, grads, shift_sums)
    for index in range(3):
        joined[:, index * 256 : index * 256 + 128] = before[:, index * 128 : index * 128 + 128]
        joined[:, index * 256 + 128 : index * 256 + 256] = grads[:, index * 128 : index * 128 + 128]
    for relative, part in enumerate((p0, p1, p32.at[BLOCK:], p32.at[:BLOCK])):
        part[...] = rounded(nt(joined[aligned(position ^ relative, BLOCK), :], qkv[...]))


def after_attention(p0, core_in, x_in, rows_in, vectors, middle, hidden, normed_o, normed_f, inverses):
    branch = wide(p0[...]) + wide(core_in[BLOCK:, :]) + wide(x_in[...]) + vectors[0:1, :]
    normed, inverse_o = standardize(branch)
    normed_o[...] = normed
    total = wide(rows_in[...]) + normed * vectors[3:4, :]
    middle[...] = total
    normed, inverse_f = standardize(total)
    normed_f[...] = normed
    hidden[...] = rounded(normed * vectors[4:5, :])
    lane = lax.broadcasted_iota(jnp.int32, inverses.shape, 1)
    inverses[...] = jnp.where(lane < 64, inverse_o, inverse_f)


def after_feed(p0, core_in, x_in, middle, cotangent, vectors, layer_out, d_branch, sums):
    branch = wide(p0[...]) + wide(core_in[BLOCK:, :]) + wide(x_in[...]) + vectors[1:2, :]
    normed, inverse = standardize(branch)
    gain = vectors[5:6, :]
    layer_out[...] = rounded(middle[...] + normed * gain)
    upstream = wide(cotangent[...])
    back = rounded(norm_back(normed, inverse, upstream * gain))
    d_branch[...] = back
    sums[...] = jnp.zeros_like(sums)
    sums[0:1, :] = jnp.sum(upstream * normed, axis=0, keepdims=True)
    sums[1:2, :] = jnp.sum(wide(back), axis=0, keepdims=True)


def after_feed_back(
    p0, core_in, x_in, cotangent, normed_o, normed_f, inverses, vectors, d_middle, d_branch, sums
):
    d_hidden = wide(p0[...]) + wide(core_in[BLOCK:, :]) + wide(x_in[...])
    normed = normed_f[...]
    sums[...] = jnp.zeros_like(sums)
    sums[0:1, :] = jnp.sum(d_hidden * normed, axis=0, keepdims=True)
    total = wide(cotangent[...]) + norm_back(normed, inverses[:, 64:65], d_hidden * vectors[4:5, :])
    d_middle[...] = total
    normed = normed_o[...]
    sums[1:2, :] = jnp.sum(total * normed, axis=0, keepdims=True)
    back = rounded(norm_back(normed, inverses[:, 0:1], total * vectors[3:4, :]))
    d_branch[...] = back
    sums[2:3, :] = jnp.sum(wide(back), axis=0, keepdims=True)


def gain_in_sums(p0, p1, p32, x0, x1, x2, x3, sums):
    sums[...] = jnp.zeros_like(sums)
    parts = (p0, p1, p32.at[BLOCK:], p32.at[:BLOCK])
    for part, rows_in in zip(parts, (x0, x1, x2, x3), strict=True):
        normed, _ = standardize(wide(rows_in[...]))
        sums[0:1, :] += jnp.sum(wide(part[...]) * normed, axis=0, keepdims=True)


def after_attention_back(p0, core_in, x_in, rows_in, d_middle, vectors, d_rows):
    d_hidden = wide(p0[...]) + wide(core_in[BLOCK:, :]) + wide(x_in[...])
    normed, inverse = standardize(wide(rows_in[...]))
    d_rows[...] = rounded(d_middle[...] + norm_back(normed, inverse, d_hidden * vectors[2:3, :]))


GELU_SCALE = math.sqrt(2.0 / math.pi)


def feed_rows(rows_in, up_mat, down_mat, vectors, before, after, part, at):
    rows = slice(at, at + BLOCK)

    def step(index, carry):
        lanes = aligned(index, BLOCK)
        raw = dot(rows_in[...], up_mat[:, lanes]) + vectors[6:7, lanes]
        before[rows, lanes] = raw
        after[rows, lanes] = rounded(jax.nn.gelu(raw))
        return carry

    lax.fori_loop(0, 4, step, 0)

    def out(index, carry):
        lanes = aligned(index, BLOCK)
        part[:, lanes] = rounded(dot(after[rows, :], down_mat[:, lanes]))
        return carry

    lax.fori_loop(0, 4, out, 0)


def feed_first(
    h0, h2, uo, u1, u2, u3, far_u, do, d1, d2, d3, far_d, vectors,
    up_mat, down_mat, before, after, p0, p2,
):
    for shard, half, piece in each_piece(uo, (u1, u2, u3), [far_u.at[i] for i in range(3)]):
        up_mat[aligned(shard * 2 + half, 128), :] = piece[...]
    for shard, half, piece in each_piece(do, (d1, d2, d3), [far_d.at[i] for i in range(3)]):
        down_mat[aligned(shard * 2 + half, 128), :] = piece[...]
    feed_rows(h0, up_mat, down_mat, vectors, before, after, p0, 0)
    feed_rows(h2, up_mat, down_mat, vectors, before, after, p2, BLOCK)


def feed_second(h1, h3, p2, up_mat, down_mat, vectors, before, after, p1, p32):
    p32[BLOCK:, :] = p2[...]
    feed_rows(h3, up_mat, down_mat, vectors, before, after, p32.at[:BLOCK], BLOCK)
    feed_rows(h1, up_mat, down_mat, vectors, before, after, p1, 0)


def feed_back_rows(rows_in, up_mat, down_mat, before, d_pre, part, sums, at):
    rows = slice(at, at + BLOCK)

    def step(index, carry):
        lanes = aligned(index, BLOCK)
        upstream = nt(rows_in[...], down_mat[lanes, :])
        raw = before[rows, lanes]
        square = raw * raw
        bent = jnp.tanh(GELU_SCALE * raw * (1.0 + 0.044715 * square))
        slope = 0.5 * (1.0 + bent) + 0.5 * GELU_SCALE * raw * (1.0 - bent * bent) * (
            1.0 + 3.0 * 0.044715 * square
        )
        back = rounded(upstream * slope)
        d_pre[rows, lanes] = back
        sums[0:1, lanes] += jnp.sum(wide(back), axis=0, keepdims=True)
        return carry

    lax.fori_loop(0, 4, step, 0)

    def out(index, carry):
        lanes = aligned(index, BLOCK)
        part[:, lanes] = rounded(nt(d_pre[rows, :], up_mat[lanes, :]))
        return carry

    lax.fori_loop(0, 4, out, 0)


def feed_back_first(m0, m2, up_mat, down_mat, before, d_pre, p0, p2, sums):
    sums[...] = jnp.zeros_like(sums)
    feed_back_rows(m0, up_mat, down_mat, before, d_pre, p0, sums, 0)
    feed_back_rows(m2, up_mat, down_mat, before, d_pre, p2, sums, BLOCK)


def feed_back_second(m1, m3, p2, up_mat, down_mat, before, sums_in, d_pre, p1, p32, sums):
    sums[...] = sums_in[...]
    p32[BLOCK:, :] = p2[...]
    feed_back_rows(m3, up_mat, down_mat, before, d_pre, p32.at[:BLOCK], sums, BLOCK)
    feed_back_rows(m1, up_mat, down_mat, before, d_pre, p1, sums, 0)


def put_halves(keep, send, step, at, top, bottom):
    _, _, y_bit, _ = spot()

    @pl.when(y_bit == 0)
    def _():
        keep[step, at : at + 128, :] = top
        send[step, at : at + 128, :] = bottom

    @pl.when(y_bit == 1)
    def _():
        keep[step, at : at + 128, :] = bottom
        send[step, at : at + 128, :] = top


def down_grads(first, second, m0, m1, m2, m3, keep, send):
    _, place, _, _ = spot()

    def one(step, carry):
        lanes = aligned(place ^ step, BLOCK)
        down = (
            tn(first[:BLOCK, lanes], m0[...])
            + tn(first[BLOCK:, lanes], m2[...])
            + tn(second[:BLOCK, lanes], m1[...])
            + tn(second[BLOCK:, lanes], m3[...])
        )
        down = rounded(down)
        put_halves(keep, send, step, 0, down[:128], down[128:])
        return carry

    lax.fori_loop(0, 4, one, 0)


def up_grads(h0, h1, h2, h3, u_first, u_second, keep, send):
    _, place, _, _ = spot()

    def one(step, carry):
        lanes = aligned(place ^ step, BLOCK)
        up = (
            tn(h0[:, lanes], u_first[:BLOCK, :])
            + tn(h2[:, lanes], u_first[BLOCK:, :])
            + tn(h1[:, lanes], u_second[:BLOCK, :])
            + tn(h3[:, lanes], u_second[BLOCK:, :])
        )
        up = rounded(up)
        put_halves(keep, send, step, 0, up[:128], up[128:])
        return carry

    lax.fori_loop(0, 4, one, 0)


def attention_grads_first(mixed, a0, a1, a2, a3, hidden, grads, keep, send, out_grad, block):
    _, place, _, position = spot()
    total = tn(mixed[aligned(position, BLOCK), :], a0[...])
    for relative, rows_in in ((1, a1), (2, a2), (3, a3)):
        total = total + tn(mixed[aligned(position ^ relative, BLOCK), :], rows_in[...])
    out_grad[...] = rounded(total)

    def one(step, carry):
        shard = place ^ step
        block[:, :384] = rounded(tn(hidden[:, aligned(shard, BLOCK)], grads[...]))
        mine = out_grad[aligned(shard, 64), :]
        for j in range(4):
            block[j * 64 : j * 64 + 64, 384:] = mine[:, j * 256 : j * 256 + 256]
        put_halves(keep, send, step, 0, block[:128, :], block[128:, :])
        return carry

    lax.fori_loop(0, 4, one, 0)


def attention_grads_second(
    hidden, grads, sums_f, sums_b, sums_a, sums_u, sums_q, sums_r, keep, send
):
    _, place, y_bit, _ = spot()

    def one(step, carry):
        shard = place ^ step
        block = rounded(tn(hidden[:, aligned(shard, BLOCK)], grads[...]))
        put_halves(keep, send, step, 0, block[:128], block[128:])
        lanes = aligned(shard, BLOCK)
        biases = []
        for index in range(3):
            at = index * 128
            pair = jnp.where(shard < 2, sums_q[0:1, at : at + 128], sums_r[0:1, at : at + 128])
            biases.append(jnp.where((shard & 1) == 0, pair[:, :64], pair[:, 64:]))
        zero = jnp.zeros((1, 192), jnp.float32)
        tops = [sums_b[2:3, lanes], sums_f[1:2, lanes], sums_a[0:1, lanes], *biases, zero]
        lows = [sums_b[1:2, lanes], sums_b[0:1, lanes], sums_f[0:1, lanes], sums_u[0:1, lanes], zero[:, :128]]
        halves = []
        for items in (tops, lows):
            flat = jnp.concatenate(items, 1)
            row = lax.broadcasted_iota(jnp.int32, (8, 384), 0)
            full = [jnp.broadcast_to(flat[:, i * 384 : i * 384 + 384], (8, 384)) for i in range(3)]
            rows = jnp.where(row == 0, full[0], jnp.where(row == 1, full[1], full[2]))
            halves.append(rounded(jnp.where(row < 3, rows, 0.0)))
        mine, other = jnp.where(y_bit == 0, halves[0], halves[1]), jnp.where(y_bit == 0, halves[1], halves[0])
        keep[step, 128:136, :] = mine
        send[step, 128:136, :] = other
        return carry

    lax.fori_loop(0, 4, one, 0)


def add_pairs(keep, come, stay, go):
    for step, out in enumerate((stay.at[0], go.at[0], stay.at[1], go.at[1])):
        out[...] = rounded(wide(keep[step]) + wide(come[step]))


def add_near(stay, come, own, go):
    own[...] = rounded(wide(stay[0]) + wide(come[0]))
    go[...] = rounded(wide(stay[1]) + wide(come[1]))


def each_part(own, x_part, y_part, core_part):
    rep = lax.axis_index("rep")
    refs = [own, x_part, y_part.at[0], y_part.at[1]] + [core_part.at[i] for i in range(4)]
    for relative, ref in enumerate(refs):
        flip = ((relative & 1) << 1) | ((relative & 2) << 1) | (relative >> 2)
        there = rep ^ flip
        yield there >> 2, there & 3, ref


def unpack_down(own, x_part, y_part, core_part, down):
    for y_bit, quarter, ref in each_part(own, x_part, y_part, core_part):
        down[aligned(quarter * 2 + y_bit, 128), :] = wide(ref[...])


def unpack_up(own, x_part, y_part, core_part, up):
    for y_bit, quarter, ref in each_part(own, x_part, y_part, core_part):
        for there in range(4):
            lanes = pl.ds(pl.multiple_of(there * 1024 + quarter * 256, 256), 256)
            up[aligned(y_bit, 128), lanes] = wide(ref[:, there * 256 : there * 256 + 256])


def unpack_attention(
    own, x_part, y_part, core_part, own2, x_part2, y_part2, core_part2,
    query, key, value, out_weight, qb, kb, vb, ob, db, ga, gb, gc, gd, ub,
):
    first = list(each_part(own, x_part, y_part, core_part))
    second = list(each_part(own2, x_part2, y_part2, core_part2))
    row = lax.broadcasted_iota(jnp.int32, (128, 512), 0)
    col = lax.broadcasted_iota(jnp.int32, (128, 512), 1)
    sets = ((0, 1, 4, 5), (2, 3, 6, 7))
    chosen = []
    for index in sets[0]:
        quarter = first[index][1]
        chosen.append(rounded(wide(col == (row // 64) * 256 + quarter * 64 + row % 64)))
    chosen = jnp.concatenate(chosen, 0)
    for pair, parts in enumerate((first, second)):
        for members in sets:
            rows = aligned(parts[members[0]][0], 128)
            for index, out in enumerate((query, key, value)):
                lanes = slice(index * 128, index * 128 + 128)
                joined = jnp.concatenate([parts[i][2][:128, lanes] for i in members], 1)
                out[rows, pair * 512 : pair * 512 + 512] = dot(joined, chosen)
    for y_bit, quarter, ref in first:
        for j in range(2):
            out_weight[aligned(quarter, 64), aligned(y_bit * 2 + j, 256)] = wide(
                ref[j * 64 : j * 64 + 64, 384:]
            )
    y_bit = first[0][0]
    flats = []
    for members in sets:
        rows = [wide(second[i][2][128:136, :]) for i in members]
        total = rows[0] + rows[1] + rows[2] + rows[3]
        flats.append((total, rows))
    mine, other = flats
    for half, (outs, size) in enumerate((((ob, db, ga), 64), ((gb, gc, gd), 256))):
        take = y_bit == half
        total = jnp.where(take, mine[0], other[0])
        flat = jnp.concatenate([total[0:1, :], total[1:2, :]], 1)
        for index, out in enumerate(outs):
            out[...] = flat[:, index * 256 : index * 256 + 256]
        locals_ = [jnp.where(take, a, b)[2:3, :] for a, b in zip(mine[1], other[1], strict=True)]
        quarters = [first[i][1] for i in sets[0]]
        for there in range(4):
            value_at = jnp.zeros((1, 384), jnp.float32)
            for quarter, item in zip(quarters, locals_, strict=True):
                value_at = value_at + jnp.where(quarter == there, item, 0.0)
            if half == 0:
                for index, out in enumerate((qb, kb, vb)):
                    out[:, there * 64 : there * 64 + 64] = value_at[:, index * 64 : index * 64 + 64]
            else:
                ub[:, there * 256 : there * 256 + 256] = value_at[:, :256]


def sum_pairs(keep, come):
    two = shaped(2, *keep.shape[1:])
    return call(add_pairs, [two, two], keep, come)


def sum_near(stay, come):
    one = shaped(*stay.shape[1:])
    return call(add_near, [one, one], stay, come)


def sum_far(own, come):
    return rounded(wide(own) + wide(come))


def gather_packs(total):
    x_part = swap(total, X)
    two = jnp.stack([total, x_part])
    y_part = swap(two, Y)
    return total, x_part, y_part, swap(jnp.concatenate([two, y_part]), CORE)


def fast_device(
    layer_input,
    query_weight,
    query_bias,
    key_weight,
    key_bias,
    value_weight,
    value_bias,
    output_weight,
    output_bias,
    up_weight,
    up_bias,
    down_weight,
    down_bias,
    attention_gain_in,
    attention_gain_out,
    feedforward_gain_in,
    feedforward_gain_out,
    layer_cotangent,
):
    f32, bf16 = jnp.float32, jnp.bfloat16
    replicas = lax.axis_size("rep")
    rows, width = layer_input.shape
    tokens = rows * GROUP
    quarter, place, y_bit, _ = spot()
    pairs = token_pairs(replicas)
    back_pairs = [(there, here) for here, there in pairs]
    both = ("rep", "shard")
    part = shaped(rows, width)
    part32 = shaped(rows, width, kind=f32)
    sums = shaped(8, width, kind=f32)

    def spread(piece):
        near, far = swap(piece, X), swap(piece, CORE)
        return piece, near, far, swap(near, CORE)

    def gather_sum(p1, p32):
        core_in = swap(p32, CORE)
        return core_in, swap(rounded(wide(p1) + wide(core_in[:rows])), X)

    own_rows = lax.ppermute(layer_input, both, pairs)
    (packed,) = call(
        pack_attention,
        [shaped(2, 144, width)],
        query_weight,
        key_weight,
        value_weight,
        output_weight,
        query_bias,
        key_bias,
        value_bias,
        up_bias,
        output_bias,
        down_bias,
        attention_gain_in,
        attention_gain_out,
        feedforward_gain_in,
        feedforward_gain_out,
    )
    near_a = near_pieces(packed, y_bit)
    cosines, sines = rope_tables(tokens, 64)
    up_packed, down_packed = call_pack_feed(up_weight, down_weight)
    own_rows = tie(own_rows, packed, cosines, sines, up_packed)
    blocks = spread(own_rows)
    far_a = far_pieces(near_a)
    near_u = near_pieces(up_packed, y_bit, *near_a, direct=True)
    two16 = shaped(2 * rows, width)
    head_rows = shaped(tokens, 256)
    query, key, value, mixed, logs, hidden_a, qkv, out_rows, vectors, p0, p1, p32 = call(
        attend,
        [head_rows] * 4
        + [
            shaped(tokens, 128, kind=f32),
            shaped(tokens, width),
            shaped(width, 768),
            shaped(256, width),
            sums,
        ]
        + [part, part, two16],
        *blocks,
        packed,
        *near_a,
        *far_a,
        cosines,
        sines,
        flops=2 * tokens * 1024 * 1024 + 8 * tokens * tokens * 64 * 2,
        exps=2 * tokens * tokens,
        room=14,
    )
    p32 = tie(p32, *near_u)
    far_u = far_together(near_u)
    near_d = near_pieces(down_packed, y_bit, *near_u, direct=True)
    core_in, x_in = gather_sum(p1, p32)
    x_in = tie(x_in, far_u, *near_d)
    far_d = far_together(near_d)
    cotangent = lax.ppermute(tie(layer_cotangent, *near_d), both, pairs)
    middle, hidden_own, normed_o, normed_f, inverses = call(
        after_attention,
        [part32, part, part32, part32, shaped(rows, 128, kind=f32)],
        p0,
        core_in,
        x_in,
        own_rows,
        vectors,
    )
    h0, h1, h2, h3 = spread(hidden_own)
    h2 = tie(h2, cotangent)
    two32 = shaped(2 * rows, width, kind=f32)
    square = shaped(width, width)
    flops = 4 * 2 * rows * 1024 * 1024
    up_mat, down_mat, before_a, after_a, p0, p2 = call(
        feed_first,
        [square, square, two32, two16, part, part],
        h0, h2, up_packed, *near_u, far_u, down_packed, *near_d, far_d, vectors,
        flops=flops, room=10,
    )
    before_b, after_b, p1, p32 = call(
        feed_second,
        [two32, two16, part, two16],
        h1, h3, p2, up_mat, down_mat, vectors,
        flops=flops, room=10,
    )
    core_in, x_in = gather_sum(p1, p32)
    layer_output, d_branch, sums_f = call(
        after_feed, [part, part, sums], p0, core_in, x_in, middle, cotangent, vectors
    )
    m0, m1, m2, m3 = spread(d_branch)
    layer_output = lax.ppermute(layer_output, both, back_pairs)
    u_first, p0, p2, sums_u = call(
        feed_back_first,
        [two16, part, part, sums],
        m0, m2, up_mat, down_mat, before_a,
        flops=flops, room=10,
    )
    u_second, p1, p32, sums_u = call(
        feed_back_second,
        [two16, part, two16, sums],
        m1, m3, p2, up_mat, down_mat, before_b, sums_u,
        flops=flops, room=10,
    )
    core_in, x_in = gather_sum(p1, p32)
    packs = [shaped(4, 128, width)] * 2
    flops = 2 * tokens * 1024 * 1024
    pack_d = call(
        down_grads, packs, after_a, tie(after_b, layer_output), m0, m1, m2, m3, flops=flops, room=10
    )
    pack_u = call(up_grads, packs, h0, h1, h2, h3, u_first, u_second, flops=flops, room=10)
    x_in = tie(x_in, *pack_d, *pack_u)
    d_middle, d_branch, sums_b = call(
        after_feed_back,
        [part32, part, sums],
        p0,
        core_in,
        x_in,
        cotangent,
        normed_o,
        normed_f,
        inverses,
        vectors,
    )
    a0, a1, a2, a3 = spread(d_branch)
    stay_d, go_d = sum_pairs(tie(pack_d[0], d_branch), swap(pack_d[1], Y))
    a1 = tie(a1, go_d)
    a_blocks = a0, a1, a2, a3
    come_d = flip(go_d, 1)
    come_u = swap(pack_u[1], Y)
    grad32 = [pltpu.VMEM((tokens, 128), f32)] * 3
    back_flops = tokens * 1024 * 1024 + 10 * tokens * tokens * 64 * 2
    d_out, grads_first, sums_q = call(
        attend_back_first,
        [shaped(tokens, 256), shaped(tokens, 384), shaped(8, 384, kind=f32)],
        *a_blocks, out_rows, query, key, value, mixed, logs, cosines, sines,
        scratch=grad32, flops=back_flops, exps=tokens * tokens, room=14,
    )
    pack_a = call(
        attention_grads_first,
        [shaped(4, 128, 640)] * 2,
        mixed, *a_blocks, hidden_a, grads_first,
        scratch=[pltpu.VMEM((256, width), bf16), pltpu.VMEM((256, 640), bf16)],
        flops=flops // 2, room=10,
    )
    grads_second, sums_r, p0, p1, p32 = call(
        attend_back_second,
        [shaped(tokens, 384), shaped(8, 384, kind=f32), part, part, two16],
        tie(d_out, *pack_a), grads_first, qkv, query, key, value, mixed, logs, cosines, sines,
        scratch=grad32 + [pltpu.VMEM((tokens, 768), bf16)],
        flops=back_flops, exps=tokens * tokens, room=14,
    )
    own_d, go_d = sum_near(tie(stay_d, *pack_a), come_d)
    come_a = swap(pack_a[1], Y)
    p32 = tie(p32, come_u, go_d)
    core_in, x_in = gather_sum(p1, p32)
    come_d = flip(go_d, 2)
    stay_u, go_u = sum_pairs(tie(pack_u[0], p32), come_u)
    (sums_a,) = call(gain_in_sums, [sums], p0, p1, p32, *blocks)
    pack_b = call(
        attention_grads_second,
        [shaped(4, 136, 384)] * 2,
        hidden_a, grads_second, sums_f, sums_b, sums_a, sums_u, sums_q, sums_r,
        flops=flops // 2, room=10,
    )
    x_in = tie(x_in, *pack_b, go_u)
    (d_rows,) = call(
        after_attention_back, [part], p0, core_in, x_in, own_rows, d_middle, vectors
    )
    input_gradient = lax.ppermute(d_rows, both, back_pairs)
    total_d = sum_far(tie(own_d, d_rows), come_d)
    own_u, go_u = sum_near(tie(stay_u, d_rows), flip(go_u, 1))
    stay_a, go_a = sum_pairs(tie(pack_a[0], d_rows), come_a)
    own_a, go_a = sum_near(stay_a, flip(go_a, 1))
    stay_b, go_b = sum_pairs(pack_b[0], swap(pack_b[1], Y))
    total_u = sum_far(own_u, flip(go_u, 2))
    own_b, go_b = sum_near(stay_b, flip(go_b, 1))
    total_a = sum_far(own_a, flip(go_a, 2))
    total_b = sum_far(own_b, flip(go_b, 2))
    (g_down,) = call(unpack_down, [shaped(*down_weight.shape, kind=f32)], *gather_packs(total_d))
    (g_up,) = call(unpack_up, [shaped(*up_weight.shape, kind=f32)], *gather_packs(total_u))
    packs_a = gather_packs(total_a)
    packs_b = gather_packs(total_b)
    g_query, g_key, g_value, g_out, *small = call(
        unpack_attention,
        [part32] * 4 + [shaped(1, 256, kind=f32)] * 9 + [shaped(1, 1024, kind=f32)],
        *packs_a,
        *packs_b,
    )
    small = [item.reshape(-1) for item in small]
    input_gradient = input_gradient.astype(f32)
    return (
        layer_output,
        input_gradient,
        g_query,
        small[0],
        g_key,
        small[1],
        g_value,
        small[2],
        g_out,
        small[3],
        g_up,
        small[9],
        g_down,
        small[4],
        small[5],
        small[6],
        small[7],
        small[8],
    )


def solution(mesh):
    replicas, shards = mesh.shape["rep"], mesh.shape["shard"]
    fits = shards == 4 and replicas == 8 and HEADS % 16 == 0
    return jax.shard_map(
        fast_device if fits else general_device,
        mesh=mesh,
        in_specs=(
            P(("rep", "shard"), None),
            P("shard", None),
            P("shard"),
            P("shard", None),
            P("shard"),
            P("shard", None),
            P("shard"),
            P("shard", None),
            P("shard"),
            P("shard", None),
            P("shard"),
            P("shard", None),
            P("shard"),
            P("shard"),
            P("shard"),
            P("shard"),
            P("shard"),
            P(("rep", "shard"), None),
        ),
        out_specs=(
            P(("rep", "shard"), None),
            P(("rep", "shard"), None),
            P("shard", None),
            P("shard"),
            P("shard", None),
            P("shard"),
            P("shard", None),
            P("shard"),
            P("shard", None),
            P("shard"),
            P("shard", None),
            P("shard"),
            P("shard", None),
            P("shard"),
            P("shard"),
            P("shard"),
            P("shard"),
            P("shard"),
        ),
        check_vma=False,
    )
```

```python
import functools
import math

import jax
import jax.numpy as jnp
import numpy as np
from jax import lax
from jax.experimental import pallas as pl
from jax.experimental.pallas import tpu as pltpu
from jax.sharding import PartitionSpec as P

HEADS = 16


norm_epsilon = 1e-05


def normalize(values):
    centered = values - jnp.mean(values, axis=-1, keepdims=True)
    inverse = lax.rsqrt(jnp.mean(centered * centered, axis=-1, keepdims=True) + norm_epsilon)
    return (centered * inverse, inverse)


def norm_back(normed, inverse, upstream):
    return inverse * (
        upstream
        - jnp.mean(upstream, axis=-1, keepdims=True)
        - normed * jnp.mean(upstream * normed, axis=-1, keepdims=True)
    )


def rotation(positions, head_dim):
    half_dim = head_dim // 2
    freqs = 10000.0 ** (-jnp.arange(half_dim, dtype=jnp.float32) / half_dim)
    angles = positions.astype(jnp.float32)[:, None] * freqs[None, :]
    return (jnp.cos(angles)[:, None, :], jnp.sin(angles)[:, None, :])


def rotate(tensor, cosines, sines, sign):
    half_dim = tensor.shape[-1] // 2
    first = tensor[..., :half_dim]
    second = tensor[..., half_dim:]
    return jnp.concatenate(
        [first * cosines - sign * second * sines, second * cosines + sign * first * sines], axis=-1
    )


def col_sum(values):
    return jnp.sum(values.astype(jnp.float32), axis=0)


def general_device(
    layer_input,
    query_weight,
    query_bias,
    key_weight,
    key_bias,
    value_weight,
    value_bias,
    output_weight,
    output_bias,
    up_weight,
    up_bias,
    down_weight,
    down_bias,
    attention_gain_in,
    attention_gain_out,
    feedforward_gain_in,
    feedforward_gain_out,
    layer_cotangent,
):
    rows = layer_input.shape[0]
    width = layer_input.shape[1]
    heads = HEADS
    head_dim = width // heads
    seq_rows = rows * lax.axis_size("shard")
    factor = head_dim ** (-0.5)
    positions = lax.axis_index("shard") * rows + jnp.arange(rows, dtype=jnp.int32)
    cosines, sines = rotation(positions, head_dim)
    attention_local = (
        query_weight,
        key_weight,
        value_weight,
        output_weight,
        query_bias,
        key_bias,
        value_bias,
        output_bias,
        attention_gain_in,
        attention_gain_out,
    )
    feed_local = (
        up_weight,
        up_bias,
        down_weight,
        down_bias,
        feedforward_gain_in,
        feedforward_gain_out,
    )
    attention_full = (
        lax.all_gather(attention_local[0], "shard", axis=0, tiled=True),
        lax.all_gather(attention_local[1], "shard", axis=0, tiled=True),
        lax.all_gather(attention_local[2], "shard", axis=0, tiled=True),
        lax.all_gather(attention_local[3], "shard", axis=0, tiled=True),
        lax.all_gather(attention_local[4], "shard", axis=0, tiled=True),
        lax.all_gather(attention_local[5], "shard", axis=0, tiled=True),
        lax.all_gather(attention_local[6], "shard", axis=0, tiled=True),
        lax.all_gather(attention_local[7], "shard", axis=0, tiled=True),
        lax.all_gather(attention_local[8], "shard", axis=0, tiled=True),
        lax.all_gather(attention_local[9], "shard", axis=0, tiled=True),
    )
    (
        query_mat,
        key_mat,
        value_mat,
        out_mat,
        query_shift,
        key_shift,
        value_shift,
        out_shift,
        gain_in_a,
        gain_out_a,
    ) = attention_full
    residual_in = layer_input.astype(jnp.float32)
    normed_a, inverse_a = normalize(residual_in)
    hidden_a = (normed_a * gain_in_a.astype(jnp.float32)).astype(jnp.bfloat16)

    def project(matrix, shift):
        return jnp.dot(hidden_a, matrix, preferred_element_type=jnp.float32) + shift.astype(
            jnp.float32
        )

    query_heads = rotate(
        project(query_mat, query_shift).reshape(rows, heads, head_dim), cosines, sines, 1.0
    ).astype(jnp.bfloat16)
    key_rows = (
        rotate(project(key_mat, key_shift).reshape(rows, heads, head_dim), cosines, sines, 1.0)
        .astype(jnp.bfloat16)
        .reshape(rows, width)
    )
    value_rows = project(value_mat, value_shift).astype(jnp.bfloat16)
    start_state = (
        jnp.full((heads, rows), -1e30, jnp.float32),
        jnp.zeros((heads, rows), jnp.float32),
        jnp.zeros((heads, rows, head_dim), jnp.float32),
    )
    key_piece = lax.all_gather(key_rows, "shard", axis=0, tiled=True)
    value_piece = lax.all_gather(value_rows, "shard", axis=0, tiled=True)
    count = key_piece.shape[0]
    block = math.gcd(count, 512)

    def forward_inner(index, state):
        best, total, accum = state
        offset = index * block
        key_block = lax.dynamic_slice_in_dim(key_piece, offset, block, 0).reshape(
            block, heads, head_dim
        )
        value_block = lax.dynamic_slice_in_dim(value_piece, offset, block, 0).reshape(
            block, heads, head_dim
        )
        key_pos = offset + jnp.arange(block, dtype=jnp.int32)
        allowed = key_pos[None, None, :] <= positions[None, :, None]
        scores = (
            jnp.einsum("qhd,khd->hqk", query_heads, key_block, preferred_element_type=jnp.float32)
            * factor
        )
        scores = jnp.where(allowed, scores, -1e30)
        newest = jnp.maximum(best, jnp.max(scores, axis=-1))
        weights = jnp.where(allowed, jnp.exp(scores - newest[..., None]), 0.0)
        decay = jnp.exp(best - newest)
        total = total * decay + jnp.sum(weights, axis=-1)
        accum = accum * decay[..., None] + jnp.einsum(
            "hqk,khd->hqd",
            weights.astype(jnp.bfloat16),
            value_block,
            preferred_element_type=jnp.float32,
        )
        return (newest, total, accum)

    best, total, accum = lax.fori_loop(0, count // block, forward_inner, start_state)
    logsum = best + jnp.log(total)
    attended = (
        jnp.transpose(accum / total[..., None], (1, 0, 2)).reshape(rows, width).astype(jnp.bfloat16)
    )
    branch_a = jnp.dot(attended, out_mat, preferred_element_type=jnp.float32) + out_shift.astype(
        jnp.float32
    )
    normed_o, inverse_o = normalize(branch_a)
    middle = residual_in + normed_o * gain_out_a.astype(jnp.float32)
    feed_full = (
        lax.all_gather(feed_local[0], "shard", axis=0, tiled=True),
        lax.all_gather(feed_local[1], "shard", axis=0, tiled=True),
        lax.all_gather(feed_local[2], "shard", axis=0, tiled=True),
        lax.all_gather(feed_local[3], "shard", axis=0, tiled=True),
        lax.all_gather(feed_local[4], "shard", axis=0, tiled=True),
        lax.all_gather(feed_local[5], "shard", axis=0, tiled=True),
    )
    up_mat, up_shift, down_mat, down_shift, gain_in_f, gain_out_f = feed_full
    normed_f, inverse_f = normalize(middle)
    hidden_f = (normed_f * gain_in_f.astype(jnp.float32)).astype(jnp.bfloat16)
    pre_act = jnp.dot(hidden_f, up_mat, preferred_element_type=jnp.float32) + up_shift.astype(
        jnp.float32
    )
    activated = jax.nn.gelu(pre_act).astype(jnp.bfloat16)
    branch_f = jnp.dot(activated, down_mat, preferred_element_type=jnp.float32) + down_shift.astype(
        jnp.float32
    )
    normed_d, inverse_d = normalize(branch_f)
    layer_output = (middle + normed_d * gain_out_f.astype(jnp.float32)).astype(jnp.bfloat16)
    feed_back = (
        lax.all_gather(feed_local[0], "shard", axis=0, tiled=True),
        lax.all_gather(feed_local[1], "shard", axis=0, tiled=True),
        lax.all_gather(feed_local[2], "shard", axis=0, tiled=True),
        lax.all_gather(feed_local[3], "shard", axis=0, tiled=True),
        lax.all_gather(feed_local[4], "shard", axis=0, tiled=True),
        lax.all_gather(feed_local[5], "shard", axis=0, tiled=True),
    )
    up_back, up_unused, down_back, down_unused, gain_in_fb, gain_out_fb = feed_back
    upstream = layer_cotangent.astype(jnp.float32)
    grad_gain_out_f = jnp.sum(upstream * normed_d, axis=0)
    d_branch_f = norm_back(normed_d, inverse_d, upstream * gain_out_fb.astype(jnp.float32)).astype(
        jnp.bfloat16
    )
    grad_down = jnp.einsum("tf,td->fd", activated, d_branch_f, preferred_element_type=jnp.float32)
    grad_down_shift = col_sum(d_branch_f)
    d_activated = jnp.einsum("td,fd->tf", d_branch_f, down_back, preferred_element_type=jnp.float32)
    gelu_out, gelu_pull = jax.vjp(jax.nn.gelu, pre_act)
    d_pre = gelu_pull(d_activated)[0].astype(jnp.bfloat16)
    grad_up = jnp.einsum("td,tf->df", hidden_f, d_pre, preferred_element_type=jnp.float32)
    grad_up_shift = col_sum(d_pre)
    d_hidden_f = jnp.einsum("tf,df->td", d_pre, up_back, preferred_element_type=jnp.float32)
    grad_gain_in_f = jnp.sum(d_hidden_f * normed_f, axis=0)
    d_middle = upstream + norm_back(
        normed_f, inverse_f, d_hidden_f * gain_in_fb.astype(jnp.float32)
    )
    feed_grads = (
        lax.psum_scatter(
            grad_up.astype(jnp.bfloat16), "shard", scatter_dimension=0, tiled=True
        ).astype(jnp.float32),
        lax.psum_scatter(
            grad_up_shift.astype(jnp.bfloat16), "shard", scatter_dimension=0, tiled=True
        ).astype(jnp.float32),
        lax.psum_scatter(
            grad_down.astype(jnp.bfloat16), "shard", scatter_dimension=0, tiled=True
        ).astype(jnp.float32),
        lax.psum_scatter(
            grad_down_shift.astype(jnp.bfloat16), "shard", scatter_dimension=0, tiled=True
        ).astype(jnp.float32),
        lax.psum_scatter(
            grad_gain_in_f.astype(jnp.bfloat16), "shard", scatter_dimension=0, tiled=True
        ).astype(jnp.float32),
        lax.psum_scatter(
            grad_gain_out_f.astype(jnp.bfloat16), "shard", scatter_dimension=0, tiled=True
        ).astype(jnp.float32),
    )
    attention_back = (
        lax.all_gather(attention_local[0], "shard", axis=0, tiled=True),
        lax.all_gather(attention_local[1], "shard", axis=0, tiled=True),
        lax.all_gather(attention_local[2], "shard", axis=0, tiled=True),
        lax.all_gather(attention_local[3], "shard", axis=0, tiled=True),
        lax.all_gather(attention_local[4], "shard", axis=0, tiled=True),
        lax.all_gather(attention_local[5], "shard", axis=0, tiled=True),
        lax.all_gather(attention_local[6], "shard", axis=0, tiled=True),
        lax.all_gather(attention_local[7], "shard", axis=0, tiled=True),
        lax.all_gather(attention_local[8], "shard", axis=0, tiled=True),
        lax.all_gather(attention_local[9], "shard", axis=0, tiled=True),
    )
    (
        query_back,
        key_back,
        value_back,
        out_back,
        qshift_unused,
        kshift_unused,
        vshift_unused,
        oshift_unused,
        gain_in_ab,
        gain_out_ab,
    ) = attention_back
    grad_gain_out_a = jnp.sum(d_middle * normed_o, axis=0)
    d_branch_a = norm_back(normed_o, inverse_o, d_middle * gain_out_ab.astype(jnp.float32)).astype(
        jnp.bfloat16
    )
    grad_out_mat = jnp.einsum("td,te->de", attended, d_branch_a, preferred_element_type=jnp.float32)
    grad_out_shift = col_sum(d_branch_a)
    d_attended = jnp.einsum(
        "te,de->td", d_branch_a, out_back, preferred_element_type=jnp.float32
    ).astype(jnp.bfloat16)
    d_heads = d_attended.reshape(rows, heads, head_dim)
    row_delta = jnp.einsum(
        "qhd,qhd->hq",
        d_heads.astype(jnp.float32),
        attended.reshape(rows, heads, head_dim).astype(jnp.float32),
    )

    def query_terms(key_block, value_block, key_pos):
        allowed = key_pos[None, None, :] <= positions[None, :, None]
        scores = (
            jnp.einsum("qhd,khd->hqk", query_heads, key_block, preferred_element_type=jnp.float32)
            * factor
        )
        probs = jnp.where(allowed, jnp.exp(scores - logsum[..., None]), 0.0)
        d_probs = jnp.einsum(
            "qhd,khd->hqk", d_heads, value_block, preferred_element_type=jnp.float32
        )
        d_scores = (probs * (d_probs - row_delta[..., None])).astype(jnp.bfloat16)
        return (probs, d_scores)

    back_state = (
        jnp.zeros((rows, heads, head_dim), jnp.float32),
        jnp.zeros((seq_rows, width), jnp.float32),
        jnp.zeros((seq_rows, width), jnp.float32),
    )
    backward_key_piece = lax.all_gather(key_rows, "shard", axis=0, tiled=True)
    backward_value_piece = lax.all_gather(value_rows, "shard", axis=0, tiled=True)
    count = backward_key_piece.shape[0]
    backward_block = math.gcd(count, 512)

    def backward_inner(index, state):
        grad_query, grad_keys, grad_values = state
        offset = index * backward_block
        key_block = lax.dynamic_slice_in_dim(backward_key_piece, offset, backward_block, 0).reshape(
            backward_block, heads, head_dim
        )
        value_block = lax.dynamic_slice_in_dim(
            backward_value_piece, offset, backward_block, 0
        ).reshape(backward_block, heads, head_dim)
        key_pos = offset + jnp.arange(backward_block, dtype=jnp.int32)
        probs, d_scores = query_terms(key_block, value_block, key_pos)
        grad_query = (
            grad_query
            + jnp.einsum("hqk,khd->qhd", d_scores, key_block, preferred_element_type=jnp.float32)
            * factor
        )
        key_grad = (
            jnp.einsum("hqk,qhd->khd", d_scores, query_heads, preferred_element_type=jnp.float32)
            * factor
        )
        value_grad = jnp.einsum(
            "hqk,qhd->khd", probs.astype(jnp.bfloat16), d_heads, preferred_element_type=jnp.float32
        )
        grad_keys = lax.dynamic_update_slice_in_dim(
            grad_keys, key_grad.reshape(backward_block, width), offset, 0
        )
        grad_values = lax.dynamic_update_slice_in_dim(
            grad_values, value_grad.reshape(backward_block, width), offset, 0
        )
        return (grad_query, grad_keys, grad_values)

    back_result = lax.fori_loop(0, count // backward_block, backward_inner, back_state)
    grad_query = back_result[0]
    key_total, value_total = (
        lax.psum_scatter(
            back_result[1].astype(jnp.bfloat16), "shard", scatter_dimension=0, tiled=True
        ).astype(jnp.float32),
        lax.psum_scatter(
            back_result[2].astype(jnp.bfloat16), "shard", scatter_dimension=0, tiled=True
        ).astype(jnp.float32),
    )
    d_query = rotate(grad_query, cosines, sines, -1.0).reshape(rows, width).astype(jnp.bfloat16)
    d_key = (
        rotate(key_total.reshape(rows, heads, head_dim), cosines, sines, -1.0)
        .reshape(rows, width)
        .astype(jnp.bfloat16)
    )
    d_value = value_total.astype(jnp.bfloat16)
    grad_query_mat = jnp.einsum("td,te->de", hidden_a, d_query, preferred_element_type=jnp.float32)
    grad_key_mat = jnp.einsum("td,te->de", hidden_a, d_key, preferred_element_type=jnp.float32)
    grad_value_mat = jnp.einsum("td,te->de", hidden_a, d_value, preferred_element_type=jnp.float32)
    d_hidden_a = jnp.einsum("te,de->td", d_query, query_back, preferred_element_type=jnp.float32)
    d_hidden_a = d_hidden_a + jnp.einsum(
        "te,de->td", d_key, key_back, preferred_element_type=jnp.float32
    )
    d_hidden_a = d_hidden_a + jnp.einsum(
        "te,de->td", d_value, value_back, preferred_element_type=jnp.float32
    )
    grad_gain_in_a = jnp.sum(d_hidden_a * normed_a, axis=0)
    input_gradient = d_middle + norm_back(
        normed_a, inverse_a, d_hidden_a * gain_in_ab.astype(jnp.float32)
    )
    attention_grads = (
        lax.psum_scatter(
            grad_query_mat.astype(jnp.bfloat16), "shard", scatter_dimension=0, tiled=True
        ).astype(jnp.float32),
        lax.psum_scatter(
            grad_key_mat.astype(jnp.bfloat16), "shard", scatter_dimension=0, tiled=True
        ).astype(jnp.float32),
        lax.psum_scatter(
            grad_value_mat.astype(jnp.bfloat16), "shard", scatter_dimension=0, tiled=True
        ).astype(jnp.float32),
        lax.psum_scatter(
            grad_out_mat.astype(jnp.bfloat16), "shard", scatter_dimension=0, tiled=True
        ).astype(jnp.float32),
        lax.psum_scatter(
            col_sum(d_query).astype(jnp.bfloat16), "shard", scatter_dimension=0, tiled=True
        ).astype(jnp.float32),
        lax.psum_scatter(
            col_sum(d_key).astype(jnp.bfloat16), "shard", scatter_dimension=0, tiled=True
        ).astype(jnp.float32),
        lax.psum_scatter(
            col_sum(d_value).astype(jnp.bfloat16), "shard", scatter_dimension=0, tiled=True
        ).astype(jnp.float32),
        lax.psum_scatter(
            grad_out_shift.astype(jnp.bfloat16), "shard", scatter_dimension=0, tiled=True
        ).astype(jnp.float32),
        lax.psum_scatter(
            grad_gain_in_a.astype(jnp.bfloat16), "shard", scatter_dimension=0, tiled=True
        ).astype(jnp.float32),
        lax.psum_scatter(
            grad_gain_out_a.astype(jnp.bfloat16), "shard", scatter_dimension=0, tiled=True
        ).astype(jnp.float32),
    )
    (
        g_query,
        g_key,
        g_value,
        g_out,
        g_qshift,
        g_kshift,
        g_vshift,
        g_oshift,
        g_gain_in_a,
        g_gain_out_a,
    ) = attention_grads
    g_up, g_up_shift, g_down, g_down_shift, g_gain_in_f, g_gain_out_f = feed_grads
    summed = (
        lax.psum(g_query.astype(jnp.bfloat16), "rep").astype(jnp.float32),
        lax.psum(g_qshift.astype(jnp.bfloat16), "rep").astype(jnp.float32),
        lax.psum(g_key.astype(jnp.bfloat16), "rep").astype(jnp.float32),
        lax.psum(g_kshift.astype(jnp.bfloat16), "rep").astype(jnp.float32),
        lax.psum(g_value.astype(jnp.bfloat16), "rep").astype(jnp.float32),
        lax.psum(g_vshift.astype(jnp.bfloat16), "rep").astype(jnp.float32),
        lax.psum(g_out.astype(jnp.bfloat16), "rep").astype(jnp.float32),
        lax.psum(g_oshift.astype(jnp.bfloat16), "rep").astype(jnp.float32),
        lax.psum(g_up.astype(jnp.bfloat16), "rep").astype(jnp.float32),
        lax.psum(g_up_shift.astype(jnp.bfloat16), "rep").astype(jnp.float32),
        lax.psum(g_down.astype(jnp.bfloat16), "rep").astype(jnp.float32),
        lax.psum(g_down_shift.astype(jnp.bfloat16), "rep").astype(jnp.float32),
        lax.psum(g_gain_in_a.astype(jnp.bfloat16), "rep").astype(jnp.float32),
        lax.psum(g_gain_out_a.astype(jnp.bfloat16), "rep").astype(jnp.float32),
        lax.psum(g_gain_in_f.astype(jnp.bfloat16), "rep").astype(jnp.float32),
        lax.psum(g_gain_out_f.astype(jnp.bfloat16), "rep").astype(jnp.float32),
    )
    return (
        layer_output,
        input_gradient,
        summed[0],
        summed[1],
        summed[2],
        summed[3],
        summed[4],
        summed[5],
        summed[6],
        summed[7],
        summed[8],
        summed[9],
        summed[10],
        summed[11],
        summed[12],
        summed[13],
        summed[14],
        summed[15],
    )


CORE, X, Y = 1, 2, 4
GROUP = 4
BLOCK = 256


def swap(values, bit):
    count = lax.axis_size("rep")
    return lax.ppermute(values, "rep", [(i, i ^ bit) for i in range(count)])


def shift(values, step):
    count = lax.axis_size("shard")
    return lax.ppermute(values, "shard", [(i, (i + step) % count) for i in range(count)])


def flip(values, bit):
    count = lax.axis_size("shard")
    return lax.ppermute(values, "shard", [(i, i ^ bit) for i in range(count)])


def token_pairs(count):
    pairs = []
    for rep in range(count):
        for z in range(GROUP):
            there = (rep & ~3) | ((z & 1) << 1) | (z >> 1)
            pairs.append((rep * GROUP + z, there * GROUP + ((rep >> 1) & 1) + 2 * (rep & 1)))
    return pairs


def spot():
    rep, place = lax.axis_index("rep"), lax.axis_index("shard")
    return rep & 3, place, rep >> 2, ((rep >> 1) & 1) + 2 * (rep & 1)


def aligned(index, size):
    return pl.ds(pl.multiple_of(index * size, size), size)


def dot(left, right):
    return jnp.dot(left, right, preferred_element_type=jnp.float32)


def nt(left, right):
    return lax.dot_general(left, right, (((1,), (1,)), ((), ())), preferred_element_type=jnp.float32)


def tn(left, right):
    return lax.dot_general(left, right, (((0,), (0,)), ((), ())), preferred_element_type=jnp.float32)


def rounded(values):
    return values.astype(jnp.bfloat16)


def wide(values):
    return values.astype(jnp.float32)


def shaped(*dims, kind=jnp.bfloat16):
    return jax.ShapeDtypeStruct(dims, kind)


VMEM_SPEC = pl.BlockSpec(memory_space=pltpu.VMEM)


def call(kernel, outs, *operands, scratch=(), flops=0, exps=0, room=6):
    size = lambda items: sum(math.prod(item.shape) * item.dtype.itemsize for item in items)
    moved = size(operands) + size(outs)
    spaces = [jax.ShapeDtypeStruct(item.shape, item.dtype) for item in scratch]
    return pl.pallas_call(
        kernel,
        out_shape=tuple(outs),
        in_specs=[VMEM_SPEC] * len(operands),
        out_specs=tuple([VMEM_SPEC] * len(outs)),
        scratch_shapes=list(scratch),
        compiler_params=pltpu.CompilerParams(vmem_limit_bytes=moved + size(spaces) + (room << 20)),
        cost_estimate=pl.CostEstimate(flops=flops // 40, bytes_accessed=moved // 40, transcendentals=0),
        name=kernel.__name__,
    )(*operands)


def standardize(values):
    centered = values - jnp.mean(values, axis=-1, keepdims=True)
    inverse = lax.rsqrt(jnp.mean(centered * centered, axis=-1, keepdims=True) + norm_epsilon)
    return centered * inverse, inverse


def turn(values, cosines, sines):
    lane = lax.broadcasted_iota(jnp.int32, values.shape, 1)
    swapped = jnp.where(lane % 64 < 32, pltpu.roll(values, 96, 1), pltpu.roll(values, 32, 1))
    return values * cosines + swapped * sines


def rope_tables(tokens, head_dim):
    half = head_dim // 2
    freqs = 10000.0 ** (-jnp.arange(half, dtype=jnp.float32) / half)
    angles = jnp.arange(tokens, dtype=jnp.int32).astype(jnp.float32)[:, None] * freqs[None, :]
    cosines, sines = jnp.cos(angles), jnp.sin(angles)
    return (
        jnp.concatenate([cosines] * 4, 1),
        jnp.concatenate([-sines, sines, -sines, sines], 1),
    )


def pack_attention(
    query_weight, key_weight, value_weight, out_weight, qb, kb, vb, ub, ob, db, ga, gb, gc, gd, packed
):
    quarter, place, _, _ = spot()
    row = lax.broadcasted_iota(jnp.int32, (1024, 256), 0)
    col = lax.broadcasted_iota(jnp.int32, (1024, 256), 1)
    chosen = rounded(wide(row == (col // 64) * 256 + quarter * 64 + col % 64))
    for index, weight in enumerate((query_weight, key_weight, value_weight)):
        mine = rounded(dot(weight[...], chosen))
        for half in range(2):
            packed[half, :128, index * 256 : index * 256 + 256] = mine[half * 128 : half * 128 + 128]
    out_mine = out_weight[aligned(quarter, 64), :]
    for j in range(4):
        at = (j % 2) * 64
        packed[j // 2, at : at + 64, 768:1024] = out_mine[:, j * 256 : j * 256 + 256]
    row = lax.broadcasted_iota(jnp.int32, (256, 256), 0)
    col = lax.broadcasted_iota(jnp.int32, (256, 256), 1)
    chosen = rounded(wide((row == quarter * 64 + col % 64) & (col // 64 == place)))
    biases = [dot(jnp.broadcast_to(item[...][None, :], (16, 256)), chosen) for item in (qb, kb, vb)]
    full = lambda item: jnp.broadcast_to(wide(item[...])[None, :], (16, 256))
    up_mine = jnp.broadcast_to(wide(ub[aligned(quarter, 256)])[None, :], (16, 256))
    zero = jnp.zeros((16, 256), jnp.float32)
    first = jnp.concatenate(biases + [zero], 1)
    second = jnp.concatenate([up_mine, full(ob), full(db), zero], 1)
    third = jnp.concatenate([full(ga), full(gb), full(gc), full(gd)], 1)
    at = lax.broadcasted_iota(jnp.int32, (16, 1024), 0)
    rows = jnp.where(at == 0, first, jnp.where(at == 1, second, jnp.where(at == 2, third, 0.0)))
    for half in range(2):
        packed[half, 128:144, :] = rounded(rows)


def pack_feed(up_weight, down_weight, up_packed, down_packed, sems):
    quarter, _, _, _ = spot()
    copies = []
    for half in range(2):
        for there in range(4):
            lanes = pl.ds(pl.multiple_of(there * 1024 + quarter * 256, 256), 256)
            copies.append(
                (
                    up_weight.at[half * 128 : half * 128 + 128, lanes],
                    up_packed.at[half, :, there * 256 : there * 256 + 256],
                )
            )
        copies.append((down_weight.at[aligned(quarter * 2 + half, 128), :], down_packed.at[half]))
    copies = [pltpu.make_async_copy(a, b, sems.at[i]) for i, (a, b) in enumerate(copies)]
    for copy in copies:
        copy.start()
    for copy in copies:
        copy.wait()


def call_pack_feed(up_weight, down_weight):
    spec = pl.BlockSpec(memory_space=pl.ANY)
    return pl.pallas_call(
        pack_feed,
        out_shape=(shaped(2, 128, 1024), shaped(2, 128, 1024)),
        in_specs=[spec, spec],
        out_specs=(VMEM_SPEC, VMEM_SPEC),
        scratch_shapes=[pltpu.SemaphoreType.DMA((10,))],
        compiler_params=pltpu.CompilerParams(vmem_limit_bytes=8 << 20),
        cost_estimate=pl.CostEstimate(flops=0, bytes_accessed=2 << 20, transcendentals=0),
        name="pack_feed",
    )(up_weight, down_weight)


def tie(value, *earlier):
    return lax.optimization_barrier((value, *earlier))[0]


def near_pieces(packed, half, *earlier, direct=False):
    mine = tie(lax.dynamic_index_in_dim(packed, half, 0, False), *earlier)
    if direct:
        return [flip(mine, step) for step in (1, 2, 3)]
    second = flip(mine, 2)
    return [flip(mine, 1), second, flip(second, 1)]


def far_pieces(near):
    return [swap(item, Y) for item in near]


def far_together(near):
    return swap(jnp.stack(near), Y)


def each_piece(own, near, far):
    _, place, y_bit, _ = spot()
    yield place, 0, own.at[0]
    yield place, 1, own.at[1]
    for step in (1, 2, 3):
        yield place ^ step, y_bit, near[step - 1]
        yield place ^ step, 1 - y_bit, far[step - 1]


def head_lanes(shape, parity):
    return (lax.broadcasted_iota(jnp.int32, shape, 1) // 64) == parity


def causal_block():
    shape = (BLOCK, BLOCK)
    return lax.broadcasted_iota(jnp.int32, shape, 0) >= lax.broadcasted_iota(jnp.int32, shape, 1)


def attend(
    x0, x1, x2, x3, own, z1, z2, z3, y1, y2, y3, cosines, sines,
    query, key, value, mixed, logs, hidden, qkv, out_rows, vectors, p0, p1, p32,
):
    _, _, _, position = spot()
    for relative, rows_in in enumerate((x0, x1, x2, x3)):
        hidden[aligned(position ^ relative, BLOCK), :] = rows_in[...]
    vectors[...] = jnp.zeros_like(vectors)
    for index, (shard, half, piece) in enumerate(each_piece(own, (z1, z2, z3), (y1, y2, y3))):
        qkv[aligned(shard * 2 + half, 128), :] = piece[:128, :768]
        for j in range(2):
            out_rows[aligned(shard, 64), aligned(half * 2 + j, 256)] = piece[j * 64 : j * 64 + 64, 768:]
        if index == 0 or index >= 2 and index % 2 == 0:
            small = wide(piece[128:144, :])
            lanes = aligned(shard, 256)
            vectors[0:1, lanes] = small[1:2, 256:512]
            vectors[1:2, lanes] = small[1:2, 512:768]
            for gain in range(4):
                vectors[2 + gain : 3 + gain, lanes] = small[2:3, gain * 256 : gain * 256 + 256]
            vectors[6:7, lanes] = small[1:2, :256]
            vectors[7:8, :] += small[0:1, :]

    def project(index, carry):
        rows = aligned(index, BLOCK)
        normed, _ = standardize(wide(hidden[rows, :]))
        block = rounded(normed * vectors[2:3, :])
        hidden[rows, :] = block
        raw = dot(block, qkv[...]) + vectors[7:8, :768]
        cos, sin = cosines[rows, :], sines[rows, :]
        for tile in range(2):
            at = tile * 128
            lanes = slice(at, at + 128)
            query[rows, lanes] = rounded(turn(raw[:, lanes], cos, sin)) * jnp.bfloat16(0.125)
            key[rows, lanes] = rounded(turn(raw[:, 256 + at : 384 + at], cos, sin))
        value[rows, :] = rounded(raw[:, 512:])
        return carry

    lax.fori_loop(0, GROUP, project, 0)
    causal = causal_block()
    logs[...] = jnp.zeros_like(logs)
    mixed[...] = jnp.zeros_like(mixed)
    lane = lax.broadcasted_iota(jnp.int32, (BLOCK, 128), 1)

    def head(index, carry):
        lanes = aligned(index >> 1, 128)
        mine = lane // 64 == (index & 1)
        for block in range(GROUP):
            rows = slice(block * BLOCK, block * BLOCK + BLOCK)
            seen = (block + 1) * BLOCK
            masked = jnp.where(mine, query[rows, lanes], jnp.bfloat16(0))
            scores = nt(masked, key[:seen, lanes])
            last = jnp.where(causal, scores[:, seen - BLOCK :], -1e30)
            scores = jnp.concatenate([scores[:, : seen - BLOCK], last], 1) if block else last
            best = jnp.max(scores, axis=1, keepdims=True)
            exps = jnp.exp(scores - best)
            total = jnp.sum(exps, axis=1, keepdims=True)
            out = dot(rounded(exps), value[:seen, lanes]) / total
            mixed[rows, lanes] = jnp.where(mine, rounded(out), mixed[rows, lanes])
            logs[rows, :] = jnp.where(lane == index, best + jnp.log(total), logs[rows, :])
        return carry

    lax.fori_loop(0, 4, head, 0)
    for relative, part in enumerate((p0, p1, p32.at[BLOCK:], p32.at[:BLOCK])):
        part[...] = rounded(dot(mixed[aligned(position ^ relative, BLOCK), :], out_rows[...]))


def pair_back(pair, query, key, value, mixed, logs, d_out, d_query, d_key, d_value):
    lanes = slice(pair * 128, pair * 128 + 128)
    causal = causal_block()
    lane = lax.broadcasted_iota(jnp.int32, (BLOCK, 128), 1)
    d_key[...] = jnp.zeros_like(d_key)
    d_value[...] = jnp.zeros_like(d_value)
    d_query[...] = jnp.zeros_like(d_query)

    def head(parity, carry):
        mine = lane // 64 == parity
        for block in range(GROUP):
            rows = slice(block * BLOCK, block * BLOCK + BLOCK)
            seen = (block + 1) * BLOCK
            keys, values = key[:seen, lanes], value[:seen, lanes]
            masked_q = jnp.where(mine, query[rows, lanes], jnp.bfloat16(0))
            masked_d = jnp.where(mine, d_out[rows, lanes], jnp.bfloat16(0))
            log = jnp.sum(jnp.where(lane == pair * 2 + parity, logs[rows, :], 0.0), 1, keepdims=True)
            delta = jnp.sum(wide(masked_d) * wide(mixed[rows, lanes]), 1, keepdims=True)
            probs = jnp.exp(nt(masked_q, keys) - log)
            last = jnp.where(causal, probs[:, seen - BLOCK :], 0.0)
            probs = jnp.concatenate([probs[:, : seen - BLOCK], last], 1) if block else last
            d_scores = rounded(probs * (nt(masked_d, values) - delta))
            d_query[rows, :] += jnp.where(mine, dot(d_scores, keys), 0.0)
            d_value[:seen, :] += tn(rounded(probs), masked_d)
            d_key[:seen, :] += tn(d_scores, masked_q)
        return carry

    lax.fori_loop(0, 2, head, 0)


def finish_back(cosines, sines, d_query, d_key, d_value, grads, shift_sums):
    shift_sums[...] = jnp.zeros_like(shift_sums)

    def finish(index, carry):
        rows = aligned(index, BLOCK)
        cos, sin = cosines[rows, :], -sines[rows, :]
        grads[rows, :128] = rounded(turn(d_query[rows, :] * 0.125, cos, sin))
        grads[rows, 128:256] = rounded(turn(d_key[rows, :], cos, sin))
        grads[rows, 256:] = rounded(d_value[rows, :])
        shift_sums[0:1, :] += jnp.sum(wide(grads[rows, :]), axis=0, keepdims=True)
        return carry

    lax.fori_loop(0, GROUP, finish, 0)


def attend_back_first(
    a0, a1, a2, a3, out_rows, query, key, value, mixed, logs, cosines, sines,
    d_out, grads, shift_sums, d_query, d_key, d_value,
):
    _, _, _, position = spot()
    for relative, rows_in in enumerate((a0, a1, a2, a3)):
        d_out[aligned(position ^ relative, BLOCK), :] = rounded(nt(rows_in[...], out_rows[...]))
    pair_back(0, query, key, value, mixed, logs, d_out, d_query, d_key, d_value)
    finish_back(cosines, sines, d_query, d_key, d_value, grads, shift_sums)


def attend_back_second(
    d_out, before, qkv, query, key, value, mixed, logs, cosines, sines,
    grads, shift_sums, p0, p1, p32, d_query, d_key, d_value, joined,
):
    _, _, _, position = spot()
    pair_back(1, query, key, value, mixed, logs, d_out, d_query, d_key, d_value)
    finish_back(cosines, sines, d_query, d_key, d_value, grads, shift_sums)
    for index in range(3):
        joined[:, index * 256 : index * 256 + 128] = before[:, index * 128 : index * 128 + 128]
        joined[:, index * 256 + 128 : index * 256 + 256] = grads[:, index * 128 : index * 128 + 128]
    for relative, part in enumerate((p0, p1, p32.at[BLOCK:], p32.at[:BLOCK])):
        part[...] = rounded(nt(joined[aligned(position ^ relative, BLOCK), :], qkv[...]))


CHUNK = 64


def in_chunks(step):
    def one(index, carry):
        step(aligned(index, CHUNK), pl.ds(pl.multiple_of(BLOCK + index * CHUNK, CHUNK), CHUNK))
        return carry

    lax.fori_loop(0, BLOCK // CHUNK, one, 0)


def after_attention(p0, core_in, x_in, rows_in, vectors, middle, hidden, normed_o, normed_f, inverses):
    def step(rows, low):
        branch = wide(p0[rows, :]) + wide(core_in[low, :]) + wide(x_in[rows, :]) + vectors[0:1, :]
        normed, inverse_o = standardize(branch)
        normed_o[rows, :] = normed
        total = wide(rows_in[rows, :]) + normed * vectors[3:4, :]
        middle[rows, :] = total
        normed, inverse_f = standardize(total)
        normed_f[rows, :] = normed
        hidden[rows, :] = rounded(normed * vectors[4:5, :])
        lane = lax.broadcasted_iota(jnp.int32, (CHUNK, 128), 1)
        inverses[rows, :] = jnp.where(lane < 64, inverse_o, inverse_f)

    in_chunks(step)


def after_feed(p0, core_in, x_in, middle, cotangent, vectors, layer_out, d_branch, sums):
    sums[...] = jnp.zeros_like(sums)

    def step(rows, low):
        branch = wide(p0[rows, :]) + wide(core_in[low, :]) + wide(x_in[rows, :]) + vectors[1:2, :]
        normed, inverse = standardize(branch)
        gain = vectors[5:6, :]
        layer_out[rows, :] = rounded(middle[rows, :] + normed * gain)
        upstream = wide(cotangent[rows, :])
        back = rounded(norm_back(normed, inverse, upstream * gain))
        d_branch[rows, :] = back
        sums[0:1, :] += jnp.sum(upstream * normed, axis=0, keepdims=True)
        sums[1:2, :] += jnp.sum(wide(back), axis=0, keepdims=True)

    in_chunks(step)


def after_feed_back(
    p0, core_in, x_in, cotangent, normed_o, normed_f, inverses, vectors, d_middle, d_branch, sums
):
    sums[...] = jnp.zeros_like(sums)

    def step(rows, low):
        d_hidden = wide(p0[rows, :]) + wide(core_in[low, :]) + wide(x_in[rows, :])
        normed = normed_f[rows, :]
        sums[0:1, :] += jnp.sum(d_hidden * normed, axis=0, keepdims=True)
        total = wide(cotangent[rows, :]) + norm_back(
            normed, inverses[rows, 64:65], d_hidden * vectors[4:5, :]
        )
        d_middle[rows, :] = total
        normed = normed_o[rows, :]
        sums[1:2, :] += jnp.sum(total * normed, axis=0, keepdims=True)
        back = rounded(norm_back(normed, inverses[rows, 0:1], total * vectors[3:4, :]))
        d_branch[rows, :] = back
        sums[2:3, :] += jnp.sum(wide(back), axis=0, keepdims=True)

    in_chunks(step)


def gain_in_sums(p0, p1, p32, x0, x1, x2, x3, sums):
    sums[...] = jnp.zeros_like(sums)

    def step(rows, low):
        for part, rows_in in ((p0[rows, :], x0), (p1[rows, :], x1), (p32[low, :], x2), (p32[rows, :], x3)):
            normed, _ = standardize(wide(rows_in[rows, :]))
            sums[0:1, :] += jnp.sum(wide(part) * normed, axis=0, keepdims=True)

    in_chunks(step)


def after_attention_back(p0, core_in, x_in, rows_in, d_middle, vectors, d_rows):
    def step(rows, low):
        d_hidden = wide(p0[rows, :]) + wide(core_in[low, :]) + wide(x_in[rows, :])
        normed, inverse = standardize(wide(rows_in[rows, :]))
        d_rows[rows, :] = rounded(
            d_middle[rows, :] + norm_back(normed, inverse, d_hidden * vectors[2:3, :])
        )

    in_chunks(step)


GELU_SCALE = math.sqrt(2.0 / math.pi)


def feed_rows(rows_in, up_mat, down_mat, vectors, before, after, part, at):
    rows = slice(at, at + BLOCK)

    def step(index, carry):
        lanes = aligned(index, BLOCK)
        raw = dot(rows_in[...], up_mat[:, lanes]) + vectors[6:7, lanes]
        before[rows, lanes] = raw
        after[rows, lanes] = rounded(jax.nn.gelu(raw))
        return carry

    lax.fori_loop(0, 4, step, 0)

    def out(index, carry):
        lanes = aligned(index, BLOCK)
        part[:, lanes] = rounded(dot(after[rows, :], down_mat[:, lanes]))
        return carry

    lax.fori_loop(0, 4, out, 0)


def feed_first(
    h0, h2, uo, u1, u2, u3, far_u, do, d1, d2, d3, far_d, vectors,
    up_mat, down_mat, before, after, p0, p2,
):
    for shard, half, piece in each_piece(uo, (u1, u2, u3), [far_u.at[i] for i in range(3)]):
        up_mat[aligned(shard * 2 + half, 128), :] = piece[...]
    for shard, half, piece in each_piece(do, (d1, d2, d3), [far_d.at[i] for i in range(3)]):
        down_mat[aligned(shard * 2 + half, 128), :] = piece[...]
    feed_rows(h0, up_mat, down_mat, vectors, before, after, p0, 0)
    feed_rows(h2, up_mat, down_mat, vectors, before, after, p2, BLOCK)


def feed_second(h1, h3, p2, up_mat, down_mat, vectors, before, after, p1, p32):
    p32[BLOCK:, :] = p2[...]
    feed_rows(h3, up_mat, down_mat, vectors, before, after, p32.at[:BLOCK], BLOCK)
    feed_rows(h1, up_mat, down_mat, vectors, before, after, p1, 0)


def feed_back_rows(rows_in, up_mat, down_mat, before, d_pre, part, sums, at):
    rows = slice(at, at + BLOCK)

    def step(index, carry):
        lanes = aligned(index, BLOCK)
        upstream = nt(rows_in[...], down_mat[lanes, :])
        raw = before[rows, lanes]
        square = raw * raw
        bent = jnp.tanh(GELU_SCALE * raw * (1.0 + 0.044715 * square))
        slope = 0.5 * (1.0 + bent) + 0.5 * GELU_SCALE * raw * (1.0 - bent * bent) * (
            1.0 + 3.0 * 0.044715 * square
        )
        back = rounded(upstream * slope)
        d_pre[rows, lanes] = back
        sums[0:1, lanes] += jnp.sum(wide(back), axis=0, keepdims=True)
        return carry

    lax.fori_loop(0, 4, step, 0)

    def out(index, carry):
        lanes = aligned(index, BLOCK)
        part[:, lanes] = rounded(nt(d_pre[rows, :], up_mat[lanes, :]))
        return carry

    lax.fori_loop(0, 4, out, 0)


def feed_back_first(m0, m2, up_mat, down_mat, before, d_pre, p0, p2, sums):
    sums[...] = jnp.zeros_like(sums)
    feed_back_rows(m0, up_mat, down_mat, before, d_pre, p0, sums, 0)
    feed_back_rows(m2, up_mat, down_mat, before, d_pre, p2, sums, BLOCK)


def feed_back_second(m1, m3, p2, up_mat, down_mat, before, sums_in, d_pre, p1, p32, sums):
    sums[...] = sums_in[...]
    p32[BLOCK:, :] = p2[...]
    feed_back_rows(m3, up_mat, down_mat, before, d_pre, p32.at[:BLOCK], sums, BLOCK)
    feed_back_rows(m1, up_mat, down_mat, before, d_pre, p1, sums, 0)


def put_halves(keep, send, step, at, top, bottom):
    _, _, y_bit, _ = spot()

    @pl.when(y_bit == 0)
    def _():
        keep[step, at : at + 128, :] = top
        send[step, at : at + 128, :] = bottom

    @pl.when(y_bit == 1)
    def _():
        keep[step, at : at + 128, :] = bottom
        send[step, at : at + 128, :] = top


def down_grads(first, second, m0, m1, m2, m3, keep, send):
    _, place, _, _ = spot()

    def one(step, carry):
        lanes = aligned(place ^ step, BLOCK)
        down = (
            tn(first[:BLOCK, lanes], m0[...])
            + tn(first[BLOCK:, lanes], m2[...])
            + tn(second[:BLOCK, lanes], m1[...])
            + tn(second[BLOCK:, lanes], m3[...])
        )
        down = rounded(down)
        put_halves(keep, send, step, 0, down[:128], down[128:])
        return carry

    lax.fori_loop(0, 4, one, 0)


def up_grads(h0, h1, h2, h3, u_first, u_second, keep, send):
    _, place, _, _ = spot()

    def one(step, carry):
        lanes = aligned(place ^ step, BLOCK)
        up = (
            tn(h0[:, lanes], u_first[:BLOCK, :])
            + tn(h2[:, lanes], u_first[BLOCK:, :])
            + tn(h1[:, lanes], u_second[:BLOCK, :])
            + tn(h3[:, lanes], u_second[BLOCK:, :])
        )
        up = rounded(up)
        put_halves(keep, send, step, 0, up[:128], up[128:])
        return carry

    lax.fori_loop(0, 4, one, 0)


def attention_grads_first(mixed, a0, a1, a2, a3, hidden, grads, keep, send, out_grad, block):
    _, place, _, position = spot()
    total = tn(mixed[aligned(position, BLOCK), :], a0[...])
    for relative, rows_in in ((1, a1), (2, a2), (3, a3)):
        total = total + tn(mixed[aligned(position ^ relative, BLOCK), :], rows_in[...])
    out_grad[...] = rounded(total)

    def one(step, carry):
        shard = place ^ step
        block[:, :384] = rounded(tn(hidden[:, aligned(shard, BLOCK)], grads[...]))
        mine = out_grad[aligned(shard, 64), :]
        for j in range(4):
            block[j * 64 : j * 64 + 64, 384:] = mine[:, j * 256 : j * 256 + 256]
        put_halves(keep, send, step, 0, block[:128, :], block[128:, :])
        return carry

    lax.fori_loop(0, 4, one, 0)


def attention_grads_second(
    hidden, grads, sums_f, sums_b, sums_a, sums_u, sums_q, sums_r, keep, send
):
    _, place, y_bit, _ = spot()

    def one(step, carry):
        shard = place ^ step
        block = rounded(tn(hidden[:, aligned(shard, BLOCK)], grads[...]))
        put_halves(keep, send, step, 0, block[:128], block[128:])
        lanes = aligned(shard, BLOCK)
        biases = []
        for index in range(3):
            at = index * 128
            pair = jnp.where(shard < 2, sums_q[0:1, at : at + 128], sums_r[0:1, at : at + 128])
            biases.append(jnp.where((shard & 1) == 0, pair[:, :64], pair[:, 64:]))
        zero = jnp.zeros((1, 192), jnp.float32)
        tops = [sums_b[2:3, lanes], sums_f[1:2, lanes], sums_a[0:1, lanes], *biases, zero]
        lows = [sums_b[1:2, lanes], sums_b[0:1, lanes], sums_f[0:1, lanes], sums_u[0:1, lanes], zero[:, :128]]
        halves = []
        for items in (tops, lows):
            flat = jnp.concatenate(items, 1)
            row = lax.broadcasted_iota(jnp.int32, (8, 384), 0)
            full = [jnp.broadcast_to(flat[:, i * 384 : i * 384 + 384], (8, 384)) for i in range(3)]
            rows = jnp.where(row == 0, full[0], jnp.where(row == 1, full[1], full[2]))
            halves.append(rounded(jnp.where(row < 3, rows, 0.0)))
        mine, other = jnp.where(y_bit == 0, halves[0], halves[1]), jnp.where(y_bit == 0, halves[1], halves[0])
        keep[step, 128:136, :] = mine
        send[step, 128:136, :] = other
        return carry

    lax.fori_loop(0, 4, one, 0)


def add_pairs(keep, come, stay, go):
    for step, out in enumerate((stay.at[0], go.at[0], stay.at[1], go.at[1])):
        out[...] = rounded(wide(keep[step]) + wide(come[step]))


def add_near(stay, come, own, go):
    own[...] = rounded(wide(stay[0]) + wide(come[0]))
    go[...] = rounded(wide(stay[1]) + wide(come[1]))


def each_part(own, x_part, y_part, core_part):
    rep = lax.axis_index("rep")
    refs = [own, x_part, y_part.at[0], y_part.at[1]] + [core_part.at[i] for i in range(4)]
    for relative, ref in enumerate(refs):
        flip = ((relative & 1) << 1) | ((relative & 2) << 1) | (relative >> 2)
        there = rep ^ flip
        yield there >> 2, there & 3, ref


def unpack_down(own, x_part, y_part, core_part, down):
    for y_bit, quarter, ref in each_part(own, x_part, y_part, core_part):
        down[aligned(quarter * 2 + y_bit, 128), :] = wide(ref[...])


def unpack_up(own, x_part, y_part, core_part, up):
    for y_bit, quarter, ref in each_part(own, x_part, y_part, core_part):
        for there in range(4):
            lanes = pl.ds(pl.multiple_of(there * 1024 + quarter * 256, 256), 256)
            up[aligned(y_bit, 128), lanes] = wide(ref[:, there * 256 : there * 256 + 256])


def unpack_attention(
    own, x_part, y_part, core_part, own2, x_part2, y_part2, core_part2,
    query, key, value, out_weight, qb, kb, vb, ob, db, ga, gb, gc, gd, ub,
):
    first = list(each_part(own, x_part, y_part, core_part))
    second = list(each_part(own2, x_part2, y_part2, core_part2))
    row = lax.broadcasted_iota(jnp.int32, (128, 512), 0)
    col = lax.broadcasted_iota(jnp.int32, (128, 512), 1)
    sets = ((0, 1, 4, 5), (2, 3, 6, 7))
    chosen = []
    for index in sets[0]:
        quarter = first[index][1]
        chosen.append(rounded(wide(col == (row // 64) * 256 + quarter * 64 + row % 64)))
    chosen = jnp.concatenate(chosen, 0)
    for pair, parts in enumerate((first, second)):
        for members in sets:
            rows = aligned(parts[members[0]][0], 128)
            for index, out in enumerate((query, key, value)):
                lanes = slice(index * 128, index * 128 + 128)
                joined = jnp.concatenate([parts[i][2][:128, lanes] for i in members], 1)
                out[rows, pair * 512 : pair * 512 + 512] = dot(joined, chosen)
    for y_bit, quarter, ref in first:
        for j in range(2):
            out_weight[aligned(quarter, 64), aligned(y_bit * 2 + j, 256)] = wide(
                ref[j * 64 : j * 64 + 64, 384:]
            )
    y_bit = first[0][0]
    flats = []
    for members in sets:
        rows = [wide(second[i][2][128:136, :]) for i in members]
        total = rows[0] + rows[1] + rows[2] + rows[3]
        flats.append((total, rows))
    mine, other = flats
    for half, (outs, size) in enumerate((((ob, db, ga), 64), ((gb, gc, gd), 256))):
        take = y_bit == half
        total = jnp.where(take, mine[0], other[0])
        flat = jnp.concatenate([total[0:1, :], total[1:2, :]], 1)
        for index, out in enumerate(outs):
            out[...] = flat[:, index * 256 : index * 256 + 256]
        locals_ = [jnp.where(take, a, b)[2:3, :] for a, b in zip(mine[1], other[1], strict=True)]
        quarters = [first[i][1] for i in sets[0]]
        for there in range(4):
            value_at = jnp.zeros((1, 384), jnp.float32)
            for quarter, item in zip(quarters, locals_, strict=True):
                value_at = value_at + jnp.where(quarter == there, item, 0.0)
            if half == 0:
                for index, out in enumerate((qb, kb, vb)):
                    out[:, there * 64 : there * 64 + 64] = value_at[:, index * 64 : index * 64 + 64]
            else:
                ub[:, there * 256 : there * 256 + 256] = value_at[:, :256]


def sum_pairs(keep, come):
    two = shaped(2, *keep.shape[1:])
    return call(add_pairs, [two, two], keep, come)


def sum_near(stay, come):
    one = shaped(*stay.shape[1:])
    return call(add_near, [one, one], stay, come)


def sum_far(own, come):
    return rounded(wide(own) + wide(come))


def gather_packs(total):
    x_part = swap(total, X)
    two = jnp.stack([total, x_part])
    y_part = swap(two, Y)
    return total, x_part, y_part, swap(jnp.concatenate([two, y_part]), CORE)


def fast_device(
    layer_input,
    query_weight,
    query_bias,
    key_weight,
    key_bias,
    value_weight,
    value_bias,
    output_weight,
    output_bias,
    up_weight,
    up_bias,
    down_weight,
    down_bias,
    attention_gain_in,
    attention_gain_out,
    feedforward_gain_in,
    feedforward_gain_out,
    layer_cotangent,
):
    f32, bf16 = jnp.float32, jnp.bfloat16
    replicas = lax.axis_size("rep")
    rows, width = layer_input.shape
    tokens = rows * GROUP
    quarter, place, y_bit, _ = spot()
    pairs = token_pairs(replicas)
    back_pairs = [(there, here) for here, there in pairs]
    both = ("rep", "shard")
    part = shaped(rows, width)
    part32 = shaped(rows, width, kind=f32)
    sums = shaped(8, width, kind=f32)

    def spread(piece):
        return swap(piece, X), swap(piece, CORE)

    def gather_sum(p1, p32):
        core_in = swap(p32, CORE)
        return core_in, swap(rounded(wide(p1) + wide(core_in[:rows])), X)

    own_rows = lax.ppermute(layer_input, both, pairs)
    (packed,) = call(
        pack_attention,
        [shaped(2, 144, width)],
        query_weight,
        key_weight,
        value_weight,
        output_weight,
        query_bias,
        key_bias,
        value_bias,
        up_bias,
        output_bias,
        down_bias,
        attention_gain_in,
        attention_gain_out,
        feedforward_gain_in,
        feedforward_gain_out,
    )
    near_a = near_pieces(packed, y_bit)
    cosines, sines = rope_tables(tokens, 64)
    up_packed, down_packed = call_pack_feed(up_weight, down_weight)
    own_rows = tie(own_rows, packed, cosines, sines, up_packed)
    x1, x2 = spread(own_rows)
    blocks = own_rows, x1, x2, swap(x1, CORE)
    far_a = far_pieces(near_a)
    near_u = near_pieces(up_packed, y_bit, *near_a)
    two16 = shaped(2 * rows, width)
    head_rows = shaped(tokens, 256)
    query, key, value, mixed, logs, hidden_a, qkv, out_rows, vectors, p0, p1, p32 = call(
        attend,
        [head_rows] * 4
        + [
            shaped(tokens, 128, kind=f32),
            shaped(tokens, width),
            shaped(width, 768),
            shaped(256, width),
            sums,
        ]
        + [part, part, two16],
        *blocks,
        packed,
        *near_a,
        *far_a,
        cosines,
        sines,
        flops=2 * tokens * 1024 * 1024 + 8 * tokens * tokens * 64 * 2,
        exps=2 * tokens * tokens,
        room=14,
    )
    p32 = tie(p32, *near_u)
    far_u = far_together(near_u)
    near_d = near_pieces(down_packed, y_bit, *near_u)
    core_in, x_in = gather_sum(p1, p32)
    x_in = tie(x_in, far_u, *near_d)
    far_d = far_together(near_d)
    cotangent = lax.ppermute(tie(layer_cotangent, *near_d), both, pairs)
    middle, hidden_own, normed_o, normed_f, inverses = call(
        after_attention,
        [part32, part, part32, part32, shaped(rows, 128, kind=f32)],
        p0,
        core_in,
        x_in,
        own_rows,
        vectors,
    )
    h0 = hidden_own
    h1, h2 = spread(h0)
    two32 = shaped(2 * rows, width, kind=f32)
    square = shaped(width, width)
    flops = 4 * 2 * rows * 1024 * 1024
    up_mat, down_mat, before_a, after_a, p0, p2 = call(
        feed_first,
        [square, square, two32, two16, part, part],
        h0, h2, up_packed, *near_u, far_u, down_packed, *near_d, far_d, vectors,
        flops=flops, room=10,
    )
    h1 = tie(h1, p2, cotangent)
    h3 = swap(h1, CORE)
    before_b, after_b, p1, p32 = call(
        feed_second,
        [two32, two16, part, two16],
        h1, h3, p2, up_mat, down_mat, vectors,
        flops=flops, room=10,
    )
    core_in, x_in = gather_sum(p1, p32)
    layer_output, d_branch, sums_f = call(
        after_feed, [part, part, sums], p0, core_in, x_in, middle, cotangent, vectors
    )
    m0 = d_branch
    m1, m2 = spread(m0)
    u_first, p0, p2, sums_u = call(
        feed_back_first,
        [two16, part, part, sums],
        m0, m2, up_mat, down_mat, before_a,
        flops=flops, room=10,
    )
    m1 = tie(m1, u_first)
    m3 = swap(m1, CORE)
    packs = [shaped(4, 128, width)] * 2
    grad_flops = 2 * tokens * 1024 * 1024
    u_second, p1, p32, sums_u = call(
        feed_back_second,
        [two16, part, two16, sums],
        m1, m3, p2, up_mat, down_mat, before_b, sums_u,
        flops=flops, room=10,
    )
    core_in, x_in = gather_sum(p1, p32)
    pack_d = call(
        down_grads, packs, after_a, after_b, m0, m1, m2, tie(m3, u_second), flops=grad_flops, room=10
    )
    come_d = swap(pack_d[1], Y)
    pack_u = call(
        up_grads,
        packs,
        h0, h1, h2, h3, u_first, tie(u_second, *pack_d),
        flops=grad_flops, room=10,
    )
    flops = grad_flops
    x_in = tie(x_in, *pack_u)
    d_middle, d_branch, sums_b = call(
        after_feed_back,
        [part32, part, sums],
        p0,
        core_in,
        x_in,
        cotangent,
        normed_o,
        normed_f,
        inverses,
        vectors,
    )
    a0 = d_branch
    a1, a2 = spread(a0)
    stay_d, go_d = sum_pairs(tie(pack_d[0], d_branch), come_d)
    come_u = swap(pack_u[1], Y)
    a1 = tie(a1, go_d)
    layer_output = lax.ppermute(tie(layer_output, a1), both, back_pairs)
    a3 = swap(a1, CORE)
    a_blocks = a0, a1, a2, a3
    come_d = flip(go_d, 1)
    grad32 = [pltpu.VMEM((tokens, 128), f32)] * 3
    back_flops = tokens * 1024 * 1024 + 10 * tokens * tokens * 64 * 2
    d_out, grads_first, sums_q = call(
        attend_back_first,
        [shaped(tokens, 256), shaped(tokens, 384), shaped(8, 384, kind=f32)],
        *a_blocks, out_rows, query, key, value, mixed, logs, cosines, sines,
        scratch=grad32, flops=back_flops, exps=tokens * tokens, room=14,
    )
    pack_a = call(
        attention_grads_first,
        [shaped(4, 128, 640)] * 2,
        mixed, *a_blocks, hidden_a, grads_first,
        scratch=[pltpu.VMEM((256, width), bf16), pltpu.VMEM((256, 640), bf16)],
        flops=flops // 2, room=10,
    )
    grads_second, sums_r, p0, p1, p32 = call(
        attend_back_second,
        [shaped(tokens, 384), shaped(8, 384, kind=f32), part, part, two16],
        tie(d_out, *pack_a), grads_first, qkv, query, key, value, mixed, logs, cosines, sines,
        scratch=grad32 + [pltpu.VMEM((tokens, 768), bf16)],
        flops=back_flops, exps=tokens * tokens, room=14,
    )
    come_a = swap(pack_a[1], Y)
    p32 = tie(p32, come_u, layer_output)
    core_in, x_in = gather_sum(p1, p32)
    own_d, go_d = sum_near(tie(stay_d, p32), come_d)
    come_d = flip(go_d, 2)
    stay_u, go_u = sum_pairs(tie(pack_u[0], p32), come_u)
    (sums_a,) = call(gain_in_sums, [sums], p0, p1, p32, *blocks)
    pack_b = call(
        attention_grads_second,
        [shaped(4, 136, 384)] * 2,
        hidden_a, grads_second, sums_f, sums_b, sums_a, sums_u, sums_q, sums_r,
        flops=flops // 2, room=10,
    )
    x_in = tie(x_in, *pack_b, go_u)
    (d_rows,) = call(
        after_attention_back, [part], p0, core_in, x_in, own_rows, d_middle, vectors
    )
    input_gradient = lax.ppermute(d_rows, both, back_pairs)
    total_d = sum_far(tie(own_d, d_rows), come_d)
    own_u, go_u = sum_near(tie(stay_u, d_rows), flip(go_u, 1))
    stay_a, go_a = sum_pairs(tie(pack_a[0], d_rows), come_a)
    own_a, go_a = sum_near(stay_a, flip(go_a, 1))
    stay_b, go_b = sum_pairs(pack_b[0], swap(pack_b[1], Y))
    total_u = sum_far(own_u, flip(go_u, 2))
    own_b, go_b = sum_near(tie(stay_b, input_gradient), flip(go_b, 1))
    total_a = sum_far(own_a, flip(go_a, 2))
    total_b = sum_far(own_b, flip(go_b, 2))
    (g_down,) = call(unpack_down, [shaped(*down_weight.shape, kind=f32)], *gather_packs(total_d))
    (g_up,) = call(unpack_up, [shaped(*up_weight.shape, kind=f32)], *gather_packs(total_u))
    packs_a = gather_packs(total_a)
    packs_b = gather_packs(total_b)
    g_query, g_key, g_value, g_out, *small = call(
        unpack_attention,
        [part32] * 4 + [shaped(1, 256, kind=f32)] * 9 + [shaped(1, 1024, kind=f32)],
        *packs_a,
        *packs_b,
    )
    small = [item.reshape(-1) for item in small]
    input_gradient = input_gradient.astype(f32)
    return (
        layer_output,
        input_gradient,
        g_query,
        small[0],
        g_key,
        small[1],
        g_value,
        small[2],
        g_out,
        small[3],
        g_up,
        small[9],
        g_down,
        small[4],
        small[5],
        small[6],
        small[7],
        small[8],
    )


def solution(mesh):
    replicas, shards = mesh.shape["rep"], mesh.shape["shard"]
    fits = shards == 4 and replicas == 8 and HEADS % 16 == 0
    return jax.shard_map(
        fast_device if fits else general_device,
        mesh=mesh,
        in_specs=(
            P(("rep", "shard"), None),
            P("shard", None),
            P("shard"),
            P("shard", None),
            P("shard"),
            P("shard", None),
            P("shard"),
            P("shard", None),
            P("shard"),
            P("shard", None),
            P("shard"),
            P("shard", None),
            P("shard"),
            P("shard"),
            P("shard"),
            P("shard"),
            P("shard"),
            P(("rep", "shard"), None),
        ),
        out_specs=(
            P(("rep", "shard"), None),
            P(("rep", "shard"), None),
            P("shard", None),
            P("shard"),
            P("shard", None),
            P("shard"),
            P("shard", None),
            P("shard"),
            P("shard", None),
            P("shard"),
            P("shard", None),
            P("shard"),
            P("shard", None),
            P("shard"),
            P("shard"),
            P("shard"),
            P("shard"),
            P("shard"),
        ),
        check_vma=False,
    )
```

```python
import functools
import math

import jax
import jax.numpy as jnp
import numpy as np
from jax import lax
from jax.experimental import pallas as pl
from jax.experimental.pallas import tpu as pltpu
from jax.sharding import PartitionSpec as P

HEADS = 16


norm_epsilon = 1e-05


def normalize(values):
    centered = values - jnp.mean(values, axis=-1, keepdims=True)
    inverse = lax.rsqrt(jnp.mean(centered * centered, axis=-1, keepdims=True) + norm_epsilon)
    return (centered * inverse, inverse)


def norm_back(normed, inverse, upstream):
    return inverse * (
        upstream
        - jnp.mean(upstream, axis=-1, keepdims=True)
        - normed * jnp.mean(upstream * normed, axis=-1, keepdims=True)
    )


def rotation(positions, head_dim):
    half_dim = head_dim // 2
    freqs = 10000.0 ** (-jnp.arange(half_dim, dtype=jnp.float32) / half_dim)
    angles = positions.astype(jnp.float32)[:, None] * freqs[None, :]
    return (jnp.cos(angles)[:, None, :], jnp.sin(angles)[:, None, :])


def rotate(tensor, cosines, sines, sign):
    half_dim = tensor.shape[-1] // 2
    first = tensor[..., :half_dim]
    second = tensor[..., half_dim:]
    return jnp.concatenate(
        [first * cosines - sign * second * sines, second * cosines + sign * first * sines], axis=-1
    )


def col_sum(values):
    return jnp.sum(values.astype(jnp.float32), axis=0)


def general_device(
    layer_input,
    query_weight,
    query_bias,
    key_weight,
    key_bias,
    value_weight,
    value_bias,
    output_weight,
    output_bias,
    up_weight,
    up_bias,
    down_weight,
    down_bias,
    attention_gain_in,
    attention_gain_out,
    feedforward_gain_in,
    feedforward_gain_out,
    layer_cotangent,
):
    rows = layer_input.shape[0]
    width = layer_input.shape[1]
    heads = HEADS
    head_dim = width // heads
    seq_rows = rows * lax.axis_size("shard")
    factor = head_dim ** (-0.5)
    positions = lax.axis_index("shard") * rows + jnp.arange(rows, dtype=jnp.int32)
    cosines, sines = rotation(positions, head_dim)
    attention_local = (
        query_weight,
        key_weight,
        value_weight,
        output_weight,
        query_bias,
        key_bias,
        value_bias,
        output_bias,
        attention_gain_in,
        attention_gain_out,
    )
    feed_local = (
        up_weight,
        up_bias,
        down_weight,
        down_bias,
        feedforward_gain_in,
        feedforward_gain_out,
    )
    attention_full = (
        lax.all_gather(attention_local[0], "shard", axis=0, tiled=True),
        lax.all_gather(attention_local[1], "shard", axis=0, tiled=True),
        lax.all_gather(attention_local[2], "shard", axis=0, tiled=True),
        lax.all_gather(attention_local[3], "shard", axis=0, tiled=True),
        lax.all_gather(attention_local[4], "shard", axis=0, tiled=True),
        lax.all_gather(attention_local[5], "shard", axis=0, tiled=True),
        lax.all_gather(attention_local[6], "shard", axis=0, tiled=True),
        lax.all_gather(attention_local[7], "shard", axis=0, tiled=True),
        lax.all_gather(attention_local[8], "shard", axis=0, tiled=True),
        lax.all_gather(attention_local[9], "shard", axis=0, tiled=True),
    )
    (
        query_mat,
        key_mat,
        value_mat,
        out_mat,
        query_shift,
        key_shift,
        value_shift,
        out_shift,
        gain_in_a,
        gain_out_a,
    ) = attention_full
    residual_in = layer_input.astype(jnp.float32)
    normed_a, inverse_a = normalize(residual_in)
    hidden_a = (normed_a * gain_in_a.astype(jnp.float32)).astype(jnp.bfloat16)

    def project(matrix, shift):
        return jnp.dot(hidden_a, matrix, preferred_element_type=jnp.float32) + shift.astype(
            jnp.float32
        )

    query_heads = rotate(
        project(query_mat, query_shift).reshape(rows, heads, head_dim), cosines, sines, 1.0
    ).astype(jnp.bfloat16)
    key_rows = (
        rotate(project(key_mat, key_shift).reshape(rows, heads, head_dim), cosines, sines, 1.0)
        .astype(jnp.bfloat16)
        .reshape(rows, width)
    )
    value_rows = project(value_mat, value_shift).astype(jnp.bfloat16)
    start_state = (
        jnp.full((heads, rows), -1e30, jnp.float32),
        jnp.zeros((heads, rows), jnp.float32),
        jnp.zeros((heads, rows, head_dim), jnp.float32),
    )
    key_piece = lax.all_gather(key_rows, "shard", axis=0, tiled=True)
    value_piece = lax.all_gather(value_rows, "shard", axis=0, tiled=True)
    count = key_piece.shape[0]
    block = math.gcd(count, 512)

    def forward_inner(index, state):
        best, total, accum = state
        offset = index * block
        key_block = lax.dynamic_slice_in_dim(key_piece, offset, block, 0).reshape(
            block, heads, head_dim
        )
        value_block = lax.dynamic_slice_in_dim(value_piece, offset, block, 0).reshape(
            block, heads, head_dim
        )
        key_pos = offset + jnp.arange(block, dtype=jnp.int32)
        allowed = key_pos[None, None, :] <= positions[None, :, None]
        scores = (
            jnp.einsum("qhd,khd->hqk", query_heads, key_block, preferred_element_type=jnp.float32)
            * factor
        )
        scores = jnp.where(allowed, scores, -1e30)
        newest = jnp.maximum(best, jnp.max(scores, axis=-1))
        weights = jnp.where(allowed, jnp.exp(scores - newest[..., None]), 0.0)
        decay = jnp.exp(best - newest)
        total = total * decay + jnp.sum(weights, axis=-1)
        accum = accum * decay[..., None] + jnp.einsum(
            "hqk,khd->hqd",
            weights.astype(jnp.bfloat16),
            value_block,
            preferred_element_type=jnp.float32,
        )
        return (newest, total, accum)

    best, total, accum = lax.fori_loop(0, count // block, forward_inner, start_state)
    logsum = best + jnp.log(total)
    attended = (
        jnp.transpose(accum / total[..., None], (1, 0, 2)).reshape(rows, width).astype(jnp.bfloat16)
    )
    branch_a = jnp.dot(attended, out_mat, preferred_element_type=jnp.float32) + out_shift.astype(
        jnp.float32
    )
    normed_o, inverse_o = normalize(branch_a)
    middle = residual_in + normed_o * gain_out_a.astype(jnp.float32)
    feed_full = (
        lax.all_gather(feed_local[0], "shard", axis=0, tiled=True),
        lax.all_gather(feed_local[1], "shard", axis=0, tiled=True),
        lax.all_gather(feed_local[2], "shard", axis=0, tiled=True),
        lax.all_gather(feed_local[3], "shard", axis=0, tiled=True),
        lax.all_gather(feed_local[4], "shard", axis=0, tiled=True),
        lax.all_gather(feed_local[5], "shard", axis=0, tiled=True),
    )
    up_mat, up_shift, down_mat, down_shift, gain_in_f, gain_out_f = feed_full
    normed_f, inverse_f = normalize(middle)
    hidden_f = (normed_f * gain_in_f.astype(jnp.float32)).astype(jnp.bfloat16)
    pre_act = jnp.dot(hidden_f, up_mat, preferred_element_type=jnp.float32) + up_shift.astype(
        jnp.float32
    )
    activated = jax.nn.gelu(pre_act).astype(jnp.bfloat16)
    branch_f = jnp.dot(activated, down_mat, preferred_element_type=jnp.float32) + down_shift.astype(
        jnp.float32
    )
    normed_d, inverse_d = normalize(branch_f)
    layer_output = (middle + normed_d * gain_out_f.astype(jnp.float32)).astype(jnp.bfloat16)
    feed_back = (
        lax.all_gather(feed_local[0], "shard", axis=0, tiled=True),
        lax.all_gather(feed_local[1], "shard", axis=0, tiled=True),
        lax.all_gather(feed_local[2], "shard", axis=0, tiled=True),
        lax.all_gather(feed_local[3], "shard", axis=0, tiled=True),
        lax.all_gather(feed_local[4], "shard", axis=0, tiled=True),
        lax.all_gather(feed_local[5], "shard", axis=0, tiled=True),
    )
    up_back, up_unused, down_back, down_unused, gain_in_fb, gain_out_fb = feed_back
    upstream = layer_cotangent.astype(jnp.float32)
    grad_gain_out_f = jnp.sum(upstream * normed_d, axis=0)
    d_branch_f = norm_back(normed_d, inverse_d, upstream * gain_out_fb.astype(jnp.float32)).astype(
        jnp.bfloat16
    )
    grad_down = jnp.einsum("tf,td->fd", activated, d_branch_f, preferred_element_type=jnp.float32)
    grad_down_shift = col_sum(d_branch_f)
    d_activated = jnp.einsum("td,fd->tf", d_branch_f, down_back, preferred_element_type=jnp.float32)
    gelu_out, gelu_pull = jax.vjp(jax.nn.gelu, pre_act)
    d_pre = gelu_pull(d_activated)[0].astype(jnp.bfloat16)
    grad_up = jnp.einsum("td,tf->df", hidden_f, d_pre, preferred_element_type=jnp.float32)
    grad_up_shift = col_sum(d_pre)
    d_hidden_f = jnp.einsum("tf,df->td", d_pre, up_back, preferred_element_type=jnp.float32)
    grad_gain_in_f = jnp.sum(d_hidden_f * normed_f, axis=0)
    d_middle = upstream + norm_back(
        normed_f, inverse_f, d_hidden_f * gain_in_fb.astype(jnp.float32)
    )
    feed_grads = (
        lax.psum_scatter(
            grad_up.astype(jnp.bfloat16), "shard", scatter_dimension=0, tiled=True
        ).astype(jnp.float32),
        lax.psum_scatter(
            grad_up_shift.astype(jnp.bfloat16), "shard", scatter_dimension=0, tiled=True
        ).astype(jnp.float32),
        lax.psum_scatter(
            grad_down.astype(jnp.bfloat16), "shard", scatter_dimension=0, tiled=True
        ).astype(jnp.float32),
        lax.psum_scatter(
            grad_down_shift.astype(jnp.bfloat16), "shard", scatter_dimension=0, tiled=True
        ).astype(jnp.float32),
        lax.psum_scatter(
            grad_gain_in_f.astype(jnp.bfloat16), "shard", scatter_dimension=0, tiled=True
        ).astype(jnp.float32),
        lax.psum_scatter(
            grad_gain_out_f.astype(jnp.bfloat16), "shard", scatter_dimension=0, tiled=True
        ).astype(jnp.float32),
    )
    attention_back = (
        lax.all_gather(attention_local[0], "shard", axis=0, tiled=True),
        lax.all_gather(attention_local[1], "shard", axis=0, tiled=True),
        lax.all_gather(attention_local[2], "shard", axis=0, tiled=True),
        lax.all_gather(attention_local[3], "shard", axis=0, tiled=True),
        lax.all_gather(attention_local[4], "shard", axis=0, tiled=True),
        lax.all_gather(attention_local[5], "shard", axis=0, tiled=True),
        lax.all_gather(attention_local[6], "shard", axis=0, tiled=True),
        lax.all_gather(attention_local[7], "shard", axis=0, tiled=True),
        lax.all_gather(attention_local[8], "shard", axis=0, tiled=True),
        lax.all_gather(attention_local[9], "shard", axis=0, tiled=True),
    )
    (
        query_back,
        key_back,
        value_back,
        out_back,
        qshift_unused,
        kshift_unused,
        vshift_unused,
        oshift_unused,
        gain_in_ab,
        gain_out_ab,
    ) = attention_back
    grad_gain_out_a = jnp.sum(d_middle * normed_o, axis=0)
    d_branch_a = norm_back(normed_o, inverse_o, d_middle * gain_out_ab.astype(jnp.float32)).astype(
        jnp.bfloat16
    )
    grad_out_mat = jnp.einsum("td,te->de", attended, d_branch_a, preferred_element_type=jnp.float32)
    grad_out_shift = col_sum(d_branch_a)
    d_attended = jnp.einsum(
        "te,de->td", d_branch_a, out_back, preferred_element_type=jnp.float32
    ).astype(jnp.bfloat16)
    d_heads = d_attended.reshape(rows, heads, head_dim)
    row_delta = jnp.einsum(
        "qhd,qhd->hq",
        d_heads.astype(jnp.float32),
        attended.reshape(rows, heads, head_dim).astype(jnp.float32),
    )

    def query_terms(key_block, value_block, key_pos):
        allowed = key_pos[None, None, :] <= positions[None, :, None]
        scores = (
            jnp.einsum("qhd,khd->hqk", query_heads, key_block, preferred_element_type=jnp.float32)
            * factor
        )
        probs = jnp.where(allowed, jnp.exp(scores - logsum[..., None]), 0.0)
        d_probs = jnp.einsum(
            "qhd,khd->hqk", d_heads, value_block, preferred_element_type=jnp.float32
        )
        d_scores = (probs * (d_probs - row_delta[..., None])).astype(jnp.bfloat16)
        return (probs, d_scores)

    back_state = (
        jnp.zeros((rows, heads, head_dim), jnp.float32),
        jnp.zeros((seq_rows, width), jnp.float32),
        jnp.zeros((seq_rows, width), jnp.float32),
    )
    backward_key_piece = lax.all_gather(key_rows, "shard", axis=0, tiled=True)
    backward_value_piece = lax.all_gather(value_rows, "shard", axis=0, tiled=True)
    count = backward_key_piece.shape[0]
    backward_block = math.gcd(count, 512)

    def backward_inner(index, state):
        grad_query, grad_keys, grad_values = state
        offset = index * backward_block
        key_block = lax.dynamic_slice_in_dim(backward_key_piece, offset, backward_block, 0).reshape(
            backward_block, heads, head_dim
        )
        value_block = lax.dynamic_slice_in_dim(
            backward_value_piece, offset, backward_block, 0
        ).reshape(backward_block, heads, head_dim)
        key_pos = offset + jnp.arange(backward_block, dtype=jnp.int32)
        probs, d_scores = query_terms(key_block, value_block, key_pos)
        grad_query = (
            grad_query
            + jnp.einsum("hqk,khd->qhd", d_scores, key_block, preferred_element_type=jnp.float32)
            * factor
        )
        key_grad = (
            jnp.einsum("hqk,qhd->khd", d_scores, query_heads, preferred_element_type=jnp.float32)
            * factor
        )
        value_grad = jnp.einsum(
            "hqk,qhd->khd", probs.astype(jnp.bfloat16), d_heads, preferred_element_type=jnp.float32
        )
        grad_keys = lax.dynamic_update_slice_in_dim(
            grad_keys, key_grad.reshape(backward_block, width), offset, 0
        )
        grad_values = lax.dynamic_update_slice_in_dim(
            grad_values, value_grad.reshape(backward_block, width), offset, 0
        )
        return (grad_query, grad_keys, grad_values)

    back_result = lax.fori_loop(0, count // backward_block, backward_inner, back_state)
    grad_query = back_result[0]
    key_total, value_total = (
        lax.psum_scatter(
            back_result[1].astype(jnp.bfloat16), "shard", scatter_dimension=0, tiled=True
        ).astype(jnp.float32),
        lax.psum_scatter(
            back_result[2].astype(jnp.bfloat16), "shard", scatter_dimension=0, tiled=True
        ).astype(jnp.float32),
    )
    d_query = rotate(grad_query, cosines, sines, -1.0).reshape(rows, width).astype(jnp.bfloat16)
    d_key = (
        rotate(key_total.reshape(rows, heads, head_dim), cosines, sines, -1.0)
        .reshape(rows, width)
        .astype(jnp.bfloat16)
    )
    d_value = value_total.astype(jnp.bfloat16)
    grad_query_mat = jnp.einsum("td,te->de", hidden_a, d_query, preferred_element_type=jnp.float32)
    grad_key_mat = jnp.einsum("td,te->de", hidden_a, d_key, preferred_element_type=jnp.float32)
    grad_value_mat = jnp.einsum("td,te->de", hidden_a, d_value, preferred_element_type=jnp.float32)
    d_hidden_a = jnp.einsum("te,de->td", d_query, query_back, preferred_element_type=jnp.float32)
    d_hidden_a = d_hidden_a + jnp.einsum(
        "te,de->td", d_key, key_back, preferred_element_type=jnp.float32
    )
    d_hidden_a = d_hidden_a + jnp.einsum(
        "te,de->td", d_value, value_back, preferred_element_type=jnp.float32
    )
    grad_gain_in_a = jnp.sum(d_hidden_a * normed_a, axis=0)
    input_gradient = d_middle + norm_back(
        normed_a, inverse_a, d_hidden_a * gain_in_ab.astype(jnp.float32)
    )
    attention_grads = (
        lax.psum_scatter(
            grad_query_mat.astype(jnp.bfloat16), "shard", scatter_dimension=0, tiled=True
        ).astype(jnp.float32),
        lax.psum_scatter(
            grad_key_mat.astype(jnp.bfloat16), "shard", scatter_dimension=0, tiled=True
        ).astype(jnp.float32),
        lax.psum_scatter(
            grad_value_mat.astype(jnp.bfloat16), "shard", scatter_dimension=0, tiled=True
        ).astype(jnp.float32),
        lax.psum_scatter(
            grad_out_mat.astype(jnp.bfloat16), "shard", scatter_dimension=0, tiled=True
        ).astype(jnp.float32),
        lax.psum_scatter(
            col_sum(d_query).astype(jnp.bfloat16), "shard", scatter_dimension=0, tiled=True
        ).astype(jnp.float32),
        lax.psum_scatter(
            col_sum(d_key).astype(jnp.bfloat16), "shard", scatter_dimension=0, tiled=True
        ).astype(jnp.float32),
        lax.psum_scatter(
            col_sum(d_value).astype(jnp.bfloat16), "shard", scatter_dimension=0, tiled=True
        ).astype(jnp.float32),
        lax.psum_scatter(
            grad_out_shift.astype(jnp.bfloat16), "shard", scatter_dimension=0, tiled=True
        ).astype(jnp.float32),
        lax.psum_scatter(
            grad_gain_in_a.astype(jnp.bfloat16), "shard", scatter_dimension=0, tiled=True
        ).astype(jnp.float32),
        lax.psum_scatter(
            grad_gain_out_a.astype(jnp.bfloat16), "shard", scatter_dimension=0, tiled=True
        ).astype(jnp.float32),
    )
    (
        g_query,
        g_key,
        g_value,
        g_out,
        g_qshift,
        g_kshift,
        g_vshift,
        g_oshift,
        g_gain_in_a,
        g_gain_out_a,
    ) = attention_grads
    g_up, g_up_shift, g_down, g_down_shift, g_gain_in_f, g_gain_out_f = feed_grads
    summed = (
        lax.psum(g_query.astype(jnp.bfloat16), "rep").astype(jnp.float32),
        lax.psum(g_qshift.astype(jnp.bfloat16), "rep").astype(jnp.float32),
        lax.psum(g_key.astype(jnp.bfloat16), "rep").astype(jnp.float32),
        lax.psum(g_kshift.astype(jnp.bfloat16), "rep").astype(jnp.float32),
        lax.psum(g_value.astype(jnp.bfloat16), "rep").astype(jnp.float32),
        lax.psum(g_vshift.astype(jnp.bfloat16), "rep").astype(jnp.float32),
        lax.psum(g_out.astype(jnp.bfloat16), "rep").astype(jnp.float32),
        lax.psum(g_oshift.astype(jnp.bfloat16), "rep").astype(jnp.float32),
        lax.psum(g_up.astype(jnp.bfloat16), "rep").astype(jnp.float32),
        lax.psum(g_up_shift.astype(jnp.bfloat16), "rep").astype(jnp.float32),
        lax.psum(g_down.astype(jnp.bfloat16), "rep").astype(jnp.float32),
        lax.psum(g_down_shift.astype(jnp.bfloat16), "rep").astype(jnp.float32),
        lax.psum(g_gain_in_a.astype(jnp.bfloat16), "rep").astype(jnp.float32),
        lax.psum(g_gain_out_a.astype(jnp.bfloat16), "rep").astype(jnp.float32),
        lax.psum(g_gain_in_f.astype(jnp.bfloat16), "rep").astype(jnp.float32),
        lax.psum(g_gain_out_f.astype(jnp.bfloat16), "rep").astype(jnp.float32),
    )
    return (
        layer_output,
        input_gradient,
        summed[0],
        summed[1],
        summed[2],
        summed[3],
        summed[4],
        summed[5],
        summed[6],
        summed[7],
        summed[8],
        summed[9],
        summed[10],
        summed[11],
        summed[12],
        summed[13],
        summed[14],
        summed[15],
    )


CORE, X, Y = 1, 2, 4
GROUP = 4
BLOCK = 256


def swap(values, bit):
    count = lax.axis_size("rep")
    return lax.ppermute(values, "rep", [(i, i ^ bit) for i in range(count)])


def shift(values, step):
    count = lax.axis_size("shard")
    return lax.ppermute(values, "shard", [(i, (i + step) % count) for i in range(count)])


def flip(values, bit):
    count = lax.axis_size("shard")
    return lax.ppermute(values, "shard", [(i, i ^ bit) for i in range(count)])


def token_pairs(count):
    pairs = []
    for rep in range(count):
        for z in range(GROUP):
            there = (rep & ~3) | (((z ^ rep) & 1) << 1) | (z >> 1)
            pairs.append((rep * GROUP + z, there * GROUP + ((rep >> 1) & 1) + 2 * (rep & 1)))
    return pairs


def spot():
    rep, place = lax.axis_index("rep"), lax.axis_index("shard")
    return rep & 3, place, rep >> 2, (((rep >> 1) & 1) ^ (place >> 1)) + 2 * (rep & 1)


def aligned(index, size):
    return pl.ds(pl.multiple_of(index * size, size), size)


def dot(left, right):
    return jnp.dot(left, right, preferred_element_type=jnp.float32)


def nt(left, right):
    return lax.dot_general(left, right, (((1,), (1,)), ((), ())), preferred_element_type=jnp.float32)


def tn(left, right):
    return lax.dot_general(left, right, (((0,), (0,)), ((), ())), preferred_element_type=jnp.float32)


def rounded(values):
    return values.astype(jnp.bfloat16)


def wide(values):
    return values.astype(jnp.float32)


def shaped(*dims, kind=jnp.bfloat16):
    return jax.ShapeDtypeStruct(dims, kind)


VMEM_SPEC = pl.BlockSpec(memory_space=pltpu.VMEM)


def call(kernel, outs, *operands, scratch=(), flops=0, exps=0, room=6):
    size = lambda items: sum(math.prod(item.shape) * item.dtype.itemsize for item in items)
    moved = size(operands) + size(outs)
    spaces = [jax.ShapeDtypeStruct(item.shape, item.dtype) for item in scratch]
    return pl.pallas_call(
        kernel,
        out_shape=tuple(outs),
        in_specs=[VMEM_SPEC] * len(operands),
        out_specs=tuple([VMEM_SPEC] * len(outs)),
        scratch_shapes=list(scratch),
        compiler_params=pltpu.CompilerParams(vmem_limit_bytes=moved + size(spaces) + (room << 20)),
        cost_estimate=pl.CostEstimate(flops=flops // 40, bytes_accessed=moved // 40, transcendentals=0),
        name=kernel.__name__,
    )(*operands)


def standardize(values):
    centered = values - jnp.mean(values, axis=-1, keepdims=True)
    inverse = lax.rsqrt(jnp.mean(centered * centered, axis=-1, keepdims=True) + norm_epsilon)
    return centered * inverse, inverse


def turn(values, cosines, sines):
    lane = lax.broadcasted_iota(jnp.int32, values.shape, 1)
    swapped = jnp.where(lane % 64 < 32, pltpu.roll(values, 96, 1), pltpu.roll(values, 32, 1))
    return values * cosines + swapped * sines


def rope_tables(tokens, head_dim):
    half = head_dim // 2
    freqs = 10000.0 ** (-jnp.arange(half, dtype=jnp.float32) / half)
    angles = jnp.arange(tokens, dtype=jnp.int32).astype(jnp.float32)[:, None] * freqs[None, :]
    cosines, sines = jnp.cos(angles), jnp.sin(angles)
    return (
        jnp.concatenate([cosines] * 4, 1),
        jnp.concatenate([-sines, sines, -sines, sines], 1),
    )


def pack_attention(
    query_weight, key_weight, value_weight, out_weight, qb, kb, vb, ub, ob, db, ga, gb, gc, gd, packed
):
    quarter, place, _, _ = spot()
    row = lax.broadcasted_iota(jnp.int32, (1024, 256), 0)
    col = lax.broadcasted_iota(jnp.int32, (1024, 256), 1)
    chosen = rounded(wide(row == (col // 64) * 256 + quarter * 64 + col % 64))
    for index, weight in enumerate((query_weight, key_weight, value_weight)):
        mine = rounded(dot(weight[...], chosen))
        for half in range(2):
            packed[half, :128, index * 256 : index * 256 + 256] = mine[half * 128 : half * 128 + 128]
    out_mine = out_weight[aligned(quarter, 64), :]
    for j in range(4):
        at = (j % 2) * 64
        packed[j // 2, at : at + 64, 768:1024] = out_mine[:, j * 256 : j * 256 + 256]
    row = lax.broadcasted_iota(jnp.int32, (256, 256), 0)
    col = lax.broadcasted_iota(jnp.int32, (256, 256), 1)
    chosen = rounded(wide((row == quarter * 64 + col % 64) & (col // 64 == place)))
    biases = [dot(jnp.broadcast_to(item[...][None, :], (16, 256)), chosen) for item in (qb, kb, vb)]
    full = lambda item: jnp.broadcast_to(wide(item[...])[None, :], (16, 256))
    up_mine = jnp.broadcast_to(wide(ub[aligned(quarter, 256)])[None, :], (16, 256))
    zero = jnp.zeros((16, 256), jnp.float32)
    first = jnp.concatenate(biases + [zero], 1)
    second = jnp.concatenate([up_mine, full(ob), full(db), zero], 1)
    third = jnp.concatenate([full(ga), full(gb), full(gc), full(gd)], 1)
    at = lax.broadcasted_iota(jnp.int32, (16, 1024), 0)
    rows = jnp.where(at == 0, first, jnp.where(at == 1, second, jnp.where(at == 2, third, 0.0)))
    for half in range(2):
        packed[half, 128:144, :] = rounded(rows)


def pack_feed(up_weight, down_weight, up_packed, down_packed, sems):
    quarter, _, _, _ = spot()
    copies = []
    for half in range(2):
        for there in range(4):
            lanes = pl.ds(pl.multiple_of(there * 1024 + quarter * 256, 256), 256)
            copies.append(
                (
                    up_weight.at[half * 128 : half * 128 + 128, lanes],
                    up_packed.at[half, :, there * 256 : there * 256 + 256],
                )
            )
        copies.append((down_weight.at[aligned(quarter * 2 + half, 128), :], down_packed.at[half]))
    copies = [pltpu.make_async_copy(a, b, sems.at[i]) for i, (a, b) in enumerate(copies)]
    for copy in copies:
        copy.start()
    for copy in copies:
        copy.wait()


def call_pack_feed(up_weight, down_weight):
    spec = pl.BlockSpec(memory_space=pl.ANY)
    return pl.pallas_call(
        pack_feed,
        out_shape=(shaped(2, 128, 1024), shaped(2, 128, 1024)),
        in_specs=[spec, spec],
        out_specs=(VMEM_SPEC, VMEM_SPEC),
        scratch_shapes=[pltpu.SemaphoreType.DMA((10,))],
        compiler_params=pltpu.CompilerParams(vmem_limit_bytes=8 << 20),
        cost_estimate=pl.CostEstimate(flops=0, bytes_accessed=2 << 20, transcendentals=0),
        name="pack_feed",
    )(up_weight, down_weight)


def tie(value, *earlier):
    return lax.optimization_barrier((value, *earlier))[0]


def near_pieces(packed, half, *earlier, direct=False):
    mine = tie(lax.dynamic_index_in_dim(packed, half, 0, False), *earlier)
    if direct:
        return [flip(mine, step) for step in (1, 2, 3)]
    second = flip(mine, 2)
    return [flip(mine, 1), second, flip(second, 1)]


def far_pieces(near):
    return [swap(item, Y) for item in near]


def far_together(near):
    return swap(jnp.stack(near), Y)


def each_piece(own, near, far):
    _, place, y_bit, _ = spot()
    yield place, 0, own.at[0]
    yield place, 1, own.at[1]
    for step in (1, 2, 3):
        yield place ^ step, y_bit, near[step - 1]
        yield place ^ step, 1 - y_bit, far[step - 1]


def head_lanes(shape, parity):
    return (lax.broadcasted_iota(jnp.int32, shape, 1) // 64) == parity


def causal_block():
    shape = (BLOCK, BLOCK)
    return lax.broadcasted_iota(jnp.int32, shape, 0) >= lax.broadcasted_iota(jnp.int32, shape, 1)


def attend(
    x0, x1, x2, x3, own, z1, z2, z3, y1, y2, y3, cosines, sines,
    query, key, value, mixed, logs, hidden, qkv, out_rows, vectors, p0, p1, p32,
):
    _, _, _, position = spot()
    for relative, rows_in in enumerate((x0, x1, x2, x3)):
        hidden[aligned(position ^ relative, BLOCK), :] = rows_in[...]
    vectors[...] = jnp.zeros_like(vectors)
    for index, (shard, half, piece) in enumerate(each_piece(own, (z1, z2, z3), (y1, y2, y3))):
        qkv[aligned(shard * 2 + half, 128), :] = piece[:128, :768]
        for j in range(2):
            out_rows[aligned(shard, 64), aligned(half * 2 + j, 256)] = piece[j * 64 : j * 64 + 64, 768:]
        if index == 0 or index >= 2 and index % 2 == 0:
            small = wide(piece[128:144, :])
            lanes = aligned(shard, 256)
            vectors[0:1, lanes] = small[1:2, 256:512]
            vectors[1:2, lanes] = small[1:2, 512:768]
            for gain in range(4):
                vectors[2 + gain : 3 + gain, lanes] = small[2:3, gain * 256 : gain * 256 + 256]
            vectors[6:7, lanes] = small[1:2, :256]
            vectors[7:8, :] += small[0:1, :]

    def project(index, carry):
        rows = aligned(index, BLOCK)
        normed, _ = standardize(wide(hidden[rows, :]))
        block = rounded(normed * vectors[2:3, :])
        hidden[rows, :] = block
        raw = dot(block, qkv[...]) + vectors[7:8, :768]
        cos, sin = cosines[rows, :], sines[rows, :]
        for tile in range(2):
            at = tile * 128
            lanes = slice(at, at + 128)
            query[rows, lanes] = rounded(turn(raw[:, lanes], cos, sin)) * jnp.bfloat16(0.125)
            key[rows, lanes] = rounded(turn(raw[:, 256 + at : 384 + at], cos, sin))
        value[rows, :] = rounded(raw[:, 512:])
        return carry

    lax.fori_loop(0, GROUP, project, 0)
    causal = causal_block()
    logs[...] = jnp.zeros_like(logs)
    mixed[...] = jnp.zeros_like(mixed)
    lane = lax.broadcasted_iota(jnp.int32, (BLOCK, 128), 1)

    def head(index, carry):
        lanes = aligned(index >> 1, 128)
        mine = lane // 64 == (index & 1)
        for block in range(GROUP):
            rows = slice(block * BLOCK, block * BLOCK + BLOCK)
            seen = (block + 1) * BLOCK
            masked = jnp.where(mine, query[rows, lanes], jnp.bfloat16(0))
            scores = nt(masked, key[:seen, lanes])
            last = jnp.where(causal, scores[:, seen - BLOCK :], -1e30)
            scores = jnp.concatenate([scores[:, : seen - BLOCK], last], 1) if block else last
            best = jnp.max(scores, axis=1, keepdims=True)
            exps = jnp.exp(scores - best)
            total = jnp.sum(exps, axis=1, keepdims=True)
            out = dot(rounded(exps), value[:seen, lanes]) / total
            mixed[rows, lanes] = jnp.where(mine, rounded(out), mixed[rows, lanes])
            logs[rows, :] = jnp.where(lane == index, best + jnp.log(total), logs[rows, :])
        return carry

    lax.fori_loop(0, 4, head, 0)
    for relative, part in enumerate((p0, p1, p32.at[BLOCK:], p32.at[:BLOCK])):
        part[...] = rounded(dot(mixed[aligned(position ^ relative, BLOCK), :], out_rows[...]))


def pair_back(pair, query, key, value, mixed, logs, d_out, d_query, d_key, d_value):
    lanes = slice(pair * 128, pair * 128 + 128)
    causal = causal_block()
    lane = lax.broadcasted_iota(jnp.int32, (BLOCK, 128), 1)
    d_key[...] = jnp.zeros_like(d_key)
    d_value[...] = jnp.zeros_like(d_value)
    d_query[...] = jnp.zeros_like(d_query)

    def head(parity, carry):
        mine = lane // 64 == parity
        for block in range(GROUP):
            rows = slice(block * BLOCK, block * BLOCK + BLOCK)
            seen = (block + 1) * BLOCK
            keys, values = key[:seen, lanes], value[:seen, lanes]
            masked_q = jnp.where(mine, query[rows, lanes], jnp.bfloat16(0))
            masked_d = jnp.where(mine, d_out[rows, lanes], jnp.bfloat16(0))
            log = jnp.sum(jnp.where(lane == pair * 2 + parity, logs[rows, :], 0.0), 1, keepdims=True)
            delta = jnp.sum(wide(masked_d) * wide(mixed[rows, lanes]), 1, keepdims=True)
            probs = jnp.exp(nt(masked_q, keys) - log)
            last = jnp.where(causal, probs[:, seen - BLOCK :], 0.0)
            probs = jnp.concatenate([probs[:, : seen - BLOCK], last], 1) if block else last
            d_scores = rounded(probs * (nt(masked_d, values) - delta))
            d_query[rows, :] += jnp.where(mine, dot(d_scores, keys), 0.0)
            d_value[:seen, :] += tn(rounded(probs), masked_d)
            d_key[:seen, :] += tn(d_scores, masked_q)
        return carry

    lax.fori_loop(0, 2, head, 0)


def finish_back(cosines, sines, d_query, d_key, d_value, grads, shift_sums):
    shift_sums[...] = jnp.zeros_like(shift_sums)

    def finish(index, carry):
        rows = aligned(index, BLOCK)
        cos, sin = cosines[rows, :], -sines[rows, :]
        grads[rows, :128] = rounded(turn(d_query[rows, :] * 0.125, cos, sin))
        grads[rows, 128:256] = rounded(turn(d_key[rows, :], cos, sin))
        grads[rows, 256:] = rounded(d_value[rows, :])
        shift_sums[0:1, :] += jnp.sum(wide(grads[rows, :]), axis=0, keepdims=True)
        return carry

    lax.fori_loop(0, GROUP, finish, 0)


def attend_back_first(
    a0, a1, a2, a3, out_rows, query, key, value, mixed, logs, cosines, sines,
    d_out, grads, shift_sums, d_query, d_key, d_value,
):
    _, _, _, position = spot()
    for relative, rows_in in enumerate((a0, a1, a2, a3)):
        d_out[aligned(position ^ relative, BLOCK), :] = rounded(nt(rows_in[...], out_rows[...]))
    pair_back(0, query, key, value, mixed, logs, d_out, d_query, d_key, d_value)
    finish_back(cosines, sines, d_query, d_key, d_value, grads, shift_sums)


def attend_back_second(
    d_out, before, qkv, query, key, value, mixed, logs, cosines, sines,
    grads, shift_sums, p0, p1, p32, d_query, d_key, d_value, joined,
):
    _, _, _, position = spot()
    pair_back(1, query, key, value, mixed, logs, d_out, d_query, d_key, d_value)
    finish_back(cosines, sines, d_query, d_key, d_value, grads, shift_sums)
    for index in range(3):
        joined[:, index * 256 : index * 256 + 128] = before[:, index * 128 : index * 128 + 128]
        joined[:, index * 256 + 128 : index * 256 + 256] = grads[:, index * 128 : index * 128 + 128]
    for relative, part in enumerate((p0, p1, p32.at[BLOCK:], p32.at[:BLOCK])):
        part[...] = rounded(nt(joined[aligned(position ^ relative, BLOCK), :], qkv[...]))


CHUNK = 64


def in_chunks(step):
    def one(index, carry):
        step(aligned(index, CHUNK), pl.ds(pl.multiple_of(BLOCK + index * CHUNK, CHUNK), CHUNK))
        return carry

    lax.fori_loop(0, BLOCK // CHUNK, one, 0)


def after_attention(p0, core_in, x_in, rows_in, vectors, middle, hidden, normed_o, normed_f, inverses):
    def step(rows, low):
        branch = wide(p0[rows, :]) + wide(core_in[low, :]) + wide(x_in[rows, :]) + vectors[0:1, :]
        normed, inverse_o = standardize(branch)
        normed_o[rows, :] = normed
        total = wide(rows_in[rows, :]) + normed * vectors[3:4, :]
        middle[rows, :] = total
        normed, inverse_f = standardize(total)
        normed_f[rows, :] = normed
        hidden[rows, :] = rounded(normed * vectors[4:5, :])
        lane = lax.broadcasted_iota(jnp.int32, (CHUNK, 128), 1)
        inverses[rows, :] = jnp.where(lane < 64, inverse_o, inverse_f)

    in_chunks(step)


def after_feed(p0, core_in, x_in, middle, cotangent, vectors, layer_out, d_branch, sums):
    sums[...] = jnp.zeros_like(sums)

    def step(rows, low):
        branch = wide(p0[rows, :]) + wide(core_in[low, :]) + wide(x_in[rows, :]) + vectors[1:2, :]
        normed, inverse = standardize(branch)
        gain = vectors[5:6, :]
        layer_out[rows, :] = rounded(middle[rows, :] + normed * gain)
        upstream = wide(cotangent[rows, :])
        back = rounded(norm_back(normed, inverse, upstream * gain))
        d_branch[rows, :] = back
        sums[0:1, :] += jnp.sum(upstream * normed, axis=0, keepdims=True)
        sums[1:2, :] += jnp.sum(wide(back), axis=0, keepdims=True)

    in_chunks(step)


def after_feed_back(
    p0, core_in, x_in, cotangent, normed_o, normed_f, inverses, vectors, d_middle, d_branch, sums
):
    sums[...] = jnp.zeros_like(sums)

    def step(rows, low):
        d_hidden = wide(p0[rows, :]) + wide(core_in[low, :]) + wide(x_in[rows, :])
        normed = normed_f[rows, :]
        sums[0:1, :] += jnp.sum(d_hidden * normed, axis=0, keepdims=True)
        total = wide(cotangent[rows, :]) + norm_back(
            normed, inverses[rows, 64:65], d_hidden * vectors[4:5, :]
        )
        d_middle[rows, :] = total
        normed = normed_o[rows, :]
        sums[1:2, :] += jnp.sum(total * normed, axis=0, keepdims=True)
        back = rounded(norm_back(normed, inverses[rows, 0:1], total * vectors[3:4, :]))
        d_branch[rows, :] = back
        sums[2:3, :] += jnp.sum(wide(back), axis=0, keepdims=True)

    in_chunks(step)


def gain_in_sums(p0, p1, p32, x0, x1, x2, x3, sums):
    sums[...] = jnp.zeros_like(sums)

    def step(rows, low):
        for part, rows_in in ((p0[rows, :], x0), (p1[rows, :], x1), (p32[low, :], x2), (p32[rows, :], x3)):
            normed, _ = standardize(wide(rows_in[rows, :]))
            sums[0:1, :] += jnp.sum(wide(part) * normed, axis=0, keepdims=True)

    in_chunks(step)


def after_attention_back(p0, core_in, x_in, rows_in, d_middle, vectors, d_rows):
    def step(rows, low):
        d_hidden = wide(p0[rows, :]) + wide(core_in[low, :]) + wide(x_in[rows, :])
        normed, inverse = standardize(wide(rows_in[rows, :]))
        d_rows[rows, :] = rounded(
            d_middle[rows, :] + norm_back(normed, inverse, d_hidden * vectors[2:3, :])
        )

    in_chunks(step)


GELU_SCALE = math.sqrt(2.0 / math.pi)


def feed_rows(rows_in, up_mat, down_mat, vectors, before, after, part, at):
    rows = slice(at, at + BLOCK)

    def step(index, carry):
        lanes = aligned(index, BLOCK)
        raw = dot(rows_in[...], up_mat[:, lanes]) + vectors[6:7, lanes]
        before[rows, lanes] = raw
        after[rows, lanes] = rounded(jax.nn.gelu(raw))
        return carry

    lax.fori_loop(0, 4, step, 0)

    def out(index, carry):
        lanes = aligned(index, BLOCK)
        part[:, lanes] = rounded(dot(after[rows, :], down_mat[:, lanes]))
        return carry

    lax.fori_loop(0, 4, out, 0)


def feed_first(
    h0, h2, uo, u1, u2, u3, far_u, do, d1, d2, d3, far_d, vectors,
    up_mat, down_mat, before, after, p0, p2,
):
    for shard, half, piece in each_piece(uo, (u1, u2, u3), [far_u.at[i] for i in range(3)]):
        up_mat[aligned(shard * 2 + half, 128), :] = piece[...]
    for shard, half, piece in each_piece(do, (d1, d2, d3), [far_d.at[i] for i in range(3)]):
        down_mat[aligned(shard * 2 + half, 128), :] = piece[...]
    feed_rows(h0, up_mat, down_mat, vectors, before, after, p0, 0)
    feed_rows(h2, up_mat, down_mat, vectors, before, after, p2, BLOCK)


def feed_second(h1, h3, p2, up_mat, down_mat, vectors, before, after, p1, p32):
    p32[BLOCK:, :] = p2[...]
    feed_rows(h3, up_mat, down_mat, vectors, before, after, p32.at[:BLOCK], BLOCK)
    feed_rows(h1, up_mat, down_mat, vectors, before, after, p1, 0)


def feed_back_rows(rows_in, up_mat, down_mat, before, d_pre, part, sums, at):
    rows = slice(at, at + BLOCK)

    def step(index, carry):
        lanes = aligned(index, BLOCK)
        upstream = nt(rows_in[...], down_mat[lanes, :])
        raw = before[rows, lanes]
        square = raw * raw
        bent = jnp.tanh(GELU_SCALE * raw * (1.0 + 0.044715 * square))
        slope = 0.5 * (1.0 + bent) + 0.5 * GELU_SCALE * raw * (1.0 - bent * bent) * (
            1.0 + 3.0 * 0.044715 * square
        )
        back = rounded(upstream * slope)
        d_pre[rows, lanes] = back
        sums[0:1, lanes] += jnp.sum(wide(back), axis=0, keepdims=True)
        return carry

    lax.fori_loop(0, 4, step, 0)

    def out(index, carry):
        lanes = aligned(index, BLOCK)
        part[:, lanes] = rounded(nt(d_pre[rows, :], up_mat[lanes, :]))
        return carry

    lax.fori_loop(0, 4, out, 0)


def feed_back_first(m0, m2, up_mat, down_mat, before, d_pre, p0, p2, sums):
    sums[...] = jnp.zeros_like(sums)
    feed_back_rows(m0, up_mat, down_mat, before, d_pre, p0, sums, 0)
    feed_back_rows(m2, up_mat, down_mat, before, d_pre, p2, sums, BLOCK)


def feed_back_second(m1, m3, p2, up_mat, down_mat, before, sums_in, d_pre, p1, p32, sums):
    sums[...] = sums_in[...]
    p32[BLOCK:, :] = p2[...]
    feed_back_rows(m3, up_mat, down_mat, before, d_pre, p32.at[:BLOCK], sums, BLOCK)
    feed_back_rows(m1, up_mat, down_mat, before, d_pre, p1, sums, 0)


def put_halves(keep, send, step, at, top, bottom):
    _, _, y_bit, _ = spot()

    @pl.when(y_bit == 0)
    def _():
        keep[step, at : at + 128, :] = top
        send[step, at : at + 128, :] = bottom

    @pl.when(y_bit == 1)
    def _():
        keep[step, at : at + 128, :] = bottom
        send[step, at : at + 128, :] = top


def down_grads(first, second, m0, m1, m2, m3, keep, send):
    _, place, _, _ = spot()

    def one(step, carry):
        lanes = aligned(place ^ step, BLOCK)
        down = (
            tn(first[:BLOCK, lanes], m0[...])
            + tn(first[BLOCK:, lanes], m2[...])
            + tn(second[:BLOCK, lanes], m1[...])
            + tn(second[BLOCK:, lanes], m3[...])
        )
        down = rounded(down)
        put_halves(keep, send, step, 0, down[:128], down[128:])
        return carry

    lax.fori_loop(0, 4, one, 0)


def up_grads(h0, h1, h2, h3, u_first, u_second, keep, send):
    _, place, _, _ = spot()

    def one(step, carry):
        lanes = aligned(place ^ step, BLOCK)
        up = (
            tn(h0[:, lanes], u_first[:BLOCK, :])
            + tn(h2[:, lanes], u_first[BLOCK:, :])
            + tn(h1[:, lanes], u_second[:BLOCK, :])
            + tn(h3[:, lanes], u_second[BLOCK:, :])
        )
        up = rounded(up)
        put_halves(keep, send, step, 0, up[:128], up[128:])
        return carry

    lax.fori_loop(0, 4, one, 0)


def attention_grads_first(mixed, a0, a1, a2, a3, hidden, grads, keep, send, out_grad, block):
    _, place, _, position = spot()
    total = tn(mixed[aligned(position, BLOCK), :], a0[...])
    for relative, rows_in in ((1, a1), (2, a2), (3, a3)):
        total = total + tn(mixed[aligned(position ^ relative, BLOCK), :], rows_in[...])
    out_grad[...] = rounded(total)

    def one(step, carry):
        shard = place ^ step
        block[:, :384] = rounded(tn(hidden[:, aligned(shard, BLOCK)], grads[...]))
        mine = out_grad[aligned(shard, 64), :]
        for j in range(4):
            block[j * 64 : j * 64 + 64, 384:] = mine[:, j * 256 : j * 256 + 256]
        put_halves(keep, send, step, 0, block[:128, :], block[128:, :])
        return carry

    lax.fori_loop(0, 4, one, 0)


def attention_grads_second(
    hidden, grads, sums_f, sums_b, sums_a, sums_u, sums_q, sums_r, keep, send
):
    _, place, y_bit, _ = spot()

    def one(step, carry):
        shard = place ^ step
        block = rounded(tn(hidden[:, aligned(shard, BLOCK)], grads[...]))
        put_halves(keep, send, step, 0, block[:128], block[128:])
        lanes = aligned(shard, BLOCK)
        biases = []
        for index in range(3):
            at = index * 128
            pair = jnp.where(shard < 2, sums_q[0:1, at : at + 128], sums_r[0:1, at : at + 128])
            biases.append(jnp.where((shard & 1) == 0, pair[:, :64], pair[:, 64:]))
        zero = jnp.zeros((1, 192), jnp.float32)
        tops = [sums_b[2:3, lanes], sums_f[1:2, lanes], sums_a[0:1, lanes], *biases, zero]
        lows = [sums_b[1:2, lanes], sums_b[0:1, lanes], sums_f[0:1, lanes], sums_u[0:1, lanes], zero[:, :128]]
        halves = []
        for items in (tops, lows):
            flat = jnp.concatenate(items, 1)
            row = lax.broadcasted_iota(jnp.int32, (8, 384), 0)
            full = [jnp.broadcast_to(flat[:, i * 384 : i * 384 + 384], (8, 384)) for i in range(3)]
            rows = jnp.where(row == 0, full[0], jnp.where(row == 1, full[1], full[2]))
            halves.append(rounded(jnp.where(row < 3, rows, 0.0)))
        mine, other = jnp.where(y_bit == 0, halves[0], halves[1]), jnp.where(y_bit == 0, halves[1], halves[0])
        keep[step, 128:136, :] = mine
        send[step, 128:136, :] = other
        return carry

    lax.fori_loop(0, 4, one, 0)


def add_pairs(keep, come, stay, go):
    for step, out in enumerate((stay.at[0], go.at[0], stay.at[1], go.at[1])):
        out[...] = rounded(wide(keep[step]) + wide(come[step]))


def add_near(stay, come, own, go):
    own[...] = rounded(wide(stay[0]) + wide(come[0]))
    go[...] = rounded(wide(stay[1]) + wide(come[1]))


def each_part(own, x_part, y_part, core_part):
    rep = lax.axis_index("rep")
    refs = [own, x_part, y_part.at[0], y_part.at[1]] + [core_part.at[i] for i in range(4)]
    for relative, ref in enumerate(refs):
        flip = ((relative & 1) << 1) | ((relative & 2) << 1) | (relative >> 2)
        there = rep ^ flip
        yield there >> 2, there & 3, ref


def unpack_down(own, x_part, y_part, core_part, down):
    for y_bit, quarter, ref in each_part(own, x_part, y_part, core_part):
        down[aligned(quarter * 2 + y_bit, 128), :] = wide(ref[...])


def unpack_up(own, x_part, y_part, core_part, up):
    for y_bit, quarter, ref in each_part(own, x_part, y_part, core_part):
        for there in range(4):
            lanes = pl.ds(pl.multiple_of(there * 1024 + quarter * 256, 256), 256)
            up[aligned(y_bit, 128), lanes] = wide(ref[:, there * 256 : there * 256 + 256])


def unpack_attention(
    own, x_part, y_part, core_part, own2, x_part2, y_part2, core_part2,
    query, key, value, out_weight, qb, kb, vb, ob, db, ga, gb, gc, gd, ub,
):
    first = list(each_part(own, x_part, y_part, core_part))
    second = list(each_part(own2, x_part2, y_part2, core_part2))
    row = lax.broadcasted_iota(jnp.int32, (128, 512), 0)
    col = lax.broadcasted_iota(jnp.int32, (128, 512), 1)
    sets = ((0, 1, 4, 5), (2, 3, 6, 7))
    chosen = []
    for index in sets[0]:
        quarter = first[index][1]
        chosen.append(rounded(wide(col == (row // 64) * 256 + quarter * 64 + row % 64)))
    chosen = jnp.concatenate(chosen, 0)
    for pair, parts in enumerate((first, second)):
        for members in sets:
            rows = aligned(parts[members[0]][0], 128)
            for index, out in enumerate((query, key, value)):
                lanes = slice(index * 128, index * 128 + 128)
                joined = jnp.concatenate([parts[i][2][:128, lanes] for i in members], 1)
                out[rows, pair * 512 : pair * 512 + 512] = dot(joined, chosen)
    for y_bit, quarter, ref in first:
        for j in range(2):
            out_weight[aligned(quarter, 64), aligned(y_bit * 2 + j, 256)] = wide(
                ref[j * 64 : j * 64 + 64, 384:]
            )
    y_bit = first[0][0]
    flats = []
    for members in sets:
        rows = [wide(second[i][2][128:136, :]) for i in members]
        total = rows[0] + rows[1] + rows[2] + rows[3]
        flats.append((total, rows))
    mine, other = flats
    for half, (outs, size) in enumerate((((ob, db, ga), 64), ((gb, gc, gd), 256))):
        take = y_bit == half
        total = jnp.where(take, mine[0], other[0])
        flat = jnp.concatenate([total[0:1, :], total[1:2, :]], 1)
        for index, out in enumerate(outs):
            out[...] = flat[:, index * 256 : index * 256 + 256]
        locals_ = [jnp.where(take, a, b)[2:3, :] for a, b in zip(mine[1], other[1], strict=True)]
        quarters = [first[i][1] for i in sets[0]]
        for there in range(4):
            value_at = jnp.zeros((1, 384), jnp.float32)
            for quarter, item in zip(quarters, locals_, strict=True):
                value_at = value_at + jnp.where(quarter == there, item, 0.0)
            if half == 0:
                for index, out in enumerate((qb, kb, vb)):
                    out[:, there * 64 : there * 64 + 64] = value_at[:, index * 64 : index * 64 + 64]
            else:
                ub[:, there * 256 : there * 256 + 256] = value_at[:, :256]


def sum_pairs(keep, come):
    two = shaped(2, *keep.shape[1:])
    return call(add_pairs, [two, two], keep, come)


def sum_near(stay, come):
    one = shaped(*stay.shape[1:])
    return call(add_near, [one, one], stay, come)


def sum_far(own, come):
    return rounded(wide(own) + wide(come))


def gather_packs(total, *earlier):
    x_part = swap(total, X)
    two = jnp.stack([total, x_part])
    y_part = swap(two, Y)
    return total, x_part, y_part, swap(tie(jnp.concatenate([two, y_part]), *earlier), CORE)


def fast_device(
    layer_input,
    query_weight,
    query_bias,
    key_weight,
    key_bias,
    value_weight,
    value_bias,
    output_weight,
    output_bias,
    up_weight,
    up_bias,
    down_weight,
    down_bias,
    attention_gain_in,
    attention_gain_out,
    feedforward_gain_in,
    feedforward_gain_out,
    layer_cotangent,
):
    f32, bf16 = jnp.float32, jnp.bfloat16
    replicas = lax.axis_size("rep")
    rows, width = layer_input.shape
    tokens = rows * GROUP
    quarter, place, y_bit, _ = spot()
    pairs = token_pairs(replicas)
    back_pairs = [(there, here) for here, there in pairs]
    both = ("rep", "shard")
    part = shaped(rows, width)
    part32 = shaped(rows, width, kind=f32)
    sums = shaped(8, width, kind=f32)

    def spread(piece):
        return swap(piece, X), swap(piece, CORE)

    def gather_sum(p1, p32):
        core_in = swap(p32, CORE)
        return core_in, swap(rounded(wide(p1) + wide(core_in[:rows])), X)

    own_rows = lax.ppermute(layer_input, both, pairs)
    (packed,) = call(
        pack_attention,
        [shaped(2, 144, width)],
        query_weight,
        key_weight,
        value_weight,
        output_weight,
        query_bias,
        key_bias,
        value_bias,
        up_bias,
        output_bias,
        down_bias,
        attention_gain_in,
        attention_gain_out,
        feedforward_gain_in,
        feedforward_gain_out,
    )
    near_a = near_pieces(packed, y_bit)
    cosines, sines = rope_tables(tokens, 64)
    up_packed, down_packed = call_pack_feed(up_weight, down_weight)
    own_rows = tie(own_rows, packed, cosines, sines, up_packed)
    x1, x2 = spread(own_rows)
    blocks = own_rows, x1, x2, swap(x1, CORE)
    far_a = far_pieces(near_a)
    near_u = near_pieces(up_packed, y_bit, *near_a)
    cotangent = lax.ppermute(tie(layer_cotangent, *near_u), both, pairs)
    two16 = shaped(2 * rows, width)
    head_rows = shaped(tokens, 256)
    query, key, value, mixed, logs, hidden_a, qkv, out_rows, vectors, p0, p1, p32 = call(
        attend,
        [head_rows] * 4
        + [
            shaped(tokens, 128, kind=f32),
            shaped(tokens, width),
            shaped(width, 768),
            shaped(256, width),
            sums,
        ]
        + [part, part, two16],
        *blocks,
        packed,
        *near_a,
        *far_a,
        cosines,
        sines,
        flops=2 * tokens * 1024 * 1024 + 8 * tokens * tokens * 64 * 2,
        exps=2 * tokens * tokens,
        room=14,
    )
    p32 = tie(p32, *near_u)
    far_u = far_together(near_u)
    near_d = near_pieces(down_packed, y_bit, *near_u)
    core_in, x_in = gather_sum(p1, p32)
    x_in = tie(x_in, far_u, cotangent, *near_d)
    far_d = far_together(near_d)
    middle, hidden_own, normed_o, normed_f, inverses = call(
        after_attention,
        [part32, part, part32, part32, shaped(rows, 128, kind=f32)],
        p0,
        core_in,
        x_in,
        own_rows,
        vectors,
    )
    h0 = hidden_own
    h1, h2 = spread(h0)
    two32 = shaped(2 * rows, width, kind=f32)
    square = shaped(width, width)
    flops = 4 * 2 * rows * 1024 * 1024
    up_mat, down_mat, before_a, after_a, p0, p2 = call(
        feed_first,
        [square, square, two32, two16, part, part],
        h0, h2, up_packed, *near_u, far_u, down_packed, *near_d, far_d, vectors,
        flops=flops, room=10,
    )
    h1 = tie(h1, p2)
    h3 = swap(h1, CORE)
    before_b, after_b, p1, p32 = call(
        feed_second,
        [two32, two16, part, two16],
        h1, h3, p2, up_mat, down_mat, vectors,
        flops=flops, room=10,
    )
    core_in, x_in = gather_sum(p1, p32)
    layer_output, d_branch, sums_f = call(
        after_feed, [part, part, sums], p0, core_in, x_in, middle, cotangent, vectors
    )
    m0 = d_branch
    m1, m2 = spread(m0)
    u_first, p0, p2, sums_u = call(
        feed_back_first,
        [two16, part, part, sums],
        m0, m2, up_mat, down_mat, before_a,
        flops=flops, room=10,
    )
    m1 = tie(m1, u_first)
    m3 = swap(m1, CORE)
    layer_output = lax.ppermute(layer_output, both, back_pairs)
    m3 = tie(m3, layer_output)
    packs = [shaped(4, 128, width)] * 2
    grad_flops = 2 * tokens * 1024 * 1024
    u_second, p1, p32, sums_u = call(
        feed_back_second,
        [two16, part, two16, sums],
        m1, m3, p2, up_mat, down_mat, before_b, sums_u,
        flops=flops, room=10,
    )
    core_in, x_in = gather_sum(p1, p32)
    pack_d = call(
        down_grads, packs, after_a, after_b, m0, m1, m2, tie(m3, u_second), flops=grad_flops, room=10
    )
    come_d = swap(pack_d[1], Y)
    pack_u = call(
        up_grads,
        packs,
        h0, h1, h2, h3, u_first, tie(u_second, *pack_d),
        flops=grad_flops, room=10,
    )
    flops = grad_flops
    x_in = tie(x_in, *pack_u)
    d_middle, d_branch, sums_b = call(
        after_feed_back,
        [part32, part, sums],
        p0,
        core_in,
        x_in,
        cotangent,
        normed_o,
        normed_f,
        inverses,
        vectors,
    )
    a0 = d_branch
    a1, a2 = spread(a0)
    stay_d, go_d = sum_pairs(tie(pack_d[0], d_branch), come_d)
    come_u = swap(pack_u[1], Y)
    a1 = tie(a1, go_d)
    a3 = swap(a1, CORE)
    a_blocks = a0, a1, a2, a3
    come_d = flip(go_d, 1)
    grad32 = [pltpu.VMEM((tokens, 128), f32)] * 3
    back_flops = tokens * 1024 * 1024 + 10 * tokens * tokens * 64 * 2
    d_out, grads_first, sums_q = call(
        attend_back_first,
        [shaped(tokens, 256), shaped(tokens, 384), shaped(8, 384, kind=f32)],
        *a_blocks, out_rows, query, key, value, mixed, logs, cosines, sines,
        scratch=grad32, flops=back_flops, exps=tokens * tokens, room=14,
    )
    pack_a = call(
        attention_grads_first,
        [shaped(4, 128, 640)] * 2,
        mixed, *a_blocks, hidden_a, grads_first,
        scratch=[pltpu.VMEM((256, width), bf16), pltpu.VMEM((256, 640), bf16)],
        flops=flops // 2, room=10,
    )
    grads_second, sums_r, p0, p1, p32 = call(
        attend_back_second,
        [shaped(tokens, 384), shaped(8, 384, kind=f32), part, part, two16],
        tie(d_out, *pack_a), grads_first, qkv, query, key, value, mixed, logs, cosines, sines,
        scratch=grad32 + [pltpu.VMEM((tokens, 768), bf16)],
        flops=back_flops, exps=tokens * tokens, room=14,
    )
    come_a = swap(pack_a[1], Y)
    p32 = tie(p32, come_u, come_d)
    core_in, x_in = gather_sum(p1, p32)
    own_d, go_d = sum_near(tie(stay_d, p32), come_d)
    come_d = flip(go_d, 2)
    stay_u, go_u = sum_pairs(tie(pack_u[0], p32), come_u)
    (sums_a,) = call(gain_in_sums, [sums], p0, p1, p32, *blocks)
    pack_b = call(
        attention_grads_second,
        [shaped(4, 136, 384)] * 2,
        hidden_a, grads_second, sums_f, sums_b, sums_a, sums_u, sums_q, sums_r,
        flops=flops // 2, room=10,
    )
    x_in = tie(x_in, *pack_b, go_u)
    (d_rows,) = call(
        after_attention_back, [part], p0, core_in, x_in, own_rows, d_middle, vectors
    )
    input_gradient = lax.ppermute(d_rows, both, back_pairs)
    total_d = sum_far(tie(own_d, d_rows), come_d)
    own_u, go_u = sum_near(tie(stay_u, d_rows), flip(go_u, 1))
    stay_a, go_a = sum_pairs(tie(pack_a[0], d_rows), come_a)
    own_a, go_a = sum_near(stay_a, flip(go_a, 1))
    stay_b, go_b = sum_pairs(pack_b[0], swap(pack_b[1], Y))
    total_u = sum_far(own_u, flip(go_u, 2))
    own_b, go_b = sum_near(tie(stay_b, input_gradient), flip(go_b, 1))
    total_a = sum_far(own_a, flip(go_a, 2))
    total_b = sum_far(own_b, flip(go_b, 2))
    (g_down,) = call(unpack_down, [shaped(*down_weight.shape, kind=f32)], *gather_packs(total_d))
    (g_up,) = call(unpack_up, [shaped(*up_weight.shape, kind=f32)], *gather_packs(total_u))
    packs_a = gather_packs(total_a)
    packs_b = gather_packs(total_b, g_down)
    g_query, g_key, g_value, g_out, *small = call(
        unpack_attention,
        [part32] * 4 + [shaped(1, 256, kind=f32)] * 9 + [shaped(1, 1024, kind=f32)],
        *packs_a,
        *packs_b,
    )
    small = [item.reshape(-1) for item in small]
    input_gradient = input_gradient.astype(f32)
    return (
        layer_output,
        input_gradient,
        g_query,
        small[0],
        g_key,
        small[1],
        g_value,
        small[2],
        g_out,
        small[3],
        g_up,
        small[9],
        g_down,
        small[4],
        small[5],
        small[6],
        small[7],
        small[8],
    )


def solution(mesh):
    replicas, shards = mesh.shape["rep"], mesh.shape["shard"]
    fits = shards == 4 and replicas == 8 and HEADS % 16 == 0
    return jax.shard_map(
        fast_device if fits else general_device,
        mesh=mesh,
        in_specs=(
            P(("rep", "shard"), None),
            P("shard", None),
            P("shard"),
            P("shard", None),
            P("shard"),
            P("shard", None),
            P("shard"),
            P("shard", None),
            P("shard"),
            P("shard", None),
            P("shard"),
            P("shard", None),
            P("shard"),
            P("shard"),
            P("shard"),
            P("shard"),
            P("shard"),
            P(("rep", "shard"), None),
        ),
        out_specs=(
            P(("rep", "shard"), None),
            P(("rep", "shard"), None),
            P("shard", None),
            P("shard"),
            P("shard", None),
            P("shard"),
            P("shard", None),
            P("shard"),
            P("shard", None),
            P("shard"),
            P("shard", None),
            P("shard"),
            P("shard", None),
            P("shard"),
            P("shard"),
            P("shard"),
            P("shard"),
            P("shard"),
        ),
        check_vma=False,
    )
```

```python
import functools
import math

import jax
import jax.numpy as jnp
import numpy as np
from jax import lax
from jax.experimental import pallas as pl
from jax.experimental.pallas import tpu as pltpu
from jax.sharding import PartitionSpec as P

HEADS = 16


norm_epsilon = 1e-05


def normalize(values):
    centered = values - jnp.mean(values, axis=-1, keepdims=True)
    inverse = lax.rsqrt(jnp.mean(centered * centered, axis=-1, keepdims=True) + norm_epsilon)
    return (centered * inverse, inverse)


def norm_back(normed, inverse, upstream):
    return inverse * (
        upstream
        - jnp.mean(upstream, axis=-1, keepdims=True)
        - normed * jnp.mean(upstream * normed, axis=-1, keepdims=True)
    )


def rotation(positions, head_dim):
    half_dim = head_dim // 2
    freqs = 10000.0 ** (-jnp.arange(half_dim, dtype=jnp.float32) / half_dim)
    angles = positions.astype(jnp.float32)[:, None] * freqs[None, :]
    return (jnp.cos(angles)[:, None, :], jnp.sin(angles)[:, None, :])


def rotate(tensor, cosines, sines, sign):
    half_dim = tensor.shape[-1] // 2
    first = tensor[..., :half_dim]
    second = tensor[..., half_dim:]
    return jnp.concatenate(
        [first * cosines - sign * second * sines, second * cosines + sign * first * sines], axis=-1
    )


def col_sum(values):
    return jnp.sum(values.astype(jnp.float32), axis=0)


def general_device(
    layer_input,
    query_weight,
    query_bias,
    key_weight,
    key_bias,
    value_weight,
    value_bias,
    output_weight,
    output_bias,
    up_weight,
    up_bias,
    down_weight,
    down_bias,
    attention_gain_in,
    attention_gain_out,
    feedforward_gain_in,
    feedforward_gain_out,
    layer_cotangent,
):
    rows = layer_input.shape[0]
    width = layer_input.shape[1]
    heads = HEADS
    head_dim = width // heads
    seq_rows = rows * lax.axis_size("shard")
    factor = head_dim ** (-0.5)
    positions = lax.axis_index("shard") * rows + jnp.arange(rows, dtype=jnp.int32)
    cosines, sines = rotation(positions, head_dim)
    attention_local = (
        query_weight,
        key_weight,
        value_weight,
        output_weight,
        query_bias,
        key_bias,
        value_bias,
        output_bias,
        attention_gain_in,
        attention_gain_out,
    )
    feed_local = (
        up_weight,
        up_bias,
        down_weight,
        down_bias,
        feedforward_gain_in,
        feedforward_gain_out,
    )
    attention_full = (
        lax.all_gather(attention_local[0], "shard", axis=0, tiled=True),
        lax.all_gather(attention_local[1], "shard", axis=0, tiled=True),
        lax.all_gather(attention_local[2], "shard", axis=0, tiled=True),
        lax.all_gather(attention_local[3], "shard", axis=0, tiled=True),
        lax.all_gather(attention_local[4], "shard", axis=0, tiled=True),
        lax.all_gather(attention_local[5], "shard", axis=0, tiled=True),
        lax.all_gather(attention_local[6], "shard", axis=0, tiled=True),
        lax.all_gather(attention_local[7], "shard", axis=0, tiled=True),
        lax.all_gather(attention_local[8], "shard", axis=0, tiled=True),
        lax.all_gather(attention_local[9], "shard", axis=0, tiled=True),
    )
    (
        query_mat,
        key_mat,
        value_mat,
        out_mat,
        query_shift,
        key_shift,
        value_shift,
        out_shift,
        gain_in_a,
        gain_out_a,
    ) = attention_full
    residual_in = layer_input.astype(jnp.float32)
    normed_a, inverse_a = normalize(residual_in)
    hidden_a = (normed_a * gain_in_a.astype(jnp.float32)).astype(jnp.bfloat16)

    def project(matrix, shift):
        return jnp.dot(hidden_a, matrix, preferred_element_type=jnp.float32) + shift.astype(
            jnp.float32
        )

    query_heads = rotate(
        project(query_mat, query_shift).reshape(rows, heads, head_dim), cosines, sines, 1.0
    ).astype(jnp.bfloat16)
    key_rows = (
        rotate(project(key_mat, key_shift).reshape(rows, heads, head_dim), cosines, sines, 1.0)
        .astype(jnp.bfloat16)
        .reshape(rows, width)
    )
    value_rows = project(value_mat, value_shift).astype(jnp.bfloat16)
    start_state = (
        jnp.full((heads, rows), -1e30, jnp.float32),
        jnp.zeros((heads, rows), jnp.float32),
        jnp.zeros((heads, rows, head_dim), jnp.float32),
    )
    key_piece = lax.all_gather(key_rows, "shard", axis=0, tiled=True)
    value_piece = lax.all_gather(value_rows, "shard", axis=0, tiled=True)
    count = key_piece.shape[0]
    block = math.gcd(count, 512)

    def forward_inner(index, state):
        best, total, accum = state
        offset = index * block
        key_block = lax.dynamic_slice_in_dim(key_piece, offset, block, 0).reshape(
            block, heads, head_dim
        )
        value_block = lax.dynamic_slice_in_dim(value_piece, offset, block, 0).reshape(
            block, heads, head_dim
        )
        key_pos = offset + jnp.arange(block, dtype=jnp.int32)
        allowed = key_pos[None, None, :] <= positions[None, :, None]
        scores = (
            jnp.einsum("qhd,khd->hqk", query_heads, key_block, preferred_element_type=jnp.float32)
            * factor
        )
        scores = jnp.where(allowed, scores, -1e30)
        newest = jnp.maximum(best, jnp.max(scores, axis=-1))
        weights = jnp.where(allowed, jnp.exp(scores - newest[..., None]), 0.0)
        decay = jnp.exp(best - newest)
        total = total * decay + jnp.sum(weights, axis=-1)
        accum = accum * decay[..., None] + jnp.einsum(
            "hqk,khd->hqd",
            weights.astype(jnp.bfloat16),
            value_block,
            preferred_element_type=jnp.float32,
        )
        return (newest, total, accum)

    best, total, accum = lax.fori_loop(0, count // block, forward_inner, start_state)
    logsum = best + jnp.log(total)
    attended = (
        jnp.transpose(accum / total[..., None], (1, 0, 2)).reshape(rows, width).astype(jnp.bfloat16)
    )
    branch_a = jnp.dot(attended, out_mat, preferred_element_type=jnp.float32) + out_shift.astype(
        jnp.float32
    )
    normed_o, inverse_o = normalize(branch_a)
    middle = residual_in + normed_o * gain_out_a.astype(jnp.float32)
    feed_full = (
        lax.all_gather(feed_local[0], "shard", axis=0, tiled=True),
        lax.all_gather(feed_local[1], "shard", axis=0, tiled=True),
        lax.all_gather(feed_local[2], "shard", axis=0, tiled=True),
        lax.all_gather(feed_local[3], "shard", axis=0, tiled=True),
        lax.all_gather(feed_local[4], "shard", axis=0, tiled=True),
        lax.all_gather(feed_local[5], "shard", axis=0, tiled=True),
    )
    up_mat, up_shift, down_mat, down_shift, gain_in_f, gain_out_f = feed_full
    normed_f, inverse_f = normalize(middle)
    hidden_f = (normed_f * gain_in_f.astype(jnp.float32)).astype(jnp.bfloat16)
    pre_act = jnp.dot(hidden_f, up_mat, preferred_element_type=jnp.float32) + up_shift.astype(
        jnp.float32
    )
    activated = jax.nn.gelu(pre_act).astype(jnp.bfloat16)
    branch_f = jnp.dot(activated, down_mat, preferred_element_type=jnp.float32) + down_shift.astype(
        jnp.float32
    )
    normed_d, inverse_d = normalize(branch_f)
    layer_output = (middle + normed_d * gain_out_f.astype(jnp.float32)).astype(jnp.bfloat16)
    feed_back = (
        lax.all_gather(feed_local[0], "shard", axis=0, tiled=True),
        lax.all_gather(feed_local[1], "shard", axis=0, tiled=True),
        lax.all_gather(feed_local[2], "shard", axis=0, tiled=True),
        lax.all_gather(feed_local[3], "shard", axis=0, tiled=True),
        lax.all_gather(feed_local[4], "shard", axis=0, tiled=True),
        lax.all_gather(feed_local[5], "shard", axis=0, tiled=True),
    )
    up_back, up_unused, down_back, down_unused, gain_in_fb, gain_out_fb = feed_back
    upstream = layer_cotangent.astype(jnp.float32)
    grad_gain_out_f = jnp.sum(upstream * normed_d, axis=0)
    d_branch_f = norm_back(normed_d, inverse_d, upstream * gain_out_fb.astype(jnp.float32)).astype(
        jnp.bfloat16
    )
    grad_down = jnp.einsum("tf,td->fd", activated, d_branch_f, preferred_element_type=jnp.float32)
    grad_down_shift = col_sum(d_branch_f)
    d_activated = jnp.einsum("td,fd->tf", d_branch_f, down_back, preferred_element_type=jnp.float32)
    gelu_out, gelu_pull = jax.vjp(jax.nn.gelu, pre_act)
    d_pre = gelu_pull(d_activated)[0].astype(jnp.bfloat16)
    grad_up = jnp.einsum("td,tf->df", hidden_f, d_pre, preferred_element_type=jnp.float32)
    grad_up_shift = col_sum(d_pre)
    d_hidden_f = jnp.einsum("tf,df->td", d_pre, up_back, preferred_element_type=jnp.float32)
    grad_gain_in_f = jnp.sum(d_hidden_f * normed_f, axis=0)
    d_middle = upstream + norm_back(
        normed_f, inverse_f, d_hidden_f * gain_in_fb.astype(jnp.float32)
    )
    feed_grads = (
        lax.psum_scatter(
            grad_up.astype(jnp.bfloat16), "shard", scatter_dimension=0, tiled=True
        ).astype(jnp.float32),
        lax.psum_scatter(
            grad_up_shift.astype(jnp.bfloat16), "shard", scatter_dimension=0, tiled=True
        ).astype(jnp.float32),
        lax.psum_scatter(
            grad_down.astype(jnp.bfloat16), "shard", scatter_dimension=0, tiled=True
        ).astype(jnp.float32),
        lax.psum_scatter(
            grad_down_shift.astype(jnp.bfloat16), "shard", scatter_dimension=0, tiled=True
        ).astype(jnp.float32),
        lax.psum_scatter(
            grad_gain_in_f.astype(jnp.bfloat16), "shard", scatter_dimension=0, tiled=True
        ).astype(jnp.float32),
        lax.psum_scatter(
            grad_gain_out_f.astype(jnp.bfloat16), "shard", scatter_dimension=0, tiled=True
        ).astype(jnp.float32),
    )
    attention_back = (
        lax.all_gather(attention_local[0], "shard", axis=0, tiled=True),
        lax.all_gather(attention_local[1], "shard", axis=0, tiled=True),
        lax.all_gather(attention_local[2], "shard", axis=0, tiled=True),
        lax.all_gather(attention_local[3], "shard", axis=0, tiled=True),
        lax.all_gather(attention_local[4], "shard", axis=0, tiled=True),
        lax.all_gather(attention_local[5], "shard", axis=0, tiled=True),
        lax.all_gather(attention_local[6], "shard", axis=0, tiled=True),
        lax.all_gather(attention_local[7], "shard", axis=0, tiled=True),
        lax.all_gather(attention_local[8], "shard", axis=0, tiled=True),
        lax.all_gather(attention_local[9], "shard", axis=0, tiled=True),
    )
    (
        query_back,
        key_back,
        value_back,
        out_back,
        qshift_unused,
        kshift_unused,
        vshift_unused,
        oshift_unused,
        gain_in_ab,
        gain_out_ab,
    ) = attention_back
    grad_gain_out_a = jnp.sum(d_middle * normed_o, axis=0)
    d_branch_a = norm_back(normed_o, inverse_o, d_middle * gain_out_ab.astype(jnp.float32)).astype(
        jnp.bfloat16
    )
    grad_out_mat = jnp.einsum("td,te->de", attended, d_branch_a, preferred_element_type=jnp.float32)
    grad_out_shift = col_sum(d_branch_a)
    d_attended = jnp.einsum(
        "te,de->td", d_branch_a, out_back, preferred_element_type=jnp.float32
    ).astype(jnp.bfloat16)
    d_heads = d_attended.reshape(rows, heads, head_dim)
    row_delta = jnp.einsum(
        "qhd,qhd->hq",
        d_heads.astype(jnp.float32),
        attended.reshape(rows, heads, head_dim).astype(jnp.float32),
    )

    def query_terms(key_block, value_block, key_pos):
        allowed = key_pos[None, None, :] <= positions[None, :, None]
        scores = (
            jnp.einsum("qhd,khd->hqk", query_heads, key_block, preferred_element_type=jnp.float32)
            * factor
        )
        probs = jnp.where(allowed, jnp.exp(scores - logsum[..., None]), 0.0)
        d_probs = jnp.einsum(
            "qhd,khd->hqk", d_heads, value_block, preferred_element_type=jnp.float32
        )
        d_scores = (probs * (d_probs - row_delta[..., None])).astype(jnp.bfloat16)
        return (probs, d_scores)

    back_state = (
        jnp.zeros((rows, heads, head_dim), jnp.float32),
        jnp.zeros((seq_rows, width), jnp.float32),
        jnp.zeros((seq_rows, width), jnp.float32),
    )
    backward_key_piece = lax.all_gather(key_rows, "shard", axis=0, tiled=True)
    backward_value_piece = lax.all_gather(value_rows, "shard", axis=0, tiled=True)
    count = backward_key_piece.shape[0]
    backward_block = math.gcd(count, 512)

    def backward_inner(index, state):
        grad_query, grad_keys, grad_values = state
        offset = index * backward_block
        key_block = lax.dynamic_slice_in_dim(backward_key_piece, offset, backward_block, 0).reshape(
            backward_block, heads, head_dim
        )
        value_block = lax.dynamic_slice_in_dim(
            backward_value_piece, offset, backward_block, 0
        ).reshape(backward_block, heads, head_dim)
        key_pos = offset + jnp.arange(backward_block, dtype=jnp.int32)
        probs, d_scores = query_terms(key_block, value_block, key_pos)
        grad_query = (
            grad_query
            + jnp.einsum("hqk,khd->qhd", d_scores, key_block, preferred_element_type=jnp.float32)
            * factor
        )
        key_grad = (
            jnp.einsum("hqk,qhd->khd", d_scores, query_heads, preferred_element_type=jnp.float32)
            * factor
        )
        value_grad = jnp.einsum(
            "hqk,qhd->khd", probs.astype(jnp.bfloat16), d_heads, preferred_element_type=jnp.float32
        )
        grad_keys = lax.dynamic_update_slice_in_dim(
            grad_keys, key_grad.reshape(backward_block, width), offset, 0
        )
        grad_values = lax.dynamic_update_slice_in_dim(
            grad_values, value_grad.reshape(backward_block, width), offset, 0
        )
        return (grad_query, grad_keys, grad_values)

    back_result = lax.fori_loop(0, count // backward_block, backward_inner, back_state)
    grad_query = back_result[0]
    key_total, value_total = (
        lax.psum_scatter(
            back_result[1].astype(jnp.bfloat16), "shard", scatter_dimension=0, tiled=True
        ).astype(jnp.float32),
        lax.psum_scatter(
            back_result[2].astype(jnp.bfloat16), "shard", scatter_dimension=0, tiled=True
        ).astype(jnp.float32),
    )
    d_query = rotate(grad_query, cosines, sines, -1.0).reshape(rows, width).astype(jnp.bfloat16)
    d_key = (
        rotate(key_total.reshape(rows, heads, head_dim), cosines, sines, -1.0)
        .reshape(rows, width)
        .astype(jnp.bfloat16)
    )
    d_value = value_total.astype(jnp.bfloat16)
    grad_query_mat = jnp.einsum("td,te->de", hidden_a, d_query, preferred_element_type=jnp.float32)
    grad_key_mat = jnp.einsum("td,te->de", hidden_a, d_key, preferred_element_type=jnp.float32)
    grad_value_mat = jnp.einsum("td,te->de", hidden_a, d_value, preferred_element_type=jnp.float32)
    d_hidden_a = jnp.einsum("te,de->td", d_query, query_back, preferred_element_type=jnp.float32)
    d_hidden_a = d_hidden_a + jnp.einsum(
        "te,de->td", d_key, key_back, preferred_element_type=jnp.float32
    )
    d_hidden_a = d_hidden_a + jnp.einsum(
        "te,de->td", d_value, value_back, preferred_element_type=jnp.float32
    )
    grad_gain_in_a = jnp.sum(d_hidden_a * normed_a, axis=0)
    input_gradient = d_middle + norm_back(
        normed_a, inverse_a, d_hidden_a * gain_in_ab.astype(jnp.float32)
    )
    attention_grads = (
        lax.psum_scatter(
            grad_query_mat.astype(jnp.bfloat16), "shard", scatter_dimension=0, tiled=True
        ).astype(jnp.float32),
        lax.psum_scatter(
            grad_key_mat.astype(jnp.bfloat16), "shard", scatter_dimension=0, tiled=True
        ).astype(jnp.float32),
        lax.psum_scatter(
            grad_value_mat.astype(jnp.bfloat16), "shard", scatter_dimension=0, tiled=True
        ).astype(jnp.float32),
        lax.psum_scatter(
            grad_out_mat.astype(jnp.bfloat16), "shard", scatter_dimension=0, tiled=True
        ).astype(jnp.float32),
        lax.psum_scatter(
            col_sum(d_query).astype(jnp.bfloat16), "shard", scatter_dimension=0, tiled=True
        ).astype(jnp.float32),
        lax.psum_scatter(
            col_sum(d_key).astype(jnp.bfloat16), "shard", scatter_dimension=0, tiled=True
        ).astype(jnp.float32),
        lax.psum_scatter(
            col_sum(d_value).astype(jnp.bfloat16), "shard", scatter_dimension=0, tiled=True
        ).astype(jnp.float32),
        lax.psum_scatter(
            grad_out_shift.astype(jnp.bfloat16), "shard", scatter_dimension=0, tiled=True
        ).astype(jnp.float32),
        lax.psum_scatter(
            grad_gain_in_a.astype(jnp.bfloat16), "shard", scatter_dimension=0, tiled=True
        ).astype(jnp.float32),
        lax.psum_scatter(
            grad_gain_out_a.astype(jnp.bfloat16), "shard", scatter_dimension=0, tiled=True
        ).astype(jnp.float32),
    )
    (
        g_query,
        g_key,
        g_value,
        g_out,
        g_qshift,
        g_kshift,
        g_vshift,
        g_oshift,
        g_gain_in_a,
        g_gain_out_a,
    ) = attention_grads
    g_up, g_up_shift, g_down, g_down_shift, g_gain_in_f, g_gain_out_f = feed_grads
    summed = (
        lax.psum(g_query.astype(jnp.bfloat16), "rep").astype(jnp.float32),
        lax.psum(g_qshift.astype(jnp.bfloat16), "rep").astype(jnp.float32),
        lax.psum(g_key.astype(jnp.bfloat16), "rep").astype(jnp.float32),
        lax.psum(g_kshift.astype(jnp.bfloat16), "rep").astype(jnp.float32),
        lax.psum(g_value.astype(jnp.bfloat16), "rep").astype(jnp.float32),
        lax.psum(g_vshift.astype(jnp.bfloat16), "rep").astype(jnp.float32),
        lax.psum(g_out.astype(jnp.bfloat16), "rep").astype(jnp.float32),
        lax.psum(g_oshift.astype(jnp.bfloat16), "rep").astype(jnp.float32),
        lax.psum(g_up.astype(jnp.bfloat16), "rep").astype(jnp.float32),
        lax.psum(g_up_shift.astype(jnp.bfloat16), "rep").astype(jnp.float32),
        lax.psum(g_down.astype(jnp.bfloat16), "rep").astype(jnp.float32),
        lax.psum(g_down_shift.astype(jnp.bfloat16), "rep").astype(jnp.float32),
        lax.psum(g_gain_in_a.astype(jnp.bfloat16), "rep").astype(jnp.float32),
        lax.psum(g_gain_out_a.astype(jnp.bfloat16), "rep").astype(jnp.float32),
        lax.psum(g_gain_in_f.astype(jnp.bfloat16), "rep").astype(jnp.float32),
        lax.psum(g_gain_out_f.astype(jnp.bfloat16), "rep").astype(jnp.float32),
    )
    return (
        layer_output,
        input_gradient,
        summed[0],
        summed[1],
        summed[2],
        summed[3],
        summed[4],
        summed[5],
        summed[6],
        summed[7],
        summed[8],
        summed[9],
        summed[10],
        summed[11],
        summed[12],
        summed[13],
        summed[14],
        summed[15],
    )


CORE, X, Y = 1, 2, 4
GROUP = 4
BLOCK = 256


def swap(values, bit):
    count = lax.axis_size("rep")
    return lax.ppermute(values, "rep", [(i, i ^ bit) for i in range(count)])


def shift(values, step):
    count = lax.axis_size("shard")
    return lax.ppermute(values, "shard", [(i, (i + step) % count) for i in range(count)])


def flip(values, bit):
    count = lax.axis_size("shard")
    return lax.ppermute(values, "shard", [(i, i ^ bit) for i in range(count)])


def token_pairs(count):
    pairs = []
    for rep in range(count):
        for z in range(GROUP):
            there = (rep & ~3) | (((z ^ rep) & 1) << 1) | (z >> 1)
            pairs.append((rep * GROUP + z, there * GROUP + ((rep >> 1) & 1) + 2 * (rep & 1)))
    return pairs


def spot():
    rep, place = lax.axis_index("rep"), lax.axis_index("shard")
    return rep & 3, place, rep >> 2, (((rep >> 1) & 1) ^ (place >> 1)) + 2 * (rep & 1)


def aligned(index, size):
    return pl.ds(pl.multiple_of(index * size, size), size)


def dot(left, right):
    return jnp.dot(left, right, preferred_element_type=jnp.float32)


def nt(left, right):
    return lax.dot_general(left, right, (((1,), (1,)), ((), ())), preferred_element_type=jnp.float32)


def tn(left, right):
    return lax.dot_general(left, right, (((0,), (0,)), ((), ())), preferred_element_type=jnp.float32)


def rounded(values):
    return values.astype(jnp.bfloat16)


def wide(values):
    return values.astype(jnp.float32)


def shaped(*dims, kind=jnp.bfloat16):
    return jax.ShapeDtypeStruct(dims, kind)


VMEM_SPEC = pl.BlockSpec(memory_space=pltpu.VMEM)


def call(kernel, outs, *operands, scratch=(), flops=0, exps=0, room=6):
    size = lambda items: sum(math.prod(item.shape) * item.dtype.itemsize for item in items)
    moved = size(operands) + size(outs)
    spaces = [jax.ShapeDtypeStruct(item.shape, item.dtype) for item in scratch]
    return pl.pallas_call(
        kernel,
        out_shape=tuple(outs),
        in_specs=[VMEM_SPEC] * len(operands),
        out_specs=tuple([VMEM_SPEC] * len(outs)),
        scratch_shapes=list(scratch),
        compiler_params=pltpu.CompilerParams(vmem_limit_bytes=moved + size(spaces) + (room << 20)),
        cost_estimate=pl.CostEstimate(flops=flops // 40, bytes_accessed=moved // 40, transcendentals=0),
        name=kernel.__name__,
    )(*operands)


def standardize(values):
    centered = values - jnp.mean(values, axis=-1, keepdims=True)
    inverse = lax.rsqrt(jnp.mean(centered * centered, axis=-1, keepdims=True) + norm_epsilon)
    return centered * inverse, inverse


def turn(values, cosines, sines):
    lane = lax.broadcasted_iota(jnp.int32, values.shape, 1)
    swapped = jnp.where(lane % 64 < 32, pltpu.roll(values, 96, 1), pltpu.roll(values, 32, 1))
    return values * cosines + swapped * sines


def rope_tables(tokens, head_dim):
    half = head_dim // 2
    freqs = 10000.0 ** (-jnp.arange(half, dtype=jnp.float32) / half)
    angles = jnp.arange(tokens, dtype=jnp.int32).astype(jnp.float32)[:, None] * freqs[None, :]
    cosines, sines = jnp.cos(angles), jnp.sin(angles)
    return (
        jnp.concatenate([cosines] * 4, 1),
        jnp.concatenate([-sines, sines, -sines, sines], 1),
    )


def pack_attention(
    query_weight, key_weight, value_weight, out_weight, qb, kb, vb, ub, ob, db, ga, gb, gc, gd, packed
):
    quarter, place, _, _ = spot()
    row = lax.broadcasted_iota(jnp.int32, (1024, 256), 0)
    col = lax.broadcasted_iota(jnp.int32, (1024, 256), 1)
    chosen = rounded(wide(row == (col // 64) * 256 + quarter * 64 + col % 64))
    for index, weight in enumerate((query_weight, key_weight, value_weight)):
        mine = rounded(dot(weight[...], chosen))
        for half in range(2):
            packed[half, :128, index * 256 : index * 256 + 256] = mine[half * 128 : half * 128 + 128]
    out_mine = out_weight[aligned(quarter, 64), :]
    for j in range(4):
        at = (j % 2) * 64
        packed[j // 2, at : at + 64, 768:1024] = out_mine[:, j * 256 : j * 256 + 256]
    row = lax.broadcasted_iota(jnp.int32, (256, 256), 0)
    col = lax.broadcasted_iota(jnp.int32, (256, 256), 1)
    chosen = rounded(wide((row == quarter * 64 + col % 64) & (col // 64 == place)))
    biases = [dot(jnp.broadcast_to(item[...][None, :], (16, 256)), chosen) for item in (qb, kb, vb)]
    full = lambda item: jnp.broadcast_to(wide(item[...])[None, :], (16, 256))
    up_mine = jnp.broadcast_to(wide(ub[aligned(quarter, 256)])[None, :], (16, 256))
    zero = jnp.zeros((16, 256), jnp.float32)
    first = jnp.concatenate(biases + [zero], 1)
    second = jnp.concatenate([up_mine, full(ob), full(db), zero], 1)
    third = jnp.concatenate([full(ga), full(gb), full(gc), full(gd)], 1)
    at = lax.broadcasted_iota(jnp.int32, (16, 1024), 0)
    rows = jnp.where(at == 0, first, jnp.where(at == 1, second, jnp.where(at == 2, third, 0.0)))
    for half in range(2):
        packed[half, 128:144, :] = rounded(rows)


def pack_feed(up_weight, down_weight, up_packed, down_packed, sems):
    quarter, _, _, _ = spot()
    copies = []
    for half in range(2):
        for there in range(4):
            lanes = pl.ds(pl.multiple_of(there * 1024 + quarter * 256, 256), 256)
            copies.append(
                (
                    up_weight.at[half * 128 : half * 128 + 128, lanes],
                    up_packed.at[half, :, there * 256 : there * 256 + 256],
                )
            )
        copies.append((down_weight.at[aligned(quarter * 2 + half, 128), :], down_packed.at[half]))
    copies = [pltpu.make_async_copy(a, b, sems.at[i]) for i, (a, b) in enumerate(copies)]
    for copy in copies:
        copy.start()
    for copy in copies:
        copy.wait()


def call_pack_feed(up_weight, down_weight):
    spec = pl.BlockSpec(memory_space=pl.ANY)
    return pl.pallas_call(
        pack_feed,
        out_shape=(shaped(2, 128, 1024), shaped(2, 128, 1024)),
        in_specs=[spec, spec],
        out_specs=(VMEM_SPEC, VMEM_SPEC),
        scratch_shapes=[pltpu.SemaphoreType.DMA((10,))],
        compiler_params=pltpu.CompilerParams(vmem_limit_bytes=8 << 20),
        cost_estimate=pl.CostEstimate(flops=0, bytes_accessed=2 << 20, transcendentals=0),
        name="pack_feed",
    )(up_weight, down_weight)


def tie(value, *earlier):
    return lax.optimization_barrier((value, *earlier))[0]


def near_pieces(packed, half, *earlier, direct=False):
    mine = tie(lax.dynamic_index_in_dim(packed, half, 0, False), *earlier)
    if direct:
        return [flip(mine, step) for step in (1, 2, 3)]
    second = flip(mine, 2)
    return [flip(mine, 1), second, flip(second, 1)]


def far_pieces(near):
    return [swap(item, Y) for item in near]


def far_together(near):
    return swap(jnp.stack(near), Y)


def each_piece(own, near, far):
    _, place, y_bit, _ = spot()
    yield place, 0, own.at[0]
    yield place, 1, own.at[1]
    for step in (1, 2, 3):
        yield place ^ step, y_bit, near[step - 1]
        yield place ^ step, 1 - y_bit, far[step - 1]


def head_lanes(shape, parity):
    return (lax.broadcasted_iota(jnp.int32, shape, 1) // 64) == parity


def causal_block():
    shape = (BLOCK, BLOCK)
    return lax.broadcasted_iota(jnp.int32, shape, 0) >= lax.broadcasted_iota(jnp.int32, shape, 1)


def attend(
    x0, x1, x2, x3, own, z1, z2, z3, y1, y2, y3, cosines, sines,
    query, key, value, mixed, logs, hidden, qkv, out_rows, vectors, p0, p1, p32,
):
    _, _, _, position = spot()
    for relative, rows_in in enumerate((x0, x1, x2, x3)):
        hidden[aligned(position ^ relative, BLOCK), :] = rows_in[...]
    vectors[...] = jnp.zeros_like(vectors)
    for index, (shard, half, piece) in enumerate(each_piece(own, (z1, z2, z3), (y1, y2, y3))):
        qkv[aligned(shard * 2 + half, 128), :] = piece[:128, :768]
        for j in range(2):
            out_rows[aligned(shard, 64), aligned(half * 2 + j, 256)] = piece[j * 64 : j * 64 + 64, 768:]
        if index == 0 or index >= 2 and index % 2 == 0:
            small = wide(piece[128:144, :])
            lanes = aligned(shard, 256)
            vectors[0:1, lanes] = small[1:2, 256:512]
            vectors[1:2, lanes] = small[1:2, 512:768]
            for gain in range(4):
                vectors[2 + gain : 3 + gain, lanes] = small[2:3, gain * 256 : gain * 256 + 256]
            vectors[6:7, lanes] = small[1:2, :256]
            vectors[7:8, :] += small[0:1, :]

    def project(index, carry):
        rows = aligned(index, BLOCK)
        normed, _ = standardize(wide(hidden[rows, :]))
        block = rounded(normed * vectors[2:3, :])
        hidden[rows, :] = block
        raw = dot(block, qkv[...]) + vectors[7:8, :768]
        cos, sin = cosines[rows, :], sines[rows, :]
        for tile in range(2):
            at = tile * 128
            lanes = slice(at, at + 128)
            query[rows, lanes] = rounded(turn(raw[:, lanes], cos, sin)) * jnp.bfloat16(0.125)
            key[rows, lanes] = rounded(turn(raw[:, 256 + at : 384 + at], cos, sin))
        value[rows, :] = rounded(raw[:, 512:])
        return carry

    lax.fori_loop(0, GROUP, project, 0)
    causal = causal_block()
    logs[...] = jnp.zeros_like(logs)
    mixed[...] = jnp.zeros_like(mixed)
    lane = lax.broadcasted_iota(jnp.int32, (BLOCK, 128), 1)

    def head(index, carry):
        lanes = aligned(index >> 1, 128)
        mine = lane // 64 == (index & 1)
        for block in range(GROUP):
            rows = slice(block * BLOCK, block * BLOCK + BLOCK)
            seen = (block + 1) * BLOCK
            masked = jnp.where(mine, query[rows, lanes], jnp.bfloat16(0))
            scores = nt(masked, key[:seen, lanes])
            last = jnp.where(causal, scores[:, seen - BLOCK :], -1e30)
            scores = jnp.concatenate([scores[:, : seen - BLOCK], last], 1) if block else last
            best = jnp.max(scores, axis=1, keepdims=True)
            exps = jnp.exp(scores - best)
            total = jnp.sum(exps, axis=1, keepdims=True)
            out = dot(rounded(exps), value[:seen, lanes]) / total
            mixed[rows, lanes] = jnp.where(mine, rounded(out), mixed[rows, lanes])
            logs[rows, :] = jnp.where(lane == index, best + jnp.log(total), logs[rows, :])
        return carry

    lax.fori_loop(0, 4, head, 0)
    for relative, part in enumerate((p0, p1, p32.at[BLOCK:], p32.at[:BLOCK])):
        part[...] = rounded(dot(mixed[aligned(position ^ relative, BLOCK), :], out_rows[...]))


def pair_back(pair, query, key, value, mixed, logs, d_out, d_query, d_key, d_value):
    lanes = slice(pair * 128, pair * 128 + 128)
    causal = causal_block()
    lane = lax.broadcasted_iota(jnp.int32, (BLOCK, 128), 1)
    d_key[...] = jnp.zeros_like(d_key)
    d_value[...] = jnp.zeros_like(d_value)
    d_query[...] = jnp.zeros_like(d_query)

    def head(parity, carry):
        mine = lane // 64 == parity
        for block in range(GROUP):
            rows = slice(block * BLOCK, block * BLOCK + BLOCK)
            seen = (block + 1) * BLOCK
            keys, values = key[:seen, lanes], value[:seen, lanes]
            masked_q = jnp.where(mine, query[rows, lanes], jnp.bfloat16(0))
            masked_d = jnp.where(mine, d_out[rows, lanes], jnp.bfloat16(0))
            log = jnp.sum(jnp.where(lane == pair * 2 + parity, logs[rows, :], 0.0), 1, keepdims=True)
            delta = jnp.sum(wide(masked_d) * wide(mixed[rows, lanes]), 1, keepdims=True)
            probs = jnp.exp(nt(masked_q, keys) - log)
            last = jnp.where(causal, probs[:, seen - BLOCK :], 0.0)
            probs = jnp.concatenate([probs[:, : seen - BLOCK], last], 1) if block else last
            d_scores = rounded(probs * (nt(masked_d, values) - delta))
            d_query[rows, :] += jnp.where(mine, dot(d_scores, keys), 0.0)
            d_value[:seen, :] += tn(rounded(probs), masked_d)
            d_key[:seen, :] += tn(d_scores, masked_q)
        return carry

    lax.fori_loop(0, 2, head, 0)


def finish_back(cosines, sines, d_query, d_key, d_value, grads, shift_sums):
    shift_sums[...] = jnp.zeros_like(shift_sums)

    def finish(index, carry):
        rows = aligned(index, BLOCK)
        cos, sin = cosines[rows, :], -sines[rows, :]
        grads[rows, :128] = rounded(turn(d_query[rows, :] * 0.125, cos, sin))
        grads[rows, 128:256] = rounded(turn(d_key[rows, :], cos, sin))
        grads[rows, 256:] = rounded(d_value[rows, :])
        shift_sums[0:1, :] += jnp.sum(wide(grads[rows, :]), axis=0, keepdims=True)
        return carry

    lax.fori_loop(0, GROUP, finish, 0)


def attend_back_first(
    a0, a1, a2, a3, out_rows, query, key, value, mixed, logs, cosines, sines,
    d_out, grads, shift_sums, d_query, d_key, d_value,
):
    _, _, _, position = spot()
    for relative, rows_in in enumerate((a0, a1, a2, a3)):
        d_out[aligned(position ^ relative, BLOCK), :] = rounded(nt(rows_in[...], out_rows[...]))
    pair_back(0, query, key, value, mixed, logs, d_out, d_query, d_key, d_value)
    finish_back(cosines, sines, d_query, d_key, d_value, grads, shift_sums)


def attend_back_second(
    d_out, before, qkv, query, key, value, mixed, logs, cosines, sines,
    grads, shift_sums, p0, p1, p32, d_query, d_key, d_value, joined,
):
    _, _, _, position = spot()
    pair_back(1, query, key, value, mixed, logs, d_out, d_query, d_key, d_value)
    finish_back(cosines, sines, d_query, d_key, d_value, grads, shift_sums)
    for index in range(3):
        joined[:, index * 256 : index * 256 + 128] = before[:, index * 128 : index * 128 + 128]
        joined[:, index * 256 + 128 : index * 256 + 256] = grads[:, index * 128 : index * 128 + 128]
    for relative, part in enumerate((p0, p1, p32.at[BLOCK:], p32.at[:BLOCK])):
        part[...] = rounded(nt(joined[aligned(position ^ relative, BLOCK), :], qkv[...]))


CHUNK = 64


def in_chunks(step):
    def one(index, carry):
        step(aligned(index, CHUNK), pl.ds(pl.multiple_of(BLOCK + index * CHUNK, CHUNK), CHUNK))
        return carry

    lax.fori_loop(0, BLOCK // CHUNK, one, 0)


def after_attention(p0, core_in, x_in, rows_in, vectors, middle, hidden, normed_o, normed_f, inverses):
    def step(rows, low):
        branch = wide(p0[rows, :]) + wide(core_in[low, :]) + wide(x_in[rows, :]) + vectors[0:1, :]
        normed, inverse_o = standardize(branch)
        normed_o[rows, :] = normed
        total = wide(rows_in[rows, :]) + normed * vectors[3:4, :]
        middle[rows, :] = total
        normed, inverse_f = standardize(total)
        normed_f[rows, :] = normed
        hidden[rows, :] = rounded(normed * vectors[4:5, :])
        lane = lax.broadcasted_iota(jnp.int32, (CHUNK, 128), 1)
        inverses[rows, :] = jnp.where(lane < 64, inverse_o, inverse_f)

    in_chunks(step)


def after_feed(p0, core_in, x_in, middle, cotangent, vectors, layer_out, d_branch, sums):
    sums[...] = jnp.zeros_like(sums)

    def step(rows, low):
        branch = wide(p0[rows, :]) + wide(core_in[low, :]) + wide(x_in[rows, :]) + vectors[1:2, :]
        normed, inverse = standardize(branch)
        gain = vectors[5:6, :]
        layer_out[rows, :] = rounded(middle[rows, :] + normed * gain)
        upstream = wide(cotangent[rows, :])
        back = rounded(norm_back(normed, inverse, upstream * gain))
        d_branch[rows, :] = back
        sums[0:1, :] += jnp.sum(upstream * normed, axis=0, keepdims=True)
        sums[1:2, :] += jnp.sum(wide(back), axis=0, keepdims=True)

    in_chunks(step)


def after_feed_back(
    p0, core_in, x_in, cotangent, normed_o, normed_f, inverses, vectors, d_middle, d_branch, sums
):
    sums[...] = jnp.zeros_like(sums)

    def step(rows, low):
        d_hidden = wide(p0[rows, :]) + wide(core_in[low, :]) + wide(x_in[rows, :])
        normed = normed_f[rows, :]
        sums[0:1, :] += jnp.sum(d_hidden * normed, axis=0, keepdims=True)
        total = wide(cotangent[rows, :]) + norm_back(
            normed, inverses[rows, 64:65], d_hidden * vectors[4:5, :]
        )
        d_middle[rows, :] = total
        normed = normed_o[rows, :]
        sums[1:2, :] += jnp.sum(total * normed, axis=0, keepdims=True)
        back = rounded(norm_back(normed, inverses[rows, 0:1], total * vectors[3:4, :]))
        d_branch[rows, :] = back
        sums[2:3, :] += jnp.sum(wide(back), axis=0, keepdims=True)

    in_chunks(step)


def gain_in_sums(p0, p1, p32, x0, x1, x2, x3, sums):
    sums[...] = jnp.zeros_like(sums)

    def step(rows, low):
        for part, rows_in in ((p0[rows, :], x0), (p1[rows, :], x1), (p32[low, :], x2), (p32[rows, :], x3)):
            normed, _ = standardize(wide(rows_in[rows, :]))
            sums[0:1, :] += jnp.sum(wide(part) * normed, axis=0, keepdims=True)

    in_chunks(step)


def after_attention_back(p0, core_in, x_in, rows_in, d_middle, vectors, d_rows):
    def step(rows, low):
        d_hidden = wide(p0[rows, :]) + wide(core_in[low, :]) + wide(x_in[rows, :])
        normed, inverse = standardize(wide(rows_in[rows, :]))
        d_rows[rows, :] = rounded(
            d_middle[rows, :] + norm_back(normed, inverse, d_hidden * vectors[2:3, :])
        )

    in_chunks(step)


GELU_SCALE = math.sqrt(2.0 / math.pi)


def feed_rows(rows_in, up_mat, down_mat, vectors, before, after, part, at):
    rows = slice(at, at + BLOCK)

    def step(index, carry):
        lanes = aligned(index, BLOCK)
        raw = dot(rows_in[...], up_mat[:, lanes]) + vectors[6:7, lanes]
        before[rows, lanes] = raw
        after[rows, lanes] = rounded(jax.nn.gelu(raw))
        return carry

    lax.fori_loop(0, 4, step, 0)

    def out(index, carry):
        lanes = aligned(index, BLOCK)
        part[:, lanes] = rounded(dot(after[rows, :], down_mat[:, lanes]))
        return carry

    lax.fori_loop(0, 4, out, 0)


def feed_first(
    h0, h2, uo, u1, u2, u3, far_u, do, d1, d2, d3, far_d, vectors,
    up_mat, down_mat, before, after, p0, p2,
):
    for shard, half, piece in each_piece(uo, (u1, u2, u3), [far_u.at[i] for i in range(3)]):
        up_mat[aligned(shard * 2 + half, 128), :] = piece[...]
    for shard, half, piece in each_piece(do, (d1, d2, d3), [far_d.at[i] for i in range(3)]):
        down_mat[aligned(shard * 2 + half, 128), :] = piece[...]
    feed_rows(h0, up_mat, down_mat, vectors, before, after, p0, 0)
    feed_rows(h2, up_mat, down_mat, vectors, before, after, p2, BLOCK)


def feed_second(h1, h3, p2, up_mat, down_mat, vectors, before, after, p1, p32):
    p32[BLOCK:, :] = p2[...]
    feed_rows(h3, up_mat, down_mat, vectors, before, after, p32.at[:BLOCK], BLOCK)
    feed_rows(h1, up_mat, down_mat, vectors, before, after, p1, 0)


def feed_back_rows(rows_in, up_mat, down_mat, before, d_pre, part, sums, at):
    rows = slice(at, at + BLOCK)

    def step(index, carry):
        lanes = aligned(index, BLOCK)
        upstream = nt(rows_in[...], down_mat[lanes, :])
        raw = before[rows, lanes]
        square = raw * raw
        bent = jnp.tanh(GELU_SCALE * raw * (1.0 + 0.044715 * square))
        slope = 0.5 * (1.0 + bent) + 0.5 * GELU_SCALE * raw * (1.0 - bent * bent) * (
            1.0 + 3.0 * 0.044715 * square
        )
        back = rounded(upstream * slope)
        d_pre[rows, lanes] = back
        sums[0:1, lanes] += jnp.sum(wide(back), axis=0, keepdims=True)
        return carry

    lax.fori_loop(0, 4, step, 0)

    def out(index, carry):
        lanes = aligned(index, BLOCK)
        part[:, lanes] = rounded(nt(d_pre[rows, :], up_mat[lanes, :]))
        return carry

    lax.fori_loop(0, 4, out, 0)


def feed_back_first(m0, m2, up_mat, down_mat, before, d_pre, p0, p2, sums):
    sums[...] = jnp.zeros_like(sums)
    feed_back_rows(m0, up_mat, down_mat, before, d_pre, p0, sums, 0)
    feed_back_rows(m2, up_mat, down_mat, before, d_pre, p2, sums, BLOCK)


def feed_back_second(m1, m3, p2, up_mat, down_mat, before, sums_in, d_pre, p1, p32, sums):
    sums[...] = sums_in[...]
    p32[BLOCK:, :] = p2[...]
    feed_back_rows(m3, up_mat, down_mat, before, d_pre, p32.at[:BLOCK], sums, BLOCK)
    feed_back_rows(m1, up_mat, down_mat, before, d_pre, p1, sums, 0)


def put_halves(keep, send, step, at, top, bottom):
    _, _, y_bit, _ = spot()

    @pl.when(y_bit == 0)
    def _():
        keep[step, at : at + 128, :] = top
        send[step, at : at + 128, :] = bottom

    @pl.when(y_bit == 1)
    def _():
        keep[step, at : at + 128, :] = bottom
        send[step, at : at + 128, :] = top


def down_grads(first, second, m0, m1, m2, m3, keep, send):
    _, place, _, _ = spot()

    def one(step, carry):
        lanes = aligned(place ^ step, BLOCK)
        down = (
            tn(first[:BLOCK, lanes], m0[...])
            + tn(first[BLOCK:, lanes], m2[...])
            + tn(second[:BLOCK, lanes], m1[...])
            + tn(second[BLOCK:, lanes], m3[...])
        )
        down = rounded(down)
        put_halves(keep, send, step, 0, down[:128], down[128:])
        return carry

    lax.fori_loop(0, 4, one, 0)


def up_grads(h0, h1, h2, h3, u_first, u_second, keep, send):
    _, place, _, _ = spot()

    def one(step, carry):
        lanes = aligned(place ^ step, BLOCK)
        up = (
            tn(h0[:, lanes], u_first[:BLOCK, :])
            + tn(h2[:, lanes], u_first[BLOCK:, :])
            + tn(h1[:, lanes], u_second[:BLOCK, :])
            + tn(h3[:, lanes], u_second[BLOCK:, :])
        )
        up = rounded(up)
        put_halves(keep, send, step, 0, up[:128], up[128:])
        return carry

    lax.fori_loop(0, 4, one, 0)


def attention_grads_first(mixed, a0, a1, a2, a3, hidden, grads, keep, send, out_grad, block):
    _, place, _, position = spot()
    total = tn(mixed[aligned(position, BLOCK), :], a0[...])
    for relative, rows_in in ((1, a1), (2, a2), (3, a3)):
        total = total + tn(mixed[aligned(position ^ relative, BLOCK), :], rows_in[...])
    out_grad[...] = rounded(total)

    def one(step, carry):
        shard = place ^ step
        block[:, :384] = rounded(tn(hidden[:, aligned(shard, BLOCK)], grads[...]))
        mine = out_grad[aligned(shard, 64), :]
        for j in range(4):
            block[j * 64 : j * 64 + 64, 384:] = mine[:, j * 256 : j * 256 + 256]
        put_halves(keep, send, step, 0, block[:128, :], block[128:, :])
        return carry

    lax.fori_loop(0, 4, one, 0)


def attention_grads_second(
    hidden, grads, sums_f, sums_b, sums_a, sums_u, sums_q, sums_r, keep, send
):
    _, place, y_bit, _ = spot()

    def one(step, carry):
        shard = place ^ step
        block = rounded(tn(hidden[:, aligned(shard, BLOCK)], grads[...]))
        put_halves(keep, send, step, 0, block[:128], block[128:])
        lanes = aligned(shard, BLOCK)
        biases = []
        for index in range(3):
            at = index * 128
            pair = jnp.where(shard < 2, sums_q[0:1, at : at + 128], sums_r[0:1, at : at + 128])
            biases.append(jnp.where((shard & 1) == 0, pair[:, :64], pair[:, 64:]))
        zero = jnp.zeros((1, 192), jnp.float32)
        tops = [sums_b[2:3, lanes], sums_f[1:2, lanes], sums_a[0:1, lanes], *biases, zero]
        lows = [sums_b[1:2, lanes], sums_b[0:1, lanes], sums_f[0:1, lanes], sums_u[0:1, lanes], zero[:, :128]]
        halves = []
        for items in (tops, lows):
            flat = jnp.concatenate(items, 1)
            row = lax.broadcasted_iota(jnp.int32, (8, 384), 0)
            full = [jnp.broadcast_to(flat[:, i * 384 : i * 384 + 384], (8, 384)) for i in range(3)]
            rows = jnp.where(row == 0, full[0], jnp.where(row == 1, full[1], full[2]))
            halves.append(rounded(jnp.where(row < 3, rows, 0.0)))
        mine, other = jnp.where(y_bit == 0, halves[0], halves[1]), jnp.where(y_bit == 0, halves[1], halves[0])
        keep[step, 128:136, :] = mine
        send[step, 128:136, :] = other
        return carry

    lax.fori_loop(0, 4, one, 0)


def add_pairs(keep, come, stay, go):
    for step, out in enumerate((stay.at[0], go.at[0], stay.at[1], go.at[1])):
        out[...] = rounded(wide(keep[step]) + wide(come[step]))


def add_near(stay, come, own, go):
    own[...] = rounded(wide(stay[0]) + wide(come[0]))
    go[...] = rounded(wide(stay[1]) + wide(come[1]))


def each_part(own, x_part, y_part, core_part):
    rep = lax.axis_index("rep")
    refs = [own, x_part, y_part.at[0], y_part.at[1]] + [core_part.at[i] for i in range(4)]
    for relative, ref in enumerate(refs):
        flip = ((relative & 1) << 1) | ((relative & 2) << 1) | (relative >> 2)
        there = rep ^ flip
        yield there >> 2, there & 3, ref


def unpack_down(own, x_part, y_part, core_part, down):
    for y_bit, quarter, ref in each_part(own, x_part, y_part, core_part):
        down[aligned(quarter * 2 + y_bit, 128), :] = wide(ref[...])


def unpack_up(own, x_part, y_part, core_part, up):
    for y_bit, quarter, ref in each_part(own, x_part, y_part, core_part):
        for there in range(4):
            lanes = pl.ds(pl.multiple_of(there * 1024 + quarter * 256, 256), 256)
            up[aligned(y_bit, 128), lanes] = wide(ref[:, there * 256 : there * 256 + 256])


def unpack_attention(
    own, x_part, y_part, core_part, own2, x_part2, y_part2, core_part2,
    query, key, value, out_weight, qb, kb, vb, ob, db, ga, gb, gc, gd, ub,
):
    first = list(each_part(own, x_part, y_part, core_part))
    second = list(each_part(own2, x_part2, y_part2, core_part2))
    row = lax.broadcasted_iota(jnp.int32, (128, 512), 0)
    col = lax.broadcasted_iota(jnp.int32, (128, 512), 1)
    sets = ((0, 1, 4, 5), (2, 3, 6, 7))
    chosen = []
    for index in sets[0]:
        quarter = first[index][1]
        chosen.append(rounded(wide(col == (row // 64) * 256 + quarter * 64 + row % 64)))
    chosen = jnp.concatenate(chosen, 0)
    for pair, parts in enumerate((first, second)):
        for members in sets:
            rows = aligned(parts[members[0]][0], 128)
            for index, out in enumerate((query, key, value)):
                lanes = slice(index * 128, index * 128 + 128)
                joined = jnp.concatenate([parts[i][2][:128, lanes] for i in members], 1)
                out[rows, pair * 512 : pair * 512 + 512] = dot(joined, chosen)
    for y_bit, quarter, ref in first:
        for j in range(2):
            out_weight[aligned(quarter, 64), aligned(y_bit * 2 + j, 256)] = wide(
                ref[j * 64 : j * 64 + 64, 384:]
            )
    y_bit = first[0][0]
    flats = []
    for members in sets:
        rows = [wide(second[i][2][128:136, :]) for i in members]
        total = rows[0] + rows[1] + rows[2] + rows[3]
        flats.append((total, rows))
    mine, other = flats
    for half, (outs, size) in enumerate((((ob, db, ga), 64), ((gb, gc, gd), 256))):
        take = y_bit == half
        total = jnp.where(take, mine[0], other[0])
        flat = jnp.concatenate([total[0:1, :], total[1:2, :]], 1)
        for index, out in enumerate(outs):
            out[...] = flat[:, index * 256 : index * 256 + 256]
        locals_ = [jnp.where(take, a, b)[2:3, :] for a, b in zip(mine[1], other[1], strict=True)]
        quarters = [first[i][1] for i in sets[0]]
        for there in range(4):
            value_at = jnp.zeros((1, 384), jnp.float32)
            for quarter, item in zip(quarters, locals_, strict=True):
                value_at = value_at + jnp.where(quarter == there, item, 0.0)
            if half == 0:
                for index, out in enumerate((qb, kb, vb)):
                    out[:, there * 64 : there * 64 + 64] = value_at[:, index * 64 : index * 64 + 64]
            else:
                ub[:, there * 256 : there * 256 + 256] = value_at[:, :256]


def sum_pairs(keep, come):
    two = shaped(2, *keep.shape[1:])
    return call(add_pairs, [two, two], keep, come)


def sum_near(stay, come):
    one = shaped(*stay.shape[1:])
    return call(add_near, [one, one], stay, come)


def sum_far(own, come):
    return rounded(wide(own) + wide(come))


def gather_packs(total, *earlier):
    x_part = swap(total, X)
    two = jnp.stack([total, x_part])
    y_part = swap(two, Y)
    return total, x_part, y_part, swap(tie(jnp.concatenate([two, y_part]), *earlier), CORE)


def fast_device(
    layer_input,
    query_weight,
    query_bias,
    key_weight,
    key_bias,
    value_weight,
    value_bias,
    output_weight,
    output_bias,
    up_weight,
    up_bias,
    down_weight,
    down_bias,
    attention_gain_in,
    attention_gain_out,
    feedforward_gain_in,
    feedforward_gain_out,
    layer_cotangent,
):
    f32, bf16 = jnp.float32, jnp.bfloat16
    replicas = lax.axis_size("rep")
    rows, width = layer_input.shape
    tokens = rows * GROUP
    quarter, place, y_bit, _ = spot()
    pairs = token_pairs(replicas)
    back_pairs = [(there, here) for here, there in pairs]
    both = ("rep", "shard")
    part = shaped(rows, width)
    part32 = shaped(rows, width, kind=f32)
    sums = shaped(8, width, kind=f32)

    def spread(piece):
        return swap(piece, X), swap(piece, CORE)

    def gather_sum(p1, p32):
        core_in = swap(p32, CORE)
        return core_in, swap(rounded(wide(p1) + wide(core_in[:rows])), X)

    own_rows = lax.ppermute(layer_input, both, pairs)
    (packed,) = call(
        pack_attention,
        [shaped(2, 144, width)],
        query_weight,
        key_weight,
        value_weight,
        output_weight,
        query_bias,
        key_bias,
        value_bias,
        up_bias,
        output_bias,
        down_bias,
        attention_gain_in,
        attention_gain_out,
        feedforward_gain_in,
        feedforward_gain_out,
    )
    near_a = near_pieces(packed, y_bit)
    cosines, sines = rope_tables(tokens, 64)
    up_packed, down_packed = call_pack_feed(up_weight, down_weight)
    own_rows = tie(own_rows, near_a[1], cosines, sines, up_packed)
    x1, x2 = spread(own_rows)
    blocks = own_rows, x1, x2, swap(x1, CORE)
    far_a = far_pieces(near_a)
    near_u = near_pieces(up_packed, y_bit, *near_a, direct=True)
    cotangent = lax.ppermute(tie(layer_cotangent, *near_u), both, pairs)
    two16 = shaped(2 * rows, width)
    head_rows = shaped(tokens, 256)
    query, key, value, mixed, logs, hidden_a, qkv, out_rows, vectors, p0, p1, p32 = call(
        attend,
        [head_rows] * 4
        + [
            shaped(tokens, 128, kind=f32),
            shaped(tokens, width),
            shaped(width, 768),
            shaped(256, width),
            sums,
        ]
        + [part, part, two16],
        *blocks,
        packed,
        *near_a,
        *far_a,
        cosines,
        sines,
        flops=2 * tokens * 1024 * 1024 + 8 * tokens * tokens * 64 * 2,
        exps=2 * tokens * tokens,
        room=14,
    )
    p32 = tie(p32, *near_u)
    far_u = far_together(near_u)
    near_d = near_pieces(down_packed, y_bit, *near_u)
    core_in, x_in = gather_sum(p1, p32)
    x_in = tie(x_in, far_u, cotangent, *near_d)
    far_d = far_together(near_d)
    middle, hidden_own, normed_o, normed_f, inverses = call(
        after_attention,
        [part32, part, part32, part32, shaped(rows, 128, kind=f32)],
        p0,
        core_in,
        x_in,
        own_rows,
        vectors,
    )
    h0 = hidden_own
    h1, h2 = spread(h0)
    two32 = shaped(2 * rows, width, kind=f32)
    square = shaped(width, width)
    flops = 4 * 2 * rows * 1024 * 1024
    up_mat, down_mat, before_a, after_a, p0, p2 = call(
        feed_first,
        [square, square, two32, two16, part, part],
        h0, h2, up_packed, *near_u, far_u, down_packed, *near_d, far_d, vectors,
        flops=flops, room=10,
    )
    h1 = tie(h1, p2)
    h3 = swap(h1, CORE)
    before_b, after_b, p1, p32 = call(
        feed_second,
        [two32, two16, part, two16],
        h1, h3, p2, up_mat, down_mat, vectors,
        flops=flops, room=10,
    )
    core_in, x_in = gather_sum(p1, p32)
    layer_output, d_branch, sums_f = call(
        after_feed, [part, part, sums], p0, core_in, x_in, middle, cotangent, vectors
    )
    m0 = d_branch
    m1, m2 = spread(m0)
    u_first, p0, p2, sums_u = call(
        feed_back_first,
        [two16, part, part, sums],
        m0, m2, up_mat, down_mat, before_a,
        flops=flops, room=10,
    )
    m1 = tie(m1, u_first)
    m3 = swap(m1, CORE)
    layer_output = lax.ppermute(layer_output, both, back_pairs)
    m3 = tie(m3, layer_output)
    packs = [shaped(4, 128, width)] * 2
    grad_flops = 2 * tokens * 1024 * 1024
    u_second, p1, p32, sums_u = call(
        feed_back_second,
        [two16, part, two16, sums],
        m1, m3, p2, up_mat, down_mat, before_b, sums_u,
        flops=flops, room=10,
    )
    core_in, x_in = gather_sum(p1, p32)
    pack_d = call(
        down_grads, packs, after_a, after_b, m0, m1, m2, tie(m3, u_second), flops=grad_flops, room=10
    )
    come_d = swap(pack_d[1], Y)
    pack_u = call(
        up_grads,
        packs,
        h0, h1, h2, h3, u_first, tie(u_second, *pack_d),
        flops=grad_flops, room=10,
    )
    flops = grad_flops
    x_in = tie(x_in, *pack_u)
    d_middle, d_branch, sums_b = call(
        after_feed_back,
        [part32, part, sums],
        p0,
        core_in,
        x_in,
        cotangent,
        normed_o,
        normed_f,
        inverses,
        vectors,
    )
    a0 = d_branch
    a1, a2 = spread(a0)
    stay_d, go_d = sum_pairs(tie(pack_d[0], d_branch), come_d)
    come_u = swap(pack_u[1], Y)
    a1 = tie(a1, go_d)
    a3 = swap(a1, CORE)
    a_blocks = a0, a1, a2, a3
    come_d = flip(go_d, 1)
    grad32 = [pltpu.VMEM((tokens, 128), f32)] * 3
    back_flops = tokens * 1024 * 1024 + 10 * tokens * tokens * 64 * 2
    d_out, grads_first, sums_q = call(
        attend_back_first,
        [shaped(tokens, 256), shaped(tokens, 384), shaped(8, 384, kind=f32)],
        *a_blocks, out_rows, query, key, value, mixed, logs, cosines, sines,
        scratch=grad32, flops=back_flops, exps=tokens * tokens, room=14,
    )
    pack_a = call(
        attention_grads_first,
        [shaped(4, 128, 640)] * 2,
        mixed, *a_blocks, hidden_a, grads_first,
        scratch=[pltpu.VMEM((256, width), bf16), pltpu.VMEM((256, 640), bf16)],
        flops=flops // 2, room=10,
    )
    grads_second, sums_r, p0, p1, p32 = call(
        attend_back_second,
        [shaped(tokens, 384), shaped(8, 384, kind=f32), part, part, two16],
        tie(d_out, *pack_a), grads_first, qkv, query, key, value, mixed, logs, cosines, sines,
        scratch=grad32 + [pltpu.VMEM((tokens, 768), bf16)],
        flops=back_flops, exps=tokens * tokens, room=14,
    )
    come_a = swap(pack_a[1], Y)
    p32 = tie(p32, come_u, come_d)
    core_in, x_in = gather_sum(p1, p32)
    own_d, go_d = sum_near(tie(stay_d, p32), come_d)
    come_d = flip(go_d, 2)
    stay_u, go_u = sum_pairs(tie(pack_u[0], p32), come_u)
    (sums_a,) = call(gain_in_sums, [sums], p0, p1, p32, *blocks)
    pack_b = call(
        attention_grads_second,
        [shaped(4, 136, 384)] * 2,
        hidden_a, grads_second, sums_f, sums_b, sums_a, sums_u, sums_q, sums_r,
        flops=flops // 2, room=10,
    )
    x_in = tie(x_in, *pack_b, go_u)
    (d_rows,) = call(
        after_attention_back, [part], p0, core_in, x_in, own_rows, d_middle, vectors
    )
    input_gradient = lax.ppermute(d_rows, both, back_pairs)
    total_d = sum_far(tie(own_d, d_rows), come_d)
    own_u, go_u = sum_near(tie(stay_u, d_rows), flip(go_u, 1))
    stay_a, go_a = sum_pairs(tie(pack_a[0], d_rows), come_a)
    own_a, go_a = sum_near(stay_a, flip(go_a, 1))
    stay_b, go_b = sum_pairs(pack_b[0], swap(pack_b[1], Y))
    total_u = sum_far(own_u, flip(go_u, 2))
    own_b, go_b = sum_near(tie(stay_b, input_gradient), flip(go_b, 1))
    total_a = sum_far(own_a, flip(go_a, 2))
    total_b = sum_far(own_b, flip(go_b, 2))
    (g_down,) = call(unpack_down, [shaped(*down_weight.shape, kind=f32)], *gather_packs(total_d))
    (g_up,) = call(unpack_up, [shaped(*up_weight.shape, kind=f32)], *gather_packs(total_u))
    packs_a = gather_packs(total_a)
    packs_b = gather_packs(total_b, g_down)
    g_query, g_key, g_value, g_out, *small = call(
        unpack_attention,
        [part32] * 4 + [shaped(1, 256, kind=f32)] * 9 + [shaped(1, 1024, kind=f32)],
        *packs_a,
        *packs_b,
    )
    small = [item.reshape(-1) for item in small]
    input_gradient = input_gradient.astype(f32)
    return (
        layer_output,
        input_gradient,
        g_query,
        small[0],
        g_key,
        small[1],
        g_value,
        small[2],
        g_out,
        small[3],
        g_up,
        small[9],
        g_down,
        small[4],
        small[5],
        small[6],
        small[7],
        small[8],
    )


def solution(mesh):
    replicas, shards = mesh.shape["rep"], mesh.shape["shard"]
    fits = shards == 4 and replicas == 8 and HEADS % 16 == 0
    return jax.shard_map(
        fast_device if fits else general_device,
        mesh=mesh,
        in_specs=(
            P(("rep", "shard"), None),
            P("shard", None),
            P("shard"),
            P("shard", None),
            P("shard"),
            P("shard", None),
            P("shard"),
            P("shard", None),
            P("shard"),
            P("shard", None),
            P("shard"),
            P("shard", None),
            P("shard"),
            P("shard"),
            P("shard"),
            P("shard"),
            P("shard"),
            P(("rep", "shard"), None),
        ),
        out_specs=(
            P(("rep", "shard"), None),
            P(("rep", "shard"), None),
            P("shard", None),
            P("shard"),
            P("shard", None),
            P("shard"),
            P("shard", None),
            P("shard"),
            P("shard", None),
            P("shard"),
            P("shard", None),
            P("shard"),
            P("shard", None),
            P("shard"),
            P("shard"),
            P("shard"),
            P("shard"),
            P("shard"),
        ),
        check_vma=False,
    )
```
